128 devices in a mesh: px: 8 (over x, z_lo), py: 16 (over z_hi, y, core).
Axes of the slice: x: 4, y: 4, z: 4 (z_hi: 2, z_lo: 2; z = z_hi * 2 + z_lo), core: 2. Of those that a mesh axis runs over, the one named last changes fastest.
Arguments:
- velocity: float32 [3, 8, 512, 2048], P(None, None, 'py', 'px'), may hold values from -6 to 6
- thickness: float32 [8, 512, 2048], P(None, 'py', 'px'), may hold values from 1 to 4
- velocity_tendency: float32 [3, 8, 512, 2048], P(None, None, 'py', 'px'), may hold values from -6 to 6
- thickness_tendency: float32 [8, 512, 2048], P(None, 'py', 'px'), may hold values from -0.5 to 0.5
- cell_distance: float32 [3, 512, 2048], P(None, 'py', 'px'), may hold values from 0.5 to 2
- edge_length: float32 [3, 512, 2048], P(None, 'py', 'px'), may hold values from 0.5 to 2
- cell_area: float32 [512, 2048], P('py', 'px'), may hold values from 1 to 4
- kite_area: float32 [2, 3, 512, 2048], P(None, None, 'py', 'px'), may hold values from 0.2 to 0.8
- coriolis: float32 [2, 512, 2048], P(None, 'py', 'px'), may hold values from -1 to 1
Outputs:
- vertex_potential: float32 [2, 8, 512, 2048], P(None, None, 'py', 'px')
- kinetic_energy: float32 [8, 512, 2048], P(None, 'py', 'px')
- cell_potential: float32 [8, 512, 2048], P(None, 'py', 'px')
- edge_potential: float32 [3, 8, 512, 2048], P(None, None, 'py', 'px')
The draws below stay inside these ranges and needn't reach their ends.
All inputs are finite; a program needn't handle non-finite values.
Results may differ from the reference program's by a relative error of at most 0.00002.
Values sent between devices are 32-bit elements; how exact they have to be, the bound alone decides.
No kernel may reach another device: no remote copies, remote signals or barrier semaphores. Data moves between devices by JAX's collectives and lax.ppermute only.
A program may use at most 64 MiB of HBM per device.

```python
import math
import jax
import jax.numpy as jnp

NLEV = 8
SECTIONS = 4
NX = 512
NY = 2048


def levels(key, shape, split, least, top_value):
    def one(position, blocks):
        draws = jax.random.uniform(jax.random.fold_in(jax.random.fold_in(key, 6), position), (blocks,), jnp.float32, least / len(split), top_value / len(split))
        return jnp.repeat(jnp.exp(draws), shape[position] // blocks).reshape((-1,) + (1,) * (len(shape) - position - 1))

    loudness = one(*split[0])
    for cut in split[1:]:
        loudness = loudness * one(*cut)
    return loudness


def noise(own_key, extent, scale, bound, shards=(), dtype=jnp.bfloat16):
    values = scale * jax.random.normal(own_key, extent, jnp.float32)
    if shards:
        values = values * levels(own_key, extent, shards, -0.22, 0.18)
    return jnp.clip(values, -bound, bound).astype(dtype)


def setup_inputs(seed: int = 0) -> dict:
    arg_keys = jax.random.split(jax.random.key(seed), 10)
    velocity = noise(arg_keys[0], (3, NLEV, NX, NY), 1.0, 6.0, ((2, 16), (3, 8)), jnp.float32)
    thickness = jnp.clip(jnp.exp(math.log(4.0) - 1.3862944 * jax.random.uniform(arg_keys[1], (NLEV, NX, NY), jnp.float32) ** levels(arg_keys[1], (NLEV, NX, NY), ((1, 16), (2, 8)), -0.2, 0.2)), 1.0, 4.0)
    velocity_tendency = noise(arg_keys[2], (3, NLEV, NX, NY), 1.0, 6.0, ((2, 16), (3, 8)), jnp.float32)
    thickness_tendency = jnp.clip(jax.random.uniform(arg_keys[3], (NLEV, NX, NY), jnp.float32, -0.5, 0.5) * levels(arg_keys[3], (NLEV, NX, NY), ((1, 16), (2, 8)), -0.4, 0.0), -0.5, 0.5)
    cell_distance = jnp.clip(jnp.exp(math.log(2.0) - 1.3862944 * jax.random.uniform(arg_keys[4], (3, NX, NY), jnp.float32) ** levels(arg_keys[4], (3, NX, NY), ((1, 16), (2, 8)), -0.2, 0.2)), 0.5, 2.0)
    edge_length = jnp.clip(jnp.exp(math.log(2.0) - 1.3862944 * jax.random.uniform(arg_keys[5], (3, NX, NY), jnp.float32) ** levels(arg_keys[5], (3, NX, NY), ((1, 16), (2, 8)), -0.2, 0.2)), 0.5, 2.0)
    cell_area = jnp.clip(jnp.exp(math.log(4.0) - 1.3862944 * jax.random.uniform(arg_keys[6], (NX, NY), jnp.float32) ** levels(arg_keys[6], (NX, NY), ((0, 16), (1, 8)), -0.2, 0.2)), 1.0, 4.0)
    kite_area = jnp.clip(jnp.exp(math.log(0.8) - 1.3862944 * jax.random.uniform(arg_keys[7], (2, 3, NX, NY), jnp.float32) ** levels(arg_keys[7], (2, 3, NX, NY), ((2, 16), (3, 8)), -0.2, 0.2)), 0.2, 0.8)
    coriolis = jnp.clip(jax.random.uniform(arg_keys[8], (2, NX, NY), jnp.float32, -1.0, 1.0) * levels(arg_keys[8], (2, NX, NY), ((1, 16), (2, 8)), -0.4, 0.0), -1.0, 1.0)
    return dict(velocity=velocity, thickness=thickness, velocity_tendency=velocity_tendency, thickness_tendency=thickness_tendency, cell_distance=cell_distance, edge_length=edge_length, cell_area=cell_area, kite_area=kite_area, coriolis=coriolis)


SECTION_STEP = (0.0, 0.5, 0.5, 1.0)
SECTION_WEIGHT = (1.0 / 6.0, 1.0 / 3.0, 1.0 / 3.0, 1.0 / 6.0)
UPWIND_FACTOR = 0.5


def neighbour(field, first_off, second_off):
    return jnp.roll(field, (-first_off, -second_off), axis=(-2, -1))


def reference(velocity, thickness, velocity_tendency, thickness_tendency, cell_distance, edge_length, cell_area, kite_area, coriolis):
    triangle_area = jnp.sum(kite_area, axis=1)
    edge_weight = 0.25 * cell_distance * edge_length
    vertex_total = jnp.zeros((2,) + thickness.shape, jnp.float32)
    energy_total = jnp.zeros(thickness.shape, jnp.float32)
    cell_total = jnp.zeros(thickness.shape, jnp.float32)
    edge_total = jnp.zeros(velocity.shape, jnp.float32)
    for section_index in range(SECTIONS):
        step_size = SECTION_STEP[section_index]
        weight_now = SECTION_WEIGHT[section_index]
        section_velocity = velocity + step_size * velocity_tendency
        section_thickness = thickness + step_size * thickness_tendency
        edge_flux = section_velocity * cell_distance[:, None]
        circulation_first = edge_flux[0] + neighbour(edge_flux[2], 1, 0) - edge_flux[1]
        circulation_second = edge_flux[1] - edge_flux[2] - neighbour(edge_flux[0], -1, 1)
        height_first = (kite_area[0, 0] * section_thickness + kite_area[0, 1] * neighbour(section_thickness, 1, 0)
                        + kite_area[0, 2] * neighbour(section_thickness, 0, 1)) / triangle_area[0]
        height_second = (kite_area[1, 0] * section_thickness + kite_area[1, 1] * neighbour(section_thickness, 0, 1)
                         + kite_area[1, 2] * neighbour(section_thickness, -1, 1)) / triangle_area[1]
        potential_first = (coriolis[0] + circulation_first / triangle_area[0]) / height_first
        potential_second = (coriolis[1] + circulation_second / triangle_area[1]) / height_second
        energy = edge_weight[:, None] * section_velocity * section_velocity
        kinetic = (energy[0] + energy[1] + energy[2] + neighbour(energy[0], -1, 0)
                   + neighbour(energy[1], 0, -1) + neighbour(energy[2], 1, -1)) / cell_area
        cell_value = (potential_first + potential_second + neighbour(potential_first, -1, 0)
                      + neighbour(potential_first, 0, -1) + neighbour(potential_second, 0, -1)
                      + neighbour(potential_second, 1, -1)) / 6.0
        mean_zero = 0.5 * (potential_first + neighbour(potential_second, 1, -1))
        mean_one = 0.5 * (potential_first + potential_second)
        mean_two = 0.5 * (potential_second + neighbour(potential_first, -1, 0))
        grad_zero = (neighbour(cell_value, 1, 0) - cell_value) / cell_distance[0]
        grad_one = (neighbour(cell_value, 0, 1) - cell_value) / cell_distance[1]
        grad_two = (neighbour(cell_value, -1, 1) - cell_value) / cell_distance[2]
        section_edge = jnp.stack([
            mean_zero - UPWIND_FACTOR * section_velocity[0] * grad_zero,
            mean_one - UPWIND_FACTOR * section_velocity[1] * grad_one,
            mean_two - UPWIND_FACTOR * section_velocity[2] * grad_two])
        vertex_total = vertex_total + weight_now * jnp.stack([potential_first, potential_second])
        energy_total = energy_total + weight_now * kinetic
        cell_total = cell_total + weight_now * cell_value
        edge_total = edge_total + weight_now * section_edge
    return vertex_total, energy_total, cell_total, edge_total
```

```python
import jax
import jax.numpy as jnp
from jax import lax
from jax.experimental import pallas as pl
from jax.experimental.pallas import tpu as pltpu
from jax.sharding import PartitionSpec as P

F32 = jnp.float32
LV = 8
BASE = 8
UPB, DNB = BASE - 1, BASE + 32


def iota(shape, dim):
    return lax.broadcasted_iota(jnp.int32, shape, dim)


def left_shift(x, col):
    n = x.shape[1]
    return jnp.where(iota(x.shape, 1) == n - 1, col, pltpu.roll(x, n - 1, 1))


def right_shift(x, col):
    return jnp.where(iota(x.shape, 1) == 0, col, pltpu.roll(x, 1, 1))


def row_up(x, row):
    n = x.shape[0]
    return jnp.where(iota(x.shape, 0) == n - 1, row, pltpu.roll(x, n - 1, 0))


def row_down(x, row):
    return jnp.where(iota(x.shape, 0) == 0, row, pltpu.roll(x, 1, 0))


def section_sums(n0, dn, d0, dd):
    n1, d1 = n0 + dn, d0 + dd
    ns, ds = n0 + n1, d0 + d1
    ends = d0 * d1
    inv = 1.0 / (ends * ds)
    half = ns * ends * inv
    side = ds * inv
    last = n1 * d0 * side
    first = n0 * d1 * side
    return (first + last) * (1.0 / 6.0) + half * (2.0 / 3.0), half * (1.0 / 3.0) + last * (1.0 / 6.0)


def energy(w, v, vt):
    return w * (v * v + v * vt + vt * vt * (1.0 / 3.0))


(RH, RHT, RU0, RU0T, RU1, RU1T, RU2, RU2T, RH1, RH1T, RU01, RU01T) = range(12)
RGEO = 96
(LH, LHT, LU0, LU0T, LU1, LU1T, LU2, LU2T, LE1, LE2) = range(10)
LGEO = 80
(TH, THT, TH1, TH1T, TU0, TU0T, TU1, TU1T, TU11, TU11T, TU2, TU2T, TU21, TU21T, TE2) = range(15)
(BH, BHT, BH1, BH1T, BU0, BU0T, BU01, BU01T, BU1, BU1T, BU11, BU11T, BU2, BU2T, BE0) = range(15, 30)
RAW = 30


def pack_kernel(v, h, vt, ht, d, el, k, f, send_a, send_b, own0, raw):
    odd = lax.rem(lax.axis_index("px"), 2) == 1
    rows, cols = h.shape[1], h.shape[2]
    half = cols - 128
    lanes = iota((rows, 128), 1)
    to_left = jnp.zeros((rows, 128), F32)
    to_right = jnp.zeros((rows, 128), F32)
    first = [d[e, :, 0:128] for e in range(3)]
    last = [d[e, :, half:cols] for e in range(3)]
    weight = [0.25 * last[e] * el[e, :, half:cols] for e in range(3)]
    for lev in range(LV):
        low, high = [], []
        for x in (h, ht):
            low.append((x[lev, :, 0:128], 0))
        low = [(h[lev, :, 0:128], 0), (ht[lev, :, 0:128], 0)]
        high = [h[lev, :, half:cols], ht[lev, :, half:cols]]
        for e in range(3):
            for x in (v, vt):
                low.append((first[e] * x[e, lev, :, 0:128], 0))
                high.append(last[e] * x[e, lev, :, half:cols])
        low += [(low[0][0], 1), (low[1][0], 1), (low[2][0], 1), (low[3][0], 1)]
        for e in (1, 2):
            high.append(energy(weight[e], v[e, lev, :, half:cols], vt[e, lev, :, half:cols]))
        for n, (x, c) in enumerate(low):
            to_left = jnp.where(lanes == LV * n + lev, x[:, c : c + 1], to_left)
        for n, x in enumerate(high):
            to_right = jnp.where(lanes == LV * n + lev, x[:, 127:128], to_right)
    geo_low = [k[a, b, :, 0:128] for a in range(2) for b in range(3)]
    geo_high = [k[a, b, :, half:cols] for a in range(2) for b in range(3)]
    for a in range(2):
        geo_low.append((geo_low[3 * a] + geo_low[3 * a + 1] + geo_low[3 * a + 2]) * f[a, :, 0:128])
        geo_high.append((geo_high[3 * a] + geo_high[3 * a + 1] + geo_high[3 * a + 2]) * f[a, :, half:cols])
    for n in range(8):
        to_left = jnp.where(lanes == RGEO + n, geo_low[n][:, 0:1], to_left)
        to_right = jnp.where(lanes == LGEO + n, geo_high[n][:, 127:128], to_right)
    send_a[...] = jnp.where(odd, to_left, to_right)
    send_b[...] = jnp.where(odd, to_right, to_left)
    own0[...] = to_left

    end = rows - 1
    for x, n in ((h, TH), (ht, THT)):
        raw[n] = x[:, 0, :]
        raw[n + 2] = x[:, 1, :]
    for x, n in ((h, BH), (ht, BHT)):
        raw[n] = x[:, end, :]
        raw[n + 2] = x[:, end - 1, :]
    for x, t in ((v, 0), (vt, 1)):
        for e, r, n in (
            (0, 0, TU0),
            (1, 0, TU1),
            (1, 1, TU11),
            (2, 0, TU2),
            (2, 1, TU21),
            (0, end, BU0),
            (0, end - 1, BU01),
            (1, end, BU1),
            (1, end - 1, BU11),
            (2, end, BU2),
        ):
            raw[n + t] = d[e, r : r + 1, :] * x[e, :, r, :]
    raw[TE2] = energy(0.25 * d[2, 0:1, :] * el[2, 0:1, :], v[2, :, 0, :], vt[2, :, 0, :])
    raw[BE0] = energy(0.25 * d[0, end : end + 1, :] * el[0, end : end + 1, :], v[0, :, end, :], vt[0, :, end, :])


def af_row(k, f, a, r):
    return (k[a, 0, r : r + 1, :] + k[a, 1, r : r + 1, :] + k[a, 2, r : r + 1, :]) * f[a, r : r + 1, :]


def fld(t, n):
    return t[LV * n : LV * n + LV, :]


def column_left(lt, h0, h0t, u00, u00t):
    k = [lt[LGEO + n : LGEO + n + 1, :] for n in range(8)]
    up = lambda x: pltpu.roll(x, 127, 1)
    dn = lambda x: pltpu.roll(x, 1, 1)
    h, hp, u0, u0p, u1, u1p, u2, u2p = (fld(lt, n) for n in range(8))
    q0 = section_sums(
        k[6] + u0 - u1 + up(u2),
        u0p - u1p + up(u2p),
        k[0] * h + k[1] * up(h) + k[2] * h0,
        k[0] * hp + k[1] * up(hp) + k[2] * h0t,
    )
    q1 = section_sums(
        k[7] + u1 - u2 - dn(u00),
        u1p - u2p - dn(u00t),
        k[3] * h + k[4] * h0 + k[5] * dn(h0),
        k[3] * hp + k[4] * h0t + k[5] * dn(h0t),
    )
    return q0, q1


def column_right(rt):
    k = [rt[RGEO + n : RGEO + n + 1, :] for n in range(8)]
    up = lambda x: pltpu.roll(x, 127, 1)
    dn = lambda x: pltpu.roll(x, 1, 1)
    h, hp, u0, u0p, u1, u1p, u2, u2p, h1, h1p, u01, u01p = (fld(rt, n) for n in range(12))
    q0 = section_sums(
        k[6] + u0 - u1 + up(u2),
        u0p - u1p + up(u2p),
        k[0] * h + k[1] * up(h) + k[2] * h1,
        k[0] * hp + k[1] * up(hp) + k[2] * h1p,
    )
    q1 = section_sums(
        k[7] + u1 - u2 - dn(u01),
        u1p - u2p - dn(u01p),
        k[3] * h + k[4] * h1 + k[5] * dn(h1),
        k[3] * hp + k[4] * h1p + k[5] * dn(h1p),
    )
    return q0, q1


def lane_col(x, lane):
    return x[:, lane : lane + 1]


def merge_kernel(slab_a, slab_b, own0, raw, k, f, msg_a, msg_b, ext):
    odd_x = lax.rem(lax.axis_index("px"), 2) == 1
    odd_y = lax.rem(lax.axis_index("py"), 2) == 1
    rows = slab_a.shape[0]
    end = rows - 1
    left = jnp.where(odd_x, slab_a[...], slab_b[...])
    right = jnp.where(odd_x, slab_b[...], slab_a[...])
    ext[0, BASE : BASE + rows, :] = left
    ext[1, BASE : BASE + rows, :] = right
    ext[2, BASE : BASE + rows, :] = own0[...]
    lt, rt, ot = (jnp.transpose(ext[n]) for n in range(3))
    q0l, q1l = column_left(lt, fld(ot, RH), fld(ot, RHT), fld(ot, RU0), fld(ot, RU0T))
    q0r, q1r = column_right(rt)
    r0, r1 = BASE, BASE + 1
    e0, e1 = BASE + end, BASE + end - 1
    krow = lambda a, b, r: k[a, b, r : r + 1, :]

    h_0 = [left_shift(raw[TH + t], lane_col(fld(rt, RH + t), r0)) for t in range(2)]
    h_1 = [left_shift(raw[TH1 + t], lane_col(fld(rt, RH + t), r1)) for t in range(2)]
    u_0 = [left_shift(raw[TU0 + t], lane_col(fld(rt, RU0 + t), r0)) for t in range(2)]
    up0 = section_sums(
        af_row(k, f, 0, 0) + raw[TU0] - raw[TU1] + raw[TU21],
        raw[TU0T] - raw[TU1T] + raw[TU21T],
        *(krow(0, 0, 0) * raw[TH + t] + krow(0, 1, 0) * raw[TH1 + t] + krow(0, 2, 0) * h_0[t] for t in range(2)),
    )
    up1 = section_sums(
        af_row(k, f, 1, 1) + raw[TU11] - raw[TU21] - u_0[0],
        raw[TU11T] - raw[TU21T] - u_0[1],
        *(krow(1, 0, 1) * raw[TH1 + t] + krow(1, 1, 1) * h_1[t] + krow(1, 2, 1) * h_0[t] for t in range(2)),
    )
    up = [
        up0[t] + right_shift(up0[t] + up1[t], lane_col(q0l[t], r0) + lane_col(q1l[t], r1)) for t in range(2)
    ]

    hb_0 = [left_shift(raw[BH + t], lane_col(fld(rt, RH + t), e0)) for t in range(2)]
    hb_1 = [left_shift(raw[BH1 + t], lane_col(fld(rt, RH + t), e1)) for t in range(2)]
    ub_1 = [left_shift(raw[BU01 + t], lane_col(fld(rt, RU0 + t), e1)) for t in range(2)]
    dn1 = section_sums(
        af_row(k, f, 1, end) + raw[BU1] - raw[BU2] - ub_1[0],
        raw[BU1T] - raw[BU2T] - ub_1[1],
        *(krow(1, 0, end) * raw[BH + t] + krow(1, 1, end) * hb_0[t] + krow(1, 2, end) * hb_1[t] for t in range(2)),
    )
    dn0 = section_sums(
        af_row(k, f, 0, end - 1) + raw[BU01] - raw[BU11] + raw[BU2],
        raw[BU01T] - raw[BU11T] + raw[BU2T],
        *(
            krow(0, 0, end - 1) * raw[BH1 + t] + krow(0, 1, end - 1) * raw[BH + t] + krow(0, 2, end - 1) * hb_1[t]
            for t in range(2)
        ),
    )
    down = [
        left_shift(dn1[t] + dn0[t], lane_col(q1r[t], e0) + lane_col(q0r[t], e1)) + dn1[t] for t in range(2)
    ]

    def store(msg_up, msg_down):
        for msg, sums, parts, geo, r in (
            (msg_up, up, (TH, THT, TU1, TU1T, TU2, TU2T, TE2), 1, 0),
            (msg_down, down, (BH, BHT, BU0, BU0T, BU1, BU1T, BE0), 0, end),
        ):
            for n in range(2):
                msg[LV * n : LV * n + LV, :] = sums[n]
            for n, part in enumerate(parts):
                msg[LV * (n + 2) : LV * (n + 3), :] = raw[part]
            for n in range(3):
                msg[72 + n : 73 + n, :] = krow(geo, n, r)
            msg[75:76, :] = af_row(k, f, geo, r)
            msg[76:77, 0:128] = left[r : r + 1, :]
            msg[76:77, 128:256] = right[r : r + 1, :]

    @pl.when(odd_y)
    def _():
        store(msg_a, msg_b)

    @pl.when(jnp.logical_not(odd_y))
    def _():
        store(msg_b, msg_a)


(
    WHB, WHBT, WUB, WUBT, WHA, WHAT, WUA, WUAT,
    WQB, WQBT, WQA, WQAT, WMA, WMAT, WMB, WMBT, WEB, WEA,
) = range(18)
(CY, CYT, CQ, CZ, CP, CPT) = range(6)


def main_kernel(
    v, h, vt, ht, d, el, area, k, f, slab_a, slab_b, own0, raw, msg_a, msg_b,
    vertex, kinetic, cell, edge, ext, msgs, halo, geo,
):
    odd_x = lax.rem(lax.axis_index("px"), 2) == 1
    odd_y = lax.rem(lax.axis_index("py"), 2) == 1
    rows, cols = h.shape[1], h.shape[2]
    end = rows - 1

    @pl.when(odd_y)
    def _():
        msgs[0] = msg_b[...]
        msgs[1] = msg_a[...]

    @pl.when(jnp.logical_not(odd_y))
    def _():
        msgs[0] = msg_a[...]
        msgs[1] = msg_b[...]

    above = lambda n: msgs[0, LV * n : LV * n + LV, :]
    below = lambda n: msgs[1, LV * n : LV * n + LV, :]
    ka = [msgs[0, 72 + n : 73 + n, :] for n in range(4)]
    kb = [msgs[1, 72 + n : 73 + n, :] for n in range(4)]

    left = jnp.where(odd_x, slab_a[...], slab_b[...])
    right = jnp.where(odd_x, slab_b[...], slab_a[...])
    ext[0, BASE : BASE + rows, :] = left
    ext[1, BASE : BASE + rows, :] = right
    ext[2, BASE : BASE + rows, :] = own0[...]
    ext[0, DNB : DNB + 1, :] = msgs[0, 76:77, 0:128]
    ext[1, DNB : DNB + 1, :] = msgs[0, 76:77, 128:256]
    ext[1, UPB : UPB + 1, :] = msgs[1, 76:77, 128:256]
    lt, rt, ot = (jnp.transpose(ext[n]) for n in range(3))
    lanes = iota((LV, 128), 1)
    low = lambda x, row: jnp.where(lanes == UPB, row[:, 0:1], x)
    high = lambda x, row: jnp.where(lanes == DNB, row[:, 0:1], x)
    h0 = [high(low(fld(ot, RH + t), below(2 + t)), above(2 + t)) for t in range(2)]
    u00 = [low(fld(ot, RU0 + t), below(4 + t)) for t in range(2)]
    q0l, q1l = column_left(lt, *h0, *u00)
    q0r, q1r = column_right(rt)
    up = lambda x: pltpu.roll(x, 127, 1)
    dn = lambda x: pltpu.roll(x, 1, 1)
    z = fld(lt, LE1) + up(fld(lt, LE2))
    cols_out = [
        q0l[0] + q1l[0] + up(q1l[0]),
        q0l[1] + q1l[1] + up(q1l[1]),
        up(q1l[0]),
        z,
        q0r[0] + q1r[0] + dn(q0r[0]),
        q0r[1] + q1r[1] + dn(q0r[1]),
    ]
    packed = jnp.concatenate(cols_out + [jnp.zeros((128 - LV * len(cols_out), 128), F32)], axis=0)
    inject = jnp.transpose(packed)[BASE : BASE + rows, :]

    hb1 = [left_shift(below(2 + t), lane_col(fld(rt, RH + t), UPB)) for t in range(2)]
    ub1 = [left_shift(below(4 + t), lane_col(fld(rt, RU0 + t), UPB)) for t in range(2)]
    qb = section_sums(
        kb[3] + below(4) - below(6) + raw[TU2],
        below(5) - below(7) + raw[TU2T],
        *(kb[0] * below(2 + t) + kb[1] * raw[TH + t] + kb[2] * hb1[t] for t in range(2)),
    )
    ha1 = [left_shift(above(2 + t), lane_col(fld(rt, RH + t), DNB)) for t in range(2)]
    he1 = [left_shift(raw[BH + t], lane_col(fld(rt, RH + t), BASE + end)) for t in range(2)]
    ue1 = [left_shift(raw[BU0 + t], lane_col(fld(rt, RU0 + t), BASE + end)) for t in range(2)]
    qa = section_sums(
        ka[3] + above(4) - above(6) - ue1[0],
        above(5) - above(7) - ue1[1],
        *(ka[0] * above(2 + t) + ka[1] * ha1[t] + ka[2] * he1[t] for t in range(2)),
    )
    for t in range(2):
        halo[WHB + t] = hb1[t]
        halo[WUB + t] = ub1[t]
        halo[WHA + t] = above(2 + t)
        halo[WUA + t] = above(6 + t)
        halo[WQB + t] = qb[t]
        halo[WQA + t] = qa[t]
        halo[WMA + t] = above(t) + qa[t] + right_shift(qa[t], lane_col(q1l[t], DNB))
        halo[WMB + t] = below(t) + qb[t] + left_shift(qb[t], lane_col(q0r[t], UPB))
    halo[WEB] = below(8)
    halo[WEA] = above(8)

    for a in range(2):
        geo[a] = (k[a, 0] + k[a, 1] + k[a, 2]) * f[a]
    for e in range(3):
        geo[2 + e] = (1.0 / 12.0) / d[e]
        geo[5 + e] = 0.25 * d[e] * el[e]
    geo[8] = 1.0 / area[...]

    for lev in range(LV):
        row = lambda n, lev=lev: halo[n, lev : lev + 1, :]
        col = lambda n, lev=lev: inject[:, LV * n + lev : LV * n + lev + 1]
        rcol = lambda n, lev=lev: right[:, LV * n + lev : LV * n + lev + 1]
        hh = [x[lev] for x in (h, ht)]
        u = [[d[e] * x[e, lev] for x in (v, vt)] for e in range(3)]
        h1 = [left_shift(hh[t], rcol(RH + t)) for t in range(2)]
        u01 = [left_shift(u[0][t], rcol(RU0 + t)) for t in range(2)]
        n0 = [u[0][t] - u[1][t] + row_up(u[2][t], row(WUA + t)) for t in range(2)]
        n1 = [u[1][t] - u[2][t] - row_down(u01[t], row(WUB + t)) for t in range(2)]
        d0 = [k[0, 0] * hh[t] + k[0, 1] * row_up(hh[t], row(WHA + t)) + k[0, 2] * h1[t] for t in range(2)]
        d1 = [k[1, 0] * hh[t] + k[1, 1] * h1[t] + k[1, 2] * row_down(h1[t], row(WHB + t)) for t in range(2)]
        q0 = section_sums(geo[0] + n0[0], n0[1], *d0)
        q1 = section_sums(geo[1] + n1[0], n1[1], *d1)
        vertex[0, lev] = q0[0]
        vertex[1, lev] = q1[0]
        grads = []
        for t in range(2):
            q0d = row_down(q0[t], row(WQB + t))
            q1u = row_up(q1[t], row(WQA + t))
            both = q0[t] + q1[t]
            p, y = both + q0d, both + q1u
            m = p + right_shift(y, col(CY + t))
            m1 = left_shift(p, col(CP + t)) + y
            grads.append(
                (
                    row_up(m, row(WMA + t) + q0[t]) - m,
                    m1 - m,
                    row_down(m1, row(WMB + t) + q1[t]) - m,
                )
            )
            if t == 0:
                cell[lev] = m * (1.0 / 6.0)
                means = (q0[0] + right_shift(q1u, col(CQ)), both, q1[0] + q0d)
        for e in range(3):
            edge[e, lev] = 0.5 * means[e] - geo[2 + e] * (v[e, lev] * grads[0][e] + vt[e, lev] * grads[1][e])
        en = [energy(geo[5 + e], v[e, lev], vt[e, lev]) for e in range(3)]
        zz = en[1] + row_up(en[2], row(WEA))
        kinetic[lev] = (
            en[0] + en[1] + en[2] + row_down(en[0], row(WEB)) + right_shift(zz, col(CZ))
        ) * geo[8]


def swap(x, axis, start):
    n = lax.axis_size(axis)
    pairs = []
    for i in range(start, n + start, 2):
        a, b = i % n, (i + 1) % n
        pairs += [(a, b), (b, a)]
    return lax.ppermute(x, axis, pairs)


def call(kernel, outs, scratch, *args):
    vmem = pl.BlockSpec(memory_space=pltpu.VMEM)
    return pl.pallas_call(
        kernel,
        out_shape=[jax.ShapeDtypeStruct(s, F32) for s in outs],
        in_specs=[vmem] * len(args),
        out_specs=[vmem] * len(outs),
        scratch_shapes=[pltpu.VMEM(s, F32) for s in scratch],
    )(*args)


def local(v, h, vt, ht, d, el, area, k, f):
    levels, rows, cols = h.shape
    slab = (rows, 128)
    send_a, send_b, own0, raw = call(
        pack_kernel, [slab, slab, slab, (RAW, levels, cols)], [], v, h, vt, ht, d, el, k, f
    )
    slab_a = swap(send_a, "px", 0)
    slab_b = swap(send_b, "px", 1)
    msg_a, msg_b = call(
        merge_kernel, [(80, cols), (80, cols)], [(3, 128, 128)], slab_a, slab_b, own0, raw, k, f
    )
    msg_a = swap(msg_a, "py", 0)
    msg_b = swap(msg_b, "py", 1)
    return tuple(
        call(
            main_kernel,
            [(2, levels, rows, cols), (levels, rows, cols), (levels, rows, cols), (3, levels, rows, cols)],
            [(3, 128, 128), (2, 80, cols), (18, levels, cols), (9, rows, cols)],
            v, h, vt, ht, d, el, area, k, f, slab_a, slab_b, own0, raw, msg_a, msg_b,
        )
    )


def solution(mesh):
    field = P(None, "py", "px")
    pair = P(None, None, "py", "px")
    return jax.shard_map(
        local,
        mesh=mesh,
        in_specs=(pair, field, pair, field, field, field, P("py", "px"), pair, field),
        out_specs=(pair, field, field, pair),
        check_vma=False,
    )
```

```python
import jax
import jax.numpy as jnp
from jax import lax
from jax.experimental import pallas as pl
from jax.experimental.pallas import tpu as pltpu
from jax.sharding import PartitionSpec as P

F32 = jnp.float32
LV = 8
BASE = 8
UPB, DNB = BASE - 1, BASE + 32


def iota(shape, dim):
    return lax.broadcasted_iota(jnp.int32, shape, dim)


def left_shift(x, col):
    n = x.shape[1]
    return jnp.where(iota(x.shape, 1) == n - 1, col, pltpu.roll(x, n - 1, 1))


def right_shift(x, col):
    return jnp.where(iota(x.shape, 1) == 0, col, pltpu.roll(x, 1, 1))


def row_up(x, row):
    n = x.shape[0]
    return jnp.where(iota(x.shape, 0) == n - 1, row, pltpu.roll(x, n - 1, 0))


def row_down(x, row):
    return jnp.where(iota(x.shape, 0) == 0, row, pltpu.roll(x, 1, 0))


def section_sums(n0, dn, d0, dd):
    n1, d1 = n0 + dn, d0 + dd
    ns, ds = n0 + n1, d0 + d1
    ends = d0 * d1
    inv = 1.0 / (ends * ds)
    half = ns * ends * inv
    side = ds * inv
    last = n1 * d0 * side
    first = n0 * d1 * side
    return (first + last) * (1.0 / 6.0) + half * (2.0 / 3.0), half * (1.0 / 3.0) + last * (1.0 / 6.0)


def energy(w, v, vt):
    return w * (v * v + v * vt + vt * vt * (1.0 / 3.0))


(RH, RHT, RU0, RU0T, RU1, RU1T, RU2, RU2T, RH1, RH1T, RU01, RU01T) = range(12)
RGEO = 96
(LH, LHT, LU0, LU0T, LU1, LU1T, LU2, LU2T, LE1, LE2) = range(10)
LGEO = 80
(TH, THT, TH1, TH1T, TU0, TU0T, TU1, TU1T, TU11, TU11T, TU2, TU2T, TU21, TU21T, TE2) = range(15)
(BH, BHT, BH1, BH1T, BU0, BU0T, BU01, BU01T, BU1, BU1T, BU11, BU11T, BU2, BU2T, BE0) = range(15, 30)
RAW = 30


def pack_kernel(
    v, h, vt, ht, d, el, area, k, f, send_a, send_b, own0, vo, ho, vto, hto, do, eo, ao, ko, fo, sems
):
    odd = lax.rem(lax.axis_index("px"), 2) == 1
    rows, cols = h.shape[1], h.shape[2]
    half = cols - 128
    started = []

    def start(src, dst):
        copy = pltpu.make_async_copy(src, dst, sems.at[len(started)])
        copy.start()
        started.append(copy)
        return copy

    fixed = [start(x, y) for x, y in ((d, do), (el, eo), (k, ko), (f, fo))]
    by_level = [
        [start(x.at[lev], y.at[lev]) for x, y in ((h, ho), (ht, hto))]
        + [start(x.at[:, lev], y.at[:, lev]) for x, y in ((v, vo), (vt, vto))]
        for lev in range(LV)
    ]
    area_copy = start(area, ao)
    for copy in fixed:
        copy.wait()

    lanes = iota((rows, 128), 1)
    to_left = jnp.zeros((rows, 128), F32)
    to_right = jnp.zeros((rows, 128), F32)
    geo_low = [ko[a, b, :, 0:128] for a in range(2) for b in range(3)]
    geo_high = [ko[a, b, :, half:cols] for a in range(2) for b in range(3)]
    for a in range(2):
        geo_low.append((geo_low[3 * a] + geo_low[3 * a + 1] + geo_low[3 * a + 2]) * fo[a, :, 0:128])
        geo_high.append((geo_high[3 * a] + geo_high[3 * a + 1] + geo_high[3 * a + 2]) * fo[a, :, half:cols])
    for n in range(8):
        to_left = jnp.where(lanes == RGEO + n, geo_low[n][:, 0:1], to_left)
        to_right = jnp.where(lanes == LGEO + n, geo_high[n][:, 127:128], to_right)
    first = [do[e, :, 0:128] for e in range(3)]
    last = [do[e, :, half:cols] for e in range(3)]
    weight = [0.25 * last[e] * eo[e, :, half:cols] for e in range(3)]
    for lev in range(LV):
        for copy in by_level[lev]:
            copy.wait()
        low = [(ho[lev, :, 0:128], 0), (hto[lev, :, 0:128], 0)]
        high = [ho[lev, :, half:cols], hto[lev, :, half:cols]]
        for e in range(3):
            for x in (vo, vto):
                low.append((first[e] * x[e, lev, :, 0:128], 0))
                high.append(last[e] * x[e, lev, :, half:cols])
        low += [(x, 1) for x, _ in low[:4]]
        for e in (1, 2):
            high.append(energy(weight[e], vo[e, lev, :, half:cols], vto[e, lev, :, half:cols]))
        for n, (x, c) in enumerate(low):
            to_left = jnp.where(lanes == LV * n + lev, x[:, c : c + 1], to_left)
        for n, x in enumerate(high):
            to_right = jnp.where(lanes == LV * n + lev, x[:, 127:128], to_right)
    send_a[...] = jnp.where(odd, to_left, to_right)
    send_b[...] = jnp.where(odd, to_right, to_left)
    own0[...] = to_left
    area_copy.wait()


PACK_COPIES = 4 + 4 * LV + 1


def prep_kernel(v, h, vt, ht, d, el, area, k, f, raw, geo):
    end = h.shape[1] - 1
    for x, n in ((h, TH), (ht, THT)):
        raw[n] = x[:, 0, :]
        raw[n + 2] = x[:, 1, :]
    for x, n in ((h, BH), (ht, BHT)):
        raw[n] = x[:, end, :]
        raw[n + 2] = x[:, end - 1, :]
    for x, t in ((v, 0), (vt, 1)):
        for e, r, n in (
            (0, 0, TU0),
            (1, 0, TU1),
            (1, 1, TU11),
            (2, 0, TU2),
            (2, 1, TU21),
            (0, end, BU0),
            (0, end - 1, BU01),
            (1, end, BU1),
            (1, end - 1, BU11),
            (2, end, BU2),
        ):
            raw[n + t] = d[e, r : r + 1, :] * x[e, :, r, :]
    raw[TE2] = energy(0.25 * d[2, 0:1, :] * el[2, 0:1, :], v[2, :, 0, :], vt[2, :, 0, :])
    raw[BE0] = energy(0.25 * d[0, end : end + 1, :] * el[0, end : end + 1, :], v[0, :, end, :], vt[0, :, end, :])
    for a in range(2):
        geo[a] = (k[a, 0] + k[a, 1] + k[a, 2]) * f[a]
    for e in range(3):
        geo[2 + e] = (1.0 / 12.0) / d[e]
        geo[5 + e] = 0.25 * d[e] * el[e]
    geo[8] = 1.0 / area[...]


def af_row(k, f, a, r):
    return (k[a, 0, r : r + 1, :] + k[a, 1, r : r + 1, :] + k[a, 2, r : r + 1, :]) * f[a, r : r + 1, :]


def fld(t, n):
    return t[LV * n : LV * n + LV, :]


def column_left(lt, h0, h0t, u00, u00t):
    k = [lt[LGEO + n : LGEO + n + 1, :] for n in range(8)]
    up = lambda x: pltpu.roll(x, 127, 1)
    dn = lambda x: pltpu.roll(x, 1, 1)
    h, hp, u0, u0p, u1, u1p, u2, u2p = (fld(lt, n) for n in range(8))
    q0 = section_sums(
        k[6] + u0 - u1 + up(u2),
        u0p - u1p + up(u2p),
        k[0] * h + k[1] * up(h) + k[2] * h0,
        k[0] * hp + k[1] * up(hp) + k[2] * h0t,
    )
    q1 = section_sums(
        k[7] + u1 - u2 - dn(u00),
        u1p - u2p - dn(u00t),
        k[3] * h + k[4] * h0 + k[5] * dn(h0),
        k[3] * hp + k[4] * h0t + k[5] * dn(h0t),
    )
    return q0, q1


def column_right(rt):
    k = [rt[RGEO + n : RGEO + n + 1, :] for n in range(8)]
    up = lambda x: pltpu.roll(x, 127, 1)
    dn = lambda x: pltpu.roll(x, 1, 1)
    h, hp, u0, u0p, u1, u1p, u2, u2p, h1, h1p, u01, u01p = (fld(rt, n) for n in range(12))
    q0 = section_sums(
        k[6] + u0 - u1 + up(u2),
        u0p - u1p + up(u2p),
        k[0] * h + k[1] * up(h) + k[2] * h1,
        k[0] * hp + k[1] * up(hp) + k[2] * h1p,
    )
    q1 = section_sums(
        k[7] + u1 - u2 - dn(u01),
        u1p - u2p - dn(u01p),
        k[3] * h + k[4] * h1 + k[5] * dn(h1),
        k[3] * hp + k[4] * h1p + k[5] * dn(h1p),
    )
    return q0, q1


def lane_col(x, lane):
    return x[:, lane : lane + 1]


def merge_kernel(slab_a, slab_b, own0, raw, k, f, msg_a, msg_b, ext):
    odd_x = lax.rem(lax.axis_index("px"), 2) == 1
    odd_y = lax.rem(lax.axis_index("py"), 2) == 1
    rows = slab_a.shape[0]
    end = rows - 1
    left = jnp.where(odd_x, slab_a[...], slab_b[...])
    right = jnp.where(odd_x, slab_b[...], slab_a[...])
    ext[0, BASE : BASE + rows, :] = left
    ext[1, BASE : BASE + rows, :] = right
    ext[2, BASE : BASE + rows, :] = own0[...]
    lt, rt, ot = (jnp.transpose(ext[n]) for n in range(3))
    q0l, q1l = column_left(lt, fld(ot, RH), fld(ot, RHT), fld(ot, RU0), fld(ot, RU0T))
    q0r, q1r = column_right(rt)
    r0, r1 = BASE, BASE + 1
    e0, e1 = BASE + end, BASE + end - 1
    krow = lambda a, b, r: k[a, b, r : r + 1, :]

    h_0 = [left_shift(raw[TH + t], lane_col(fld(rt, RH + t), r0)) for t in range(2)]
    h_1 = [left_shift(raw[TH1 + t], lane_col(fld(rt, RH + t), r1)) for t in range(2)]
    u_0 = [left_shift(raw[TU0 + t], lane_col(fld(rt, RU0 + t), r0)) for t in range(2)]
    up0 = section_sums(
        af_row(k, f, 0, 0) + raw[TU0] - raw[TU1] + raw[TU21],
        raw[TU0T] - raw[TU1T] + raw[TU21T],
        *(krow(0, 0, 0) * raw[TH + t] + krow(0, 1, 0) * raw[TH1 + t] + krow(0, 2, 0) * h_0[t] for t in range(2)),
    )
    up1 = section_sums(
        af_row(k, f, 1, 1) + raw[TU11] - raw[TU21] - u_0[0],
        raw[TU11T] - raw[TU21T] - u_0[1],
        *(krow(1, 0, 1) * raw[TH1 + t] + krow(1, 1, 1) * h_1[t] + krow(1, 2, 1) * h_0[t] for t in range(2)),
    )
    up = [
        up0[t] + right_shift(up0[t] + up1[t], lane_col(q0l[t], r0) + lane_col(q1l[t], r1)) for t in range(2)
    ]

    hb_0 = [left_shift(raw[BH + t], lane_col(fld(rt, RH + t), e0)) for t in range(2)]
    hb_1 = [left_shift(raw[BH1 + t], lane_col(fld(rt, RH + t), e1)) for t in range(2)]
    ub_1 = [left_shift(raw[BU01 + t], lane_col(fld(rt, RU0 + t), e1)) for t in range(2)]
    dn1 = section_sums(
        af_row(k, f, 1, end) + raw[BU1] - raw[BU2] - ub_1[0],
        raw[BU1T] - raw[BU2T] - ub_1[1],
        *(krow(1, 0, end) * raw[BH + t] + krow(1, 1, end) * hb_0[t] + krow(1, 2, end) * hb_1[t] for t in range(2)),
    )
    dn0 = section_sums(
        af_row(k, f, 0, end - 1) + raw[BU01] - raw[BU11] + raw[BU2],
        raw[BU01T] - raw[BU11T] + raw[BU2T],
        *(
            krow(0, 0, end - 1) * raw[BH1 + t] + krow(0, 1, end - 1) * raw[BH + t] + krow(0, 2, end - 1) * hb_1[t]
            for t in range(2)
        ),
    )
    down = [
        left_shift(dn1[t] + dn0[t], lane_col(q1r[t], e0) + lane_col(q0r[t], e1)) + dn1[t] for t in range(2)
    ]

    def store(msg_up, msg_down):
        for msg, sums, parts, geo, r in (
            (msg_up, up, (TH, THT, TU1, TU1T, TU2, TU2T, TE2), 1, 0),
            (msg_down, down, (BH, BHT, BU0, BU0T, BU1, BU1T, BE0), 0, end),
        ):
            for n in range(2):
                msg[LV * n : LV * n + LV, :] = sums[n]
            for n, part in enumerate(parts):
                msg[LV * (n + 2) : LV * (n + 3), :] = raw[part]
            for n in range(3):
                msg[72 + n : 73 + n, :] = krow(geo, n, r)
            msg[75:76, :] = af_row(k, f, geo, r)
            msg[76:77, 0:128] = left[r : r + 1, :]
            msg[76:77, 128:256] = right[r : r + 1, :]

    @pl.when(odd_y)
    def _():
        store(msg_a, msg_b)

    @pl.when(jnp.logical_not(odd_y))
    def _():
        store(msg_b, msg_a)


(WQB, WQBT, WQA, WQAT, WMA, WMAT, WMB, WMBT, WE0, WE0T, WF1, WF1T, WEB, WEA) = range(14)
(CY, CYT, CQ, CP, CPT) = range(5)


def vertex_kernel(v, h, vt, ht, d, k, geo, slab_a, slab_b, q, kin):
    odd_x = lax.rem(lax.axis_index("px"), 2) == 1
    left = jnp.where(odd_x, slab_a[...], slab_b[...])
    right = jnp.where(odd_x, slab_b[...], slab_a[...])
    z = left + row_up(pltpu.roll(left, 128 - LV, 1), 0.0)
    for lev in range(LV):
        rcol = lambda n, lev=lev: right[:, LV * n + lev : LV * n + lev + 1]
        hh = [x[lev] for x in (h, ht)]
        u = [[d[e] * x[e, lev] for x in (v, vt)] for e in range(3)]
        h1 = [left_shift(hh[t], rcol(RH + t)) for t in range(2)]
        u01 = [left_shift(u[0][t], rcol(RU0 + t)) for t in range(2)]
        up = lambda x: pltpu.roll(x, x.shape[0] - 1, 0)
        dn = lambda x: pltpu.roll(x, 1, 0)
        n0 = [u[0][t] - u[1][t] + up(u[2][t]) for t in range(2)]
        n1 = [u[1][t] - u[2][t] - dn(u01[t]) for t in range(2)]
        d0 = [k[0, 0] * hh[t] + k[0, 1] * up(hh[t]) + k[0, 2] * h1[t] for t in range(2)]
        d1 = [k[1, 0] * hh[t] + k[1, 1] * h1[t] + k[1, 2] * dn(h1[t]) for t in range(2)]
        q0 = section_sums(geo[0] + n0[0], n0[1], *d0)
        q1 = section_sums(geo[1] + n1[0], n1[1], *d1)
        for t in range(2):
            q[t, 0, lev] = q0[t]
            q[t, 1, lev] = q1[t]
        en = [energy(geo[5 + e], v[e, lev], vt[e, lev]) for e in range(3)]
        zz = en[1] + row_up(en[2], 0.0)
        zcol = z[:, LV * LE1 + lev : LV * LE1 + lev + 1]
        kin[lev] = en[0] + en[1] + en[2] + row_down(en[0], 0.0) + right_shift(zz, zcol)


def last_kernel(
    v, vt, k, f, geo, slab_a, slab_b, own0, raw, q, kin, msg_a, msg_b,
    vertex, kinetic, cell, edge, ext, msgs, halo, vertex_v, kinetic_v, cell_v, edge_v, sems,
):
    odd_x = lax.rem(lax.axis_index("px"), 2) == 1
    odd_y = lax.rem(lax.axis_index("py"), 2) == 1
    rows = kin.shape[1]
    end = rows - 1

    @pl.when(odd_y)
    def _():
        msgs[0] = msg_b[...]
        msgs[1] = msg_a[...]

    @pl.when(jnp.logical_not(odd_y))
    def _():
        msgs[0] = msg_a[...]
        msgs[1] = msg_b[...]

    above = lambda n: msgs[0, LV * n : LV * n + LV, :]
    below = lambda n: msgs[1, LV * n : LV * n + LV, :]
    ka = [msgs[0, 72 + n : 73 + n, :] for n in range(4)]
    kb = [msgs[1, 72 + n : 73 + n, :] for n in range(4)]
    krow = lambda a, b, r: k[a, b, r : r + 1, :]

    left = jnp.where(odd_x, slab_a[...], slab_b[...])
    right = jnp.where(odd_x, slab_b[...], slab_a[...])
    ext[0, BASE : BASE + rows, :] = left
    ext[1, BASE : BASE + rows, :] = right
    ext[2, BASE : BASE + rows, :] = own0[...]
    ext[0, DNB : DNB + 1, :] = msgs[0, 76:77, 0:128]
    ext[1, DNB : DNB + 1, :] = msgs[0, 76:77, 128:256]
    ext[1, UPB : UPB + 1, :] = msgs[1, 76:77, 128:256]
    lt, rt, ot = (jnp.transpose(ext[n]) for n in range(3))
    lanes = iota((LV, 128), 1)
    low = lambda x, row: jnp.where(lanes == UPB, row[:, 0:1], x)
    high = lambda x, row: jnp.where(lanes == DNB, row[:, 0:1], x)
    h0 = [high(low(fld(ot, RH + t), below(2 + t)), above(2 + t)) for t in range(2)]
    u00 = [low(fld(ot, RU0 + t), below(4 + t)) for t in range(2)]
    q0l, q1l = column_left(lt, *h0, *u00)
    q0r, q1r = column_right(rt)
    up = lambda x: pltpu.roll(x, 127, 1)
    dn = lambda x: pltpu.roll(x, 1, 1)
    cols_out = [
        q0l[0] + q1l[0] + up(q1l[0]),
        q0l[1] + q1l[1] + up(q1l[1]),
        up(q1l[0]),
        q0r[0] + q1r[0] + dn(q0r[0]),
        q0r[1] + q1r[1] + dn(q0r[1]),
    ]
    packed = jnp.concatenate(cols_out + [jnp.zeros((128 - LV * len(cols_out), 128), F32)], axis=0)
    inject = jnp.transpose(packed)[BASE : BASE + rows, :]

    hb1 = [left_shift(below(2 + t), lane_col(fld(rt, RH + t), UPB)) for t in range(2)]
    ub1 = [left_shift(below(4 + t), lane_col(fld(rt, RU0 + t), UPB)) for t in range(2)]
    h01 = [left_shift(raw[TH + t], lane_col(fld(rt, RH + t), BASE)) for t in range(2)]
    qb = section_sums(
        kb[3] + below(4) - below(6) + raw[TU2],
        below(5) - below(7) + raw[TU2T],
        *(kb[0] * below(2 + t) + kb[1] * raw[TH + t] + kb[2] * hb1[t] for t in range(2)),
    )
    q1f = section_sums(
        af_row(k, f, 1, 0) + raw[TU1] - raw[TU2] - ub1[0],
        raw[TU1T] - raw[TU2T] - ub1[1],
        *(krow(1, 0, 0) * raw[TH + t] + krow(1, 1, 0) * h01[t] + krow(1, 2, 0) * hb1[t] for t in range(2)),
    )
    ha1 = [left_shift(above(2 + t), lane_col(fld(rt, RH + t), DNB)) for t in range(2)]
    he1 = [left_shift(raw[BH + t], lane_col(fld(rt, RH + t), BASE + end)) for t in range(2)]
    ue1 = [left_shift(raw[BU0 + t], lane_col(fld(rt, RU0 + t), BASE + end)) for t in range(2)]
    qa = section_sums(
        ka[3] + above(4) - above(6) - ue1[0],
        above(5) - above(7) - ue1[1],
        *(ka[0] * above(2 + t) + ka[1] * ha1[t] + ka[2] * he1[t] for t in range(2)),
    )
    q0e = section_sums(
        af_row(k, f, 0, end) + raw[BU0] - raw[BU1] + above(6),
        raw[BU0T] - raw[BU1T] + above(7),
        *(krow(0, 0, end) * raw[BH + t] + krow(0, 1, end) * above(2 + t) + krow(0, 2, end) * he1[t] for t in range(2)),
    )
    for t in range(2):
        halo[WQB + t] = qb[t]
        halo[WQA + t] = qa[t]
        halo[WMA + t] = above(t) + qa[t] + right_shift(qa[t], lane_col(q1l[t], DNB)) + q0e[t]
        halo[WMB + t] = below(t) + qb[t] + left_shift(qb[t], lane_col(q0r[t], UPB)) + q1f[t]
        halo[WE0 + t] = q0e[t]
        halo[WF1 + t] = q1f[t]
    halo[WEB] = below(8)
    halo[WEA] = right_shift(above(8), lane_col(fld(lt, LE2), DNB))

    copies = []
    for lev in range(LV):
        row = lambda n, lev=lev: halo[n, lev : lev + 1, :]
        col = lambda n, lev=lev: inject[:, LV * n + lev : LV * n + lev + 1]
        spot = iota(kin.shape[1:], 0)
        grads = []
        for t in range(2):
            q0 = jnp.where(spot == end, row(WE0 + t), q[t, 0, lev])
            q1 = jnp.where(spot == 0, row(WF1 + t), q[t, 1, lev])
            q0d = row_down(q0, row(WQB + t))
            q1u = row_up(q1, row(WQA + t))
            both = q0 + q1
            p, y = both + q0d, both + q1u
            m = p + right_shift(y, col(CY + t))
            m1 = left_shift(p, col(CP + t)) + y
            grads.append((row_up(m, row(WMA + t)) - m, m1 - m, row_down(m1, row(WMB + t)) - m))
            if t == 0:
                cell_v[lev] = m * (1.0 / 6.0)
                vertex_v[0, lev] = q0
                vertex_v[1, lev] = q1
                means = (q0 + right_shift(q1u, col(CQ)), both, q1 + q0d)
        for e in range(3):
            edge_v[e, lev] = 0.5 * means[e] - geo[2 + e] * (v[e, lev] * grads[0][e] + vt[e, lev] * grads[1][e])
        rim = jnp.where(spot == 0, row(WEB), 0.0) + jnp.where(spot == end, row(WEA), 0.0)
        kinetic_v[lev] = (kin[lev] + rim) * geo[8]
        for n, (src, dst) in enumerate(
            (
                (vertex_v.at[:, lev], vertex.at[:, lev]),
                (kinetic_v.at[lev], kinetic.at[lev]),
                (cell_v.at[lev], cell.at[lev]),
                (edge_v.at[:, lev], edge.at[:, lev]),
            )
        ):
            copy = pltpu.make_async_copy(src, dst, sems.at[4 * lev + n])
            copy.start()
            copies.append(copy)
    for copy in copies:
        copy.wait()


def swap(x, axis, start):
    n = lax.axis_size(axis)
    pairs = []
    for i in range(start, n + start, 2):
        a, b = i % n, (i + 1) % n
        pairs += [(a, b), (b, a)]
    return lax.ppermute(x, axis, pairs)


VM = pl.BlockSpec(memory_space=pltpu.VMEM)
ANY = pl.BlockSpec(memory_space=pl.ANY)


def call(kernel, args, outs, scratch=(), sems=0, hbm_in=False, hbm_out=False, flops=0):
    args = [pltpu.with_memory_space_constraint(x, pltpu.HBM if hbm_in else pltpu.VMEM) for x in args]
    shape = (lambda s: jax.ShapeDtypeStruct(s, F32)) if hbm_out else (lambda s: pltpu.VMEM(s, F32))
    return pl.pallas_call(
        kernel,
        out_shape=[shape(s) for s in outs],
        in_specs=[ANY if hbm_in else VM] * len(args),
        out_specs=[ANY if hbm_out else VM] * len(outs),
        scratch_shapes=[pltpu.VMEM(s, F32) for s in scratch]
        + ([pltpu.SemaphoreType.DMA((sems,))] if sems else []),
        compiler_params=pltpu.CompilerParams(vmem_limit_bytes=16 * 2**20),
        cost_estimate=pl.CostEstimate(flops=flops, transcendentals=0, bytes_accessed=0) if flops else None,
    )(*args)


def local(*args):
    levels, rows, cols = args[1].shape
    slab = (rows, 128)
    send_a, send_b, own0, *held = call(
        pack_kernel, args, [slab, slab, slab] + [x.shape for x in args], sems=PACK_COPIES, hbm_in=True
    )
    v, h, vt, ht, d, el, area, k, f = held
    slab_a = swap(send_a, "px", 0)
    slab_b = swap(send_b, "px", 1)
    raw, geo = call(prep_kernel, held, [(RAW, levels, cols), (9, rows, cols)], flops=20_000_000)
    msg_a, msg_b = call(
        merge_kernel, [slab_a, slab_b, own0, raw, k, f], [(80, cols), (80, cols)], [(3, 128, 128)]
    )
    msg_a = swap(msg_a, "py", 0)
    msg_b = swap(msg_b, "py", 1)
    q, kin = call(
        vertex_kernel,
        [v, h, vt, ht, d, k, geo, slab_a, slab_b],
        [(2, 2, levels, rows, cols), (levels, rows, cols)],
        flops=40_000_000,
    )
    return tuple(
        call(
            last_kernel,
            [v, vt, k, f, geo, slab_a, slab_b, own0, raw, q, kin, msg_a, msg_b],
            [(2, levels, rows, cols), (levels, rows, cols), (levels, rows, cols), (3, levels, rows, cols)],
            [
                (3, 128, 128), (2, 80, cols), (14, levels, cols),
                (2, levels, rows, cols), (levels, rows, cols), (levels, rows, cols), (3, levels, rows, cols),
            ],
            sems=4 * LV,
            hbm_out=True,
        )
    )


def solution(mesh):
    field = P(None, "py", "px")
    pair = P(None, None, "py", "px")
    return jax.shard_map(
        local,
        mesh=mesh,
        in_specs=(pair, field, pair, field, field, field, P("py", "px"), pair, field),
        out_specs=(pair, field, field, pair),
        check_vma=False,
    )
```

```python
import jax
import jax.numpy as jnp
from jax import lax
from jax.experimental import pallas as pl
from jax.experimental.pallas import tpu as pltpu
from jax.sharding import PartitionSpec as P

F32 = jnp.float32
LV = 8
BASE = 8
UPB, DNB = BASE - 1, BASE + 32


def iota(shape, dim):
    return lax.broadcasted_iota(jnp.int32, shape, dim)


def left_shift(x, col):
    n = x.shape[1]
    return jnp.where(iota(x.shape, 1) == n - 1, col, pltpu.roll(x, n - 1, 1))


def right_shift(x, col):
    return jnp.where(iota(x.shape, 1) == 0, col, pltpu.roll(x, 1, 1))


def row_up(x, row):
    n = x.shape[0]
    return jnp.where(iota(x.shape, 0) == n - 1, row, pltpu.roll(x, n - 1, 0))


def row_down(x, row):
    return jnp.where(iota(x.shape, 0) == 0, row, pltpu.roll(x, 1, 0))


def section_sums(n0, dn, d0, dd):
    n1, d1 = n0 + dn, d0 + dd
    ns, ds = n0 + n1, d0 + d1
    ends = d0 * d1
    inv = 1.0 / (ends * ds)
    half = ns * ends * inv
    side = ds * inv
    last = n1 * d0 * side
    first = n0 * d1 * side
    return (first + last) * (1.0 / 6.0) + half * (2.0 / 3.0), half * (1.0 / 3.0) + last * (1.0 / 6.0)


def energy(w, v, vt):
    return w * (v * v + v * vt + vt * vt * (1.0 / 3.0))


RGEO = 96
LGEO, LEN, LFLD = 40, 48, 64
(TH, THT, TH1, _, TU0, TU0T, TU1, TU1T, TU11, TU11T, TU2, TU2T, TU21, TU21T, TE2) = range(15)
(BH, BHT, BH1, _, BU0, BU0T, BU01, BU01T, BU1, BU1T, BU11, BU11T, BU2, BU2T, BE0) = range(15, 30)
RAW = 30


def pack_kernel(
    v, h, vt, ht, d, el, area, k, f, send_right, send_left, vo, ho, vto, hto, do, eo, ao, ko, fo, sems
):
    rows, cols = h.shape[1], h.shape[2]
    half = cols - 128
    started = []

    def start(src, dst):
        copy = pltpu.make_async_copy(src, dst, sems.at[len(started)])
        copy.start()
        started.append(copy)
        return copy

    fixed = [start(x, y) for x, y in ((d, do), (el, eo), (k, ko), (f, fo))]
    by_level = [
        [start(x.at[lev], y.at[lev]) for x, y in ((h, ho), (ht, hto))]
        + [start(x.at[:, lev], y.at[:, lev]) for x, y in ((v, vo), (vt, vto))]
        for lev in range(LV)
    ]
    area_copy = start(area, ao)
    for copy in fixed:
        copy.wait()

    lanes = iota((rows, 128), 1)

    def grow(x, y, n):
        return jnp.where(lanes < n, x, pltpu.roll(y, n, 1))

    def grow_back(x, y, n):
        return jnp.where(lanes >= 128 - n, y, pltpu.roll(x, 128 - n, 1))

    def tree(join, items, n):
        while len(items) > 1:
            items = [join(x, y, n) for x, y in zip(items[::2], items[1::2])]
            n *= 2
        return items[0]

    def geometry(part):
        out = [ko[a, b, :, part] for a in range(2) for b in range(3)]
        return out + [(out[3 * a] + out[3 * a + 1] + out[3 * a + 2]) * fo[a, :, part] for a in range(2)]

    low, high = slice(0, 128), slice(half, cols)
    geo_left = tree(grow, geometry(low), 1)
    geo_right = tree(grow_back, geometry(high), 1)
    first = [do[e, :, low] for e in range(3)]
    last = [do[e, :, high] for e in range(3)]
    weight = [0.25 * last[e] * eo[e, :, high] for e in range(3)]
    kinds = [(grow, 2)] * 4 + [(grow, 1)] * 4 + [(grow_back, 1)] * 10
    stacks = [[] for _ in kinds]
    for lev in range(LV):
        for copy in by_level[lev]:
            copy.wait()
        for part, dist, base in ((low, first, 0), (high, last, 8)):
            fields = [ho[lev, :, part], hto[lev, :, part]]
            fields += [dist[e] * x[e, lev, :, part] for e in range(3) for x in (vo, vto)]
            for n, x in enumerate(fields):
                stacks[base + n].append((1, x))
        for e in (1, 2):
            stacks[15 + e].append((1, energy(weight[e], vo[e, lev, :, high], vto[e, lev, :, high])))
        for stack, (join, width) in zip(stacks, kinds):
            while len(stack) > 1 and stack[-1][0] == stack[-2][0]:
                (count, x), (_, y) = stack[-2:]
                stack[-2:] = [(2 * count, join(x, y, count * width))]
    done = [stack[0][1] for stack in stacks]
    to_left = grow(tree(grow, done[0:4], 16), tree(grow, done[4:8], 8), 64)
    to_left = jnp.where(lanes < RGEO, to_left, pltpu.roll(geo_left, RGEO, 1))
    to_right = tree(grow_back, done[8:16], 8)
    to_right = grow_back(grow_back(done[16], done[17], 8), to_right, 64)
    to_right = jnp.where(lanes < LEN, pltpu.roll(geo_right, LEN, 1), to_right)
    send_right[...] = to_right
    send_left[...] = to_left
    area_copy.wait()


PACK_COPIES = 4 + 4 * LV + 1


def prep_kernel(v, h, vt, ht, d, el, area, k, f, raw, geo):
    end = h.shape[1] - 1
    for x, n in ((h, TH), (ht, THT)):
        raw[n] = x[:, 0, :]
        raw[n + 2] = x[:, 1, :]
    for x, n in ((h, BH), (ht, BHT)):
        raw[n] = x[:, end, :]
        raw[n + 2] = x[:, end - 1, :]
    for x, t in ((v, 0), (vt, 1)):
        for e, r, n in (
            (0, 0, TU0),
            (1, 0, TU1),
            (1, 1, TU11),
            (2, 0, TU2),
            (2, 1, TU21),
            (0, end, BU0),
            (0, end - 1, BU01),
            (1, end, BU1),
            (1, end - 1, BU11),
            (2, end, BU2),
        ):
            raw[n + t] = d[e, r : r + 1, :] * x[e, :, r, :]
    raw[TE2] = energy(0.25 * d[2, 0:1, :] * el[2, 0:1, :], v[2, :, 0, :], vt[2, :, 0, :])
    raw[BE0] = energy(0.25 * d[0, end : end + 1, :] * el[0, end : end + 1, :], v[0, :, end, :], vt[0, :, end, :])
    for a in range(2):
        geo[a] = (k[a, 0] + k[a, 1] + k[a, 2]) * f[a]
    for e in range(3):
        geo[2 + e] = (1.0 / 12.0) / d[e]
        geo[5 + e] = 0.25 * d[e] * el[e]
    geo[8] = 1.0 / area[...]


def af_row(k, f, a, r):
    return (k[a, 0, r : r + 1, :] + k[a, 1, r : r + 1, :] + k[a, 2, r : r + 1, :]) * f[a, r : r + 1, :]


def left_field(t, n):
    return t[LFLD + LV * n : LFLD + LV * n + LV, :]


def right_field(t, n, c=0):
    if n >= 4:
        return t[32 + LV * n : 32 + LV * n + LV, :]
    return t[pl.ds(16 * n + c, LV, stride=2), :]


def column_left(lt, h0, h0t, u00, u00t):
    k = [lt[LGEO + n : LGEO + n + 1, :] for n in range(8)]
    up = lambda x: pltpu.roll(x, 127, 1)
    dn = lambda x: pltpu.roll(x, 1, 1)
    h, hp, u0, u0p, u1, u1p, u2, u2p = (left_field(lt, n) for n in range(8))
    q0 = section_sums(
        k[6] + u0 - u1 + up(u2),
        u0p - u1p + up(u2p),
        k[0] * h + k[1] * up(h) + k[2] * h0,
        k[0] * hp + k[1] * up(hp) + k[2] * h0t,
    )
    q1 = section_sums(
        k[7] + u1 - u2 - dn(u00),
        u1p - u2p - dn(u00t),
        k[3] * h + k[4] * h0 + k[5] * dn(h0),
        k[3] * hp + k[4] * h0t + k[5] * dn(h0t),
    )
    return q0, q1


def column_right(rt):
    k = [rt[RGEO + n : RGEO + n + 1, :] for n in range(8)]
    up = lambda x: pltpu.roll(x, 127, 1)
    dn = lambda x: pltpu.roll(x, 1, 1)
    h, hp, u0, u0p, u1, u1p, u2, u2p = (right_field(rt, n) for n in range(8))
    h1, h1p, u01, u01p = (right_field(rt, n, 1) for n in range(4))
    q0 = section_sums(
        k[6] + u0 - u1 + up(u2),
        u0p - u1p + up(u2p),
        k[0] * h + k[1] * up(h) + k[2] * h1,
        k[0] * hp + k[1] * up(hp) + k[2] * h1p,
    )
    q1 = section_sums(
        k[7] + u1 - u2 - dn(u01),
        u1p - u2p - dn(u01p),
        k[3] * h + k[4] * h1 + k[5] * dn(h1),
        k[3] * hp + k[4] * h1p + k[5] * dn(h1p),
    )
    return q0, q1


def lane_col(x, lane):
    return x[:, lane : lane + 1]


def merge_kernel(slab_l, slab_r, own0, raw, k, f, msg_a, msg_b, ext, turned):
    odd_y = lax.rem(lax.axis_index("py"), 2) == 1
    rows = slab_l.shape[0]
    end = rows - 1
    left, right = slab_l[...], slab_r[...]
    ext[0, BASE : BASE + rows, :] = left
    ext[1, BASE : BASE + rows, :] = right
    ext[2, BASE : BASE + rows, :] = own0[...]
    for n in range(3):
        turned[n] = jnp.transpose(ext[n])
    lt, rt, ot = (turned.at[n] for n in range(3))
    q0l, q1l = column_left(lt, *(right_field(ot, n) for n in range(4)))
    q0r, q1r = column_right(rt)
    r0, r1 = BASE, BASE + 1
    e0, e1 = BASE + end, BASE + end - 1
    krow = lambda a, b, r: k[a, b, r : r + 1, :]

    h_0 = [left_shift(raw[TH + t], lane_col(right_field(rt, t), r0)) for t in range(2)]
    h_1 = [left_shift(raw[TH1 + t], lane_col(right_field(rt, t), r1)) for t in range(2)]
    u_0 = [left_shift(raw[TU0 + t], lane_col(right_field(rt, 2 + t), r0)) for t in range(2)]
    up0 = section_sums(
        af_row(k, f, 0, 0) + raw[TU0] - raw[TU1] + raw[TU21],
        raw[TU0T] - raw[TU1T] + raw[TU21T],
        *(krow(0, 0, 0) * raw[TH + t] + krow(0, 1, 0) * raw[TH1 + t] + krow(0, 2, 0) * h_0[t] for t in range(2)),
    )
    up1 = section_sums(
        af_row(k, f, 1, 1) + raw[TU11] - raw[TU21] - u_0[0],
        raw[TU11T] - raw[TU21T] - u_0[1],
        *(krow(1, 0, 1) * raw[TH1 + t] + krow(1, 1, 1) * h_1[t] + krow(1, 2, 1) * h_0[t] for t in range(2)),
    )
    up = [
        up0[t] + right_shift(up0[t] + up1[t], lane_col(q0l[t], r0) + lane_col(q1l[t], r1)) for t in range(2)
    ]

    hb_0 = [left_shift(raw[BH + t], lane_col(right_field(rt, t), e0)) for t in range(2)]
    hb_1 = [left_shift(raw[BH1 + t], lane_col(right_field(rt, t), e1)) for t in range(2)]
    ub_1 = [left_shift(raw[BU01 + t], lane_col(right_field(rt, 2 + t), e1)) for t in range(2)]
    dn1 = section_sums(
        af_row(k, f, 1, end) + raw[BU1] - raw[BU2] - ub_1[0],
        raw[BU1T] - raw[BU2T] - ub_1[1],
        *(krow(1, 0, end) * raw[BH + t] + krow(1, 1, end) * hb_0[t] + krow(1, 2, end) * hb_1[t] for t in range(2)),
    )
    dn0 = section_sums(
        af_row(k, f, 0, end - 1) + raw[BU01] - raw[BU11] + raw[BU2],
        raw[BU01T] - raw[BU11T] + raw[BU2T],
        *(
            krow(0, 0, end - 1) * raw[BH1 + t] + krow(0, 1, end - 1) * raw[BH + t] + krow(0, 2, end - 1) * hb_1[t]
            for t in range(2)
        ),
    )
    down = [
        left_shift(dn1[t] + dn0[t], lane_col(q1r[t], e0) + lane_col(q0r[t], e1)) + dn1[t] for t in range(2)
    ]

    def store(msg_up, msg_down):
        for msg, sums, parts, geo, r in (
            (msg_up, up, (TH, THT, TU1, TU1T, TU2, TU2T, TE2), 1, 0),
            (msg_down, down, (BH, BHT, BU0, BU0T, BU1, BU1T, BE0), 0, end),
        ):
            for n in range(2):
                msg[LV * n : LV * n + LV, :] = sums[n]
            for n, part in enumerate(parts):
                msg[LV * (n + 2) : LV * (n + 3), :] = raw[part]
            for n in range(3):
                msg[72 + n : 73 + n, :] = krow(geo, n, r)
            msg[75:76, :] = af_row(k, f, geo, r)
            msg[76:77, 0:128] = left[r : r + 1, :]
            msg[76:77, 128:256] = right[r : r + 1, :]

    @pl.when(odd_y)
    def _():
        store(msg_a, msg_b)

    @pl.when(jnp.logical_not(odd_y))
    def _():
        store(msg_b, msg_a)


(WQB, _, WQA, _, WMA, _, WMB, _, WE0, _, WF1, _, WEB, WEA) = range(14)
(CY, _, CQ, CP, _) = range(5)


def vertex_kernel(v, h, vt, ht, d, k, geo, slab_l, slab_r, q, kin):
    left, right = slab_l[...], slab_r[...]
    z = left + row_up(pltpu.roll(left, 128 - LV, 1), 0.0)
    for lev in range(LV):
        rcol = lambda n, lev=lev: right[:, 16 * n + 2 * lev : 16 * n + 2 * lev + 1]
        hh = [x[lev] for x in (h, ht)]
        u = [[d[e] * x[e, lev] for x in (v, vt)] for e in range(3)]
        h1 = [left_shift(hh[t], rcol(t)) for t in range(2)]
        u01 = [left_shift(u[0][t], rcol(2 + t)) for t in range(2)]
        up = lambda x: pltpu.roll(x, x.shape[0] - 1, 0)
        dn = lambda x: pltpu.roll(x, 1, 0)
        n0 = [u[0][t] - u[1][t] + up(u[2][t]) for t in range(2)]
        n1 = [u[1][t] - u[2][t] - dn(u01[t]) for t in range(2)]
        d0 = [k[0, 0] * hh[t] + k[0, 1] * up(hh[t]) + k[0, 2] * h1[t] for t in range(2)]
        d1 = [k[1, 0] * hh[t] + k[1, 1] * h1[t] + k[1, 2] * dn(h1[t]) for t in range(2)]
        q0 = section_sums(geo[0] + n0[0], n0[1], *d0)
        q1 = section_sums(geo[1] + n1[0], n1[1], *d1)
        for t in range(2):
            q[t, 0, lev] = q0[t]
            q[t, 1, lev] = q1[t]
        en = [energy(geo[5 + e], v[e, lev], vt[e, lev]) for e in range(3)]
        zz = en[1] + row_up(en[2], 0.0)
        zcol = z[:, LEN + lev : LEN + lev + 1]
        kin[lev] = en[0] + en[1] + en[2] + row_down(en[0], 0.0) + right_shift(zz, zcol)


def last_kernel(
    v, vt, k, f, geo, slab_l, slab_r, own0, raw, q, kin, msg_a, msg_b,
    vertex, kinetic, cell, edge, ext, turned, msgs, halo, vertex_v, kinetic_v, cell_v, edge_v, sems,
):
    odd_y = lax.rem(lax.axis_index("py"), 2) == 1
    rows = kin.shape[1]
    end = rows - 1

    @pl.when(odd_y)
    def _():
        msgs[0] = msg_b[...]
        msgs[1] = msg_a[...]

    @pl.when(jnp.logical_not(odd_y))
    def _():
        msgs[0] = msg_a[...]
        msgs[1] = msg_b[...]

    above = lambda n: msgs[0, LV * n : LV * n + LV, :]
    below = lambda n: msgs[1, LV * n : LV * n + LV, :]
    ka = [msgs[0, 72 + n : 73 + n, :] for n in range(4)]
    kb = [msgs[1, 72 + n : 73 + n, :] for n in range(4)]
    krow = lambda a, b, r: k[a, b, r : r + 1, :]

    left, right = slab_l[...], slab_r[...]
    ext[0, BASE : BASE + rows, :] = left
    ext[1, BASE : BASE + rows, :] = right
    ext[2, BASE : BASE + rows, :] = own0[...]
    ext[0, DNB : DNB + 1, :] = msgs[0, 76:77, 0:128]
    ext[1, DNB : DNB + 1, :] = msgs[0, 76:77, 128:256]
    ext[1, UPB : UPB + 1, :] = msgs[1, 76:77, 128:256]
    for n in range(3):
        turned[n] = jnp.transpose(ext[n])
    lt, rt, ot = (turned.at[n] for n in range(3))
    lanes = iota((LV, 128), 1)
    low = lambda x, row: jnp.where(lanes == UPB, row[:, 0:1], x)
    high = lambda x, row: jnp.where(lanes == DNB, row[:, 0:1], x)
    h0 = [high(low(right_field(ot, t), below(2 + t)), above(2 + t)) for t in range(2)]
    u00 = [low(right_field(ot, 2 + t), below(4 + t)) for t in range(2)]
    q0l, q1l = column_left(lt, *h0, *u00)
    q0r, q1r = column_right(rt)
    up = lambda x: pltpu.roll(x, 127, 1)
    dn = lambda x: pltpu.roll(x, 1, 1)
    cols_out = [
        q0l[0] + q1l[0] + up(q1l[0]),
        q0l[1] + q1l[1] + up(q1l[1]),
        up(q1l[0]),
        q0r[0] + q1r[0] + dn(q0r[0]),
        q0r[1] + q1r[1] + dn(q0r[1]),
    ]
    packed = jnp.concatenate(cols_out + [jnp.zeros((128 - LV * len(cols_out), 128), F32)], axis=0)
    inject = jnp.transpose(packed)[BASE : BASE + rows, :]

    hb1 = [left_shift(below(2 + t), lane_col(right_field(rt, t), UPB)) for t in range(2)]
    ub1 = [left_shift(below(4 + t), lane_col(right_field(rt, 2 + t), UPB)) for t in range(2)]
    h01 = [left_shift(raw[TH + t], lane_col(right_field(rt, t), BASE)) for t in range(2)]
    qb = section_sums(
        kb[3] + below(4) - below(6) + raw[TU2],
        below(5) - below(7) + raw[TU2T],
        *(kb[0] * below(2 + t) + kb[1] * raw[TH + t] + kb[2] * hb1[t] for t in range(2)),
    )
    q1f = section_sums(
        af_row(k, f, 1, 0) + raw[TU1] - raw[TU2] - ub1[0],
        raw[TU1T] - raw[TU2T] - ub1[1],
        *(krow(1, 0, 0) * raw[TH + t] + krow(1, 1, 0) * h01[t] + krow(1, 2, 0) * hb1[t] for t in range(2)),
    )
    ha1 = [left_shift(above(2 + t), lane_col(right_field(rt, t), DNB)) for t in range(2)]
    he1 = [left_shift(raw[BH + t], lane_col(right_field(rt, t), BASE + end)) for t in range(2)]
    ue1 = [left_shift(raw[BU0 + t], lane_col(right_field(rt, 2 + t), BASE + end)) for t in range(2)]
    qa = section_sums(
        ka[3] + above(4) - above(6) - ue1[0],
        above(5) - above(7) - ue1[1],
        *(ka[0] * above(2 + t) + ka[1] * ha1[t] + ka[2] * he1[t] for t in range(2)),
    )
    q0e = section_sums(
        af_row(k, f, 0, end) + raw[BU0] - raw[BU1] + above(6),
        raw[BU0T] - raw[BU1T] + above(7),
        *(krow(0, 0, end) * raw[BH + t] + krow(0, 1, end) * above(2 + t) + krow(0, 2, end) * he1[t] for t in range(2)),
    )
    for t in range(2):
        halo[WQB + t] = qb[t]
        halo[WQA + t] = qa[t]
        halo[WMA + t] = above(t) + qa[t] + right_shift(qa[t], lane_col(q1l[t], DNB)) + q0e[t]
        halo[WMB + t] = below(t) + qb[t] + left_shift(qb[t], lane_col(q0r[t], UPB)) + q1f[t]
        halo[WE0 + t] = q0e[t]
        halo[WF1 + t] = q1f[t]
    halo[WEB] = below(8)
    halo[WEA] = right_shift(above(8), lane_col(lt[LEN + LV : LEN + 2 * LV, :], DNB))

    copies = []
    for lev in range(LV):
        row = lambda n, lev=lev: halo[n, lev : lev + 1, :]
        col = lambda n, lev=lev: inject[:, LV * n + lev : LV * n + lev + 1]
        spot = iota(kin.shape[1:], 0)
        grads = []
        for t in range(2):
            q0 = jnp.where(spot == end, row(WE0 + t), q[t, 0, lev])
            q1 = jnp.where(spot == 0, row(WF1 + t), q[t, 1, lev])
            q0d = row_down(q0, row(WQB + t))
            q1u = row_up(q1, row(WQA + t))
            both = q0 + q1
            p, y = both + q0d, both + q1u
            m = p + right_shift(y, col(CY + t))
            m1 = left_shift(p, col(CP + t)) + y
            grads.append((row_up(m, row(WMA + t)) - m, m1 - m, row_down(m1, row(WMB + t)) - m))
            if t == 0:
                cell_v[lev] = m * (1.0 / 6.0)
                vertex_v[0, lev] = q0
                vertex_v[1, lev] = q1
                means = (q0 + right_shift(q1u, col(CQ)), both, q1 + q0d)
        for e in range(3):
            edge_v[e, lev] = 0.5 * means[e] - geo[2 + e] * (v[e, lev] * grads[0][e] + vt[e, lev] * grads[1][e])
        rim = jnp.where(spot == 0, row(WEB), 0.0) + jnp.where(spot == end, row(WEA), 0.0)
        kinetic_v[lev] = (kin[lev] + rim) * geo[8]
        for n, (src, dst) in enumerate(
            (
                (vertex_v.at[:, lev], vertex.at[:, lev]),
                (kinetic_v.at[lev], kinetic.at[lev]),
                (cell_v.at[lev], cell.at[lev]),
                (edge_v.at[:, lev], edge.at[:, lev]),
            )
        ):
            copy = pltpu.make_async_copy(src, dst, sems.at[4 * lev + n])
            copy.start()
            copies.append(copy)
    for copy in copies:
        copy.wait()


def shift(x, axis, by):
    n = lax.axis_size(axis)
    return lax.ppermute(x, axis, [(i, (i + by) % n) for i in range(n)])


def swap(x, axis, start):
    n = lax.axis_size(axis)
    pairs = []
    for i in range(start, n + start, 2):
        a, b = i % n, (i + 1) % n
        pairs += [(a, b), (b, a)]
    return lax.ppermute(x, axis, pairs)


VM = pl.BlockSpec(memory_space=pltpu.VMEM)
ANY = pl.BlockSpec(memory_space=pl.ANY)


def call(kernel, args, outs, scratch=(), sems=0, hbm_in=False, hbm_out=False, flops=0):
    args = [pltpu.with_memory_space_constraint(x, pltpu.HBM if hbm_in else pltpu.VMEM) for x in args]
    shape = (lambda s: jax.ShapeDtypeStruct(s, F32)) if hbm_out else (lambda s: pltpu.VMEM(s, F32))
    return pl.pallas_call(
        kernel,
        out_shape=[shape(s) for s in outs],
        in_specs=[ANY if hbm_in else VM] * len(args),
        out_specs=[ANY if hbm_out else VM] * len(outs),
        scratch_shapes=[pltpu.VMEM(s, F32) for s in scratch]
        + ([pltpu.SemaphoreType.DMA((sems,))] if sems else []),
        compiler_params=pltpu.CompilerParams(vmem_limit_bytes=16 * 2**20),
        cost_estimate=pl.CostEstimate(flops=flops, transcendentals=0, bytes_accessed=0) if flops else None,
    )(*args)


def step(*args):
    levels, rows, cols = args[1].shape
    slab = (rows, 128)
    send_right, send_left, *held = call(
        pack_kernel, args, [slab, slab] + [x.shape for x in args], sems=PACK_COPIES, hbm_in=True
    )
    v, h, vt, ht, d, _, _, k, f = held
    slab_l = shift(send_right, "px", 1)
    slab_r = shift(send_left, "px", -1)
    raw, geo = call(prep_kernel, held, [(RAW, levels, cols), (9, rows, cols)], flops=20_000_000)
    msg_a, msg_b = call(
        merge_kernel, [slab_l, slab_r, send_left, raw, k, f], [(80, cols), (80, cols)], [(3, 128, 128), (3, 128, 128)]
    )
    msg_b = swap(msg_b, "py", 1)
    msg_a = swap(msg_a, "py", 0)
    q, kin = call(
        vertex_kernel,
        [v, h, vt, ht, d, k, geo, slab_l, slab_r],
        [(2, 2, levels, rows, cols), (levels, rows, cols)],
        flops=40_000_000,
    )
    return tuple(
        call(
            last_kernel,
            [v, vt, k, f, geo, slab_l, slab_r, send_left, raw, q, kin, msg_a, msg_b],
            [(2, levels, rows, cols), (levels, rows, cols), (levels, rows, cols), (3, levels, rows, cols)],
            [
                (3, 128, 128), (3, 128, 128), (2, 80, cols), (14, levels, cols),
                (2, levels, rows, cols), (levels, rows, cols), (levels, rows, cols), (3, levels, rows, cols),
            ],
            sems=4 * LV,
            hbm_out=True,
        )
    )


def solution(mesh):
    field = P(None, "py", "px")
    pair = P(None, None, "py", "px")
    return jax.shard_map(
        step,
        mesh=mesh,
        in_specs=(pair, field, pair, field, field, field, P("py", "px"), pair, field),
        out_specs=(pair, field, field, pair),
        check_vma=False,
    )
```

```python
import jax
import jax.numpy as jnp
from jax import lax
from jax.experimental import pallas as pl
from jax.experimental.pallas import tpu as pltpu
from jax.sharding import PartitionSpec as P

F32 = jnp.float32
LV = 8
BASE = 8
UPB, DNB = BASE - 1, BASE + 32


def iota(shape, dim):
    return lax.broadcasted_iota(jnp.int32, shape, dim)


def left_shift(x, col):
    n = x.shape[1]
    return jnp.where(iota(x.shape, 1) == n - 1, col, pltpu.roll(x, n - 1, 1))


def right_shift(x, col):
    return jnp.where(iota(x.shape, 1) == 0, col, pltpu.roll(x, 1, 1))


def row_up(x, row):
    n = x.shape[0]
    return jnp.where(iota(x.shape, 0) == n - 1, row, pltpu.roll(x, n - 1, 0))


def row_down(x, row):
    return jnp.where(iota(x.shape, 0) == 0, row, pltpu.roll(x, 1, 0))


def section_sums(n0, dn, d0, dd):
    n1, d1 = n0 + dn, d0 + dd
    ns, ds = n0 + n1, d0 + d1
    ends = d0 * d1
    inv = 1.0 / (ends * ds)
    half = ns * ends * inv
    side = ds * inv
    last = n1 * d0 * side
    first = n0 * d1 * side
    return (first + last) * (1.0 / 6.0) + half * (2.0 / 3.0), half * (1.0 / 3.0) + last * (1.0 / 6.0)


def energy(w, v, vt):
    return w * (v * v + v * vt + vt * vt * (1.0 / 3.0))


RGEO = 96
LGEO, LEN, LFLD = 40, 48, 64
(TH, THT, TH1, _, TU0, TU0T, TU1, TU1T, TU11, TU11T, TU2, TU2T, TU21, TU21T, TE2) = range(15)
(BH, BHT, BH1, _, BU0, BU0T, BU01, BU01T, BU1, BU1T, BU11, BU11T, BU2, BU2T, BE0) = range(15, 30)
RIM = ((0, 0), (1, 0), (2, 0), (2, 1), (0, -2), (0, -1), (1, -1), (2, -1))
RAW = 30 + 2 * len(RIM)


def pack_kernel(
    v, h, vt, ht, d, el, area, k, f, send_right, send_left, vo, ho, vto, hto, do, eo, ao, ko, fo, sems
):
    rows, cols = h.shape[1], h.shape[2]
    half = cols - 128
    started = []

    def start(src, dst):
        copy = pltpu.make_async_copy(src, dst, sems.at[len(started)])
        copy.start()
        started.append(copy)
        return copy

    fixed = [start(x, y) for x, y in ((d, do), (el, eo), (k, ko), (f, fo))]
    by_level = []
    for lev in range(0, LV, LV // 2):
        cut = slice(lev, lev + LV // 2)
        by_level.append([start(x.at[cut], y.at[cut]) for x, y in ((h, ho), (ht, hto))])
        by_level[-1] += [start(x.at[:, cut], y.at[:, cut]) for x, y in ((v, vo), (vt, vto))]
    area_copy = start(area, ao)
    for copy in fixed:
        copy.wait()

    lanes = iota((rows, 128), 1)

    def push(stack, x, wide=1, first=0):
        if stack is None:
            return x
        back = pltpu.roll(stack, 128 - wide, 1)
        return jnp.where(lanes == 127, x, back) if first else jnp.where(lanes < wide, x, back)

    def place(slab, stack, by, start, stop):
        moved = pltpu.roll(stack, by % 128, 1) if by % 128 else stack
        return jnp.where((lanes >= start) & (lanes < stop), moved, slab)

    def geometry(part):
        out = [ko[a, b, :, part] for a in range(2) for b in range(3)]
        return out + [(out[3 * a] + out[3 * a + 1] + out[3 * a + 2]) * fo[a, :, part] for a in range(2)]

    low, high = slice(0, 128), slice(half, cols)
    geo_left = geo_right = None
    for x, y in zip(geometry(low), geometry(high)):
        geo_left = push(geo_left, x)
        geo_right = push(geo_right, y, 1, 127)
    near = [do[e, :, low] for e in range(3)]
    far = [do[e, :, high] for e in range(3)]
    weight = [0.25 * far[e] * eo[e, :, high] for e in range(3)]
    left, right = [None] * 8, [None] * 10
    for lev in range(LV):
        if lev % (LV // 2) == 0:
            for copy in by_level[lev // (LV // 2)]:
                copy.wait()
        for part, dist, stacks in ((low, near, left), (high, far, right)):
            fields = [ho[lev, :, part], hto[lev, :, part]]
            fields += [dist[e] * x[e, lev, :, part] for e in range(3) for x in (vo, vto)]
            if part is high:
                fields += [energy(weight[e], vo[e, lev, :, part], vto[e, lev, :, part]) for e in (1, 2)]
            for n, x in enumerate(fields):
                stacks[n] = push(stacks[n], x, *((1, 127) if part is high else (2,) if n < 4 else (1,)))
    to_left = jnp.zeros((rows, 128), F32)
    to_right = right[7]
    for n in range(4):
        to_left = place(to_left, left[n], 16 * n + 14, 16 * n, 16 * n + 16)
        to_left = place(to_left, left[n + 4], 64 + LV * n + 7, 64 + LV * n, 72 + LV * n)
    to_left = place(to_left, geo_left, RGEO + 7, RGEO, RGEO + 8)
    for n in range(7):
        to_right = place(to_right, right[n], LFLD + LV * n - 120, LFLD + LV * n, LFLD + LV * n + LV)
    for n in range(2):
        to_right = place(to_right, right[8 + n], LEN + LV * n - 120, LEN + LV * n, LEN + LV * n + LV)
    to_right = place(to_right, geo_right, LGEO - 120, LGEO, LGEO + 8)
    send_right[...] = to_right
    send_left[...] = to_left
    area_copy.wait()


PACK_COPIES = 4 + 4 * 2 + 1


def vertex_kernel(v, h, vt, ht, d, el, area, k, f, raw, geo, q, kin):
    rows = h.shape[1]
    end = rows - 1
    for x, n in ((h, TH), (ht, THT)):
        raw[n] = x[:, 0, :]
        raw[n + 2] = x[:, 1, :]
    for x, n in ((h, BH), (ht, BHT)):
        raw[n] = x[:, end, :]
        raw[n + 2] = x[:, end - 1, :]
    for x, t in ((v, 0), (vt, 1)):
        for e, r, n in (
            (0, 0, TU0),
            (1, 0, TU1),
            (1, 1, TU11),
            (2, 0, TU2),
            (2, 1, TU21),
            (0, end, BU0),
            (0, end - 1, BU01),
            (1, end, BU1),
            (1, end - 1, BU11),
            (2, end, BU2),
        ):
            raw[n + t] = d[e, r : r + 1, :] * x[e, :, r, :]
    raw[TE2] = energy(0.25 * d[2, 0:1, :] * el[2, 0:1, :], v[2, :, 0, :], vt[2, :, 0, :])
    raw[BE0] = energy(0.25 * d[0, end : end + 1, :] * el[0, end : end + 1, :], v[0, :, end, :], vt[0, :, end, :])
    for a in range(2):
        geo[a] = (k[a, 0] + k[a, 1] + k[a, 2]) * f[a]
    for e in range(3):
        geo[2 + e] = (1.0 / 12.0) / d[e]
        geo[5 + e] = 0.25 * d[e] * el[e]
    geo[8] = 1.0 / area[...]
    for n, (e, r) in enumerate(RIM):
        for x, t in ((v, 0), (vt, 1)):
            raw[30 + 2 * n + t] = x[e, :, r % rows, :]

    up = lambda x: pltpu.roll(x, rows - 1, 0)
    dn = lambda x: pltpu.roll(x, 1, 0)
    right = lambda x: pltpu.roll(x, x.shape[1] - 1, 1)
    for lev in range(LV):
        hh = [x[lev] for x in (h, ht)]
        u = [[d[e] * x[e, lev] for x in (v, vt)] for e in range(3)]
        h1 = [right(x) for x in hh]
        u01 = [right(x) for x in u[0]]
        n0 = [u[0][t] - u[1][t] + up(u[2][t]) for t in range(2)]
        n1 = [u[1][t] - u[2][t] - dn(u01[t]) for t in range(2)]
        d0 = [k[0, 0] * hh[t] + k[0, 1] * up(hh[t]) + k[0, 2] * h1[t] for t in range(2)]
        d1 = [k[1, 0] * hh[t] + k[1, 1] * h1[t] + k[1, 2] * dn(h1[t]) for t in range(2)]
        q0 = section_sums(geo[0] + n0[0], n0[1], *d0)
        q1 = section_sums(geo[1] + n1[0], n1[1], *d1)
        for t in range(2):
            q[t, 0, lev] = q0[t]
            q[t, 1, lev] = q1[t]
        en = [energy(geo[5 + e], v[e, lev], vt[e, lev]) for e in range(3)]
        zz = en[1] + row_up(en[2], 0.0)
        kin[lev] = en[0] + en[1] + en[2] + row_down(en[0], 0.0) + right_shift(zz, 0.0)


def af_row(k, f, a, r):
    return (k[a, 0, r : r + 1, :] + k[a, 1, r : r + 1, :] + k[a, 2, r : r + 1, :]) * f[a, r : r + 1, :]


def left_field(t, n):
    return t[LFLD + LV * n : LFLD + LV * n + LV, :]


def right_field(t, n, c=0):
    if n >= 4:
        return t[32 + LV * n : 32 + LV * n + LV, :]
    return t[pl.ds(16 * n + c, LV, stride=2), :]


def column_left(lt, h0, h0t, u00, u00t):
    k = [lt[LGEO + n : LGEO + n + 1, :] for n in range(8)]
    up = lambda x: pltpu.roll(x, 127, 1)
    dn = lambda x: pltpu.roll(x, 1, 1)
    h, hp, u0, u0p, u1, u1p, u2, u2p = (left_field(lt, n) for n in range(8))
    q0 = section_sums(
        k[6] + u0 - u1 + up(u2),
        u0p - u1p + up(u2p),
        k[0] * h + k[1] * up(h) + k[2] * h0,
        k[0] * hp + k[1] * up(hp) + k[2] * h0t,
    )
    q1 = section_sums(
        k[7] + u1 - u2 - dn(u00),
        u1p - u2p - dn(u00t),
        k[3] * h + k[4] * h0 + k[5] * dn(h0),
        k[3] * hp + k[4] * h0t + k[5] * dn(h0t),
    )
    return q0, q1


def column_right(rt):
    k = [rt[RGEO + n : RGEO + n + 1, :] for n in range(8)]
    up = lambda x: pltpu.roll(x, 127, 1)
    dn = lambda x: pltpu.roll(x, 1, 1)
    h, hp, u0, u0p, u1, u1p, u2, u2p = (right_field(rt, n) for n in range(8))
    h1, h1p, u01, u01p = (right_field(rt, n, 1) for n in range(4))
    q0 = section_sums(
        k[6] + u0 - u1 + up(u2),
        u0p - u1p + up(u2p),
        k[0] * h + k[1] * up(h) + k[2] * h1,
        k[0] * hp + k[1] * up(hp) + k[2] * h1p,
    )
    q1 = section_sums(
        k[7] + u1 - u2 - dn(u01),
        u1p - u2p - dn(u01p),
        k[3] * h + k[4] * h1 + k[5] * dn(h1),
        k[3] * hp + k[4] * h1p + k[5] * dn(h1p),
    )
    return q0, q1


def lane_col(x, lane):
    return x[:, lane : lane + 1]


def merge_kernel(slab_l, slab_r, own0, raw, k, f, msg_a, msg_b, ext, turned):
    odd_y = lax.rem(lax.axis_index("py"), 2) == 1
    rows = slab_l.shape[0]
    end = rows - 1
    left, right = slab_l[...], slab_r[...]
    ext[0, BASE : BASE + rows, :] = left
    ext[1, BASE : BASE + rows, :] = right
    ext[2, BASE : BASE + rows, :] = own0[...]
    lt, rt, ot = turn(turned, *(ext[n] for n in range(3)))
    q0l, q1l = column_left(lt, *(right_field(ot, n) for n in range(4)))
    q0r, q1r = column_right(rt)
    r0, r1 = BASE, BASE + 1
    e0, e1 = BASE + end, BASE + end - 1
    krow = lambda a, b, r: k[a, b, r : r + 1, :]

    h_0 = [left_shift(raw[TH + t], lane_col(right_field(rt, t), r0)) for t in range(2)]
    h_1 = [left_shift(raw[TH1 + t], lane_col(right_field(rt, t), r1)) for t in range(2)]
    u_0 = [left_shift(raw[TU0 + t], lane_col(right_field(rt, 2 + t), r0)) for t in range(2)]
    up0 = section_sums(
        af_row(k, f, 0, 0) + raw[TU0] - raw[TU1] + raw[TU21],
        raw[TU0T] - raw[TU1T] + raw[TU21T],
        *(krow(0, 0, 0) * raw[TH + t] + krow(0, 1, 0) * raw[TH1 + t] + krow(0, 2, 0) * h_0[t] for t in range(2)),
    )
    up1 = section_sums(
        af_row(k, f, 1, 1) + raw[TU11] - raw[TU21] - u_0[0],
        raw[TU11T] - raw[TU21T] - u_0[1],
        *(krow(1, 0, 1) * raw[TH1 + t] + krow(1, 1, 1) * h_1[t] + krow(1, 2, 1) * h_0[t] for t in range(2)),
    )
    up = [
        up0[t] + right_shift(up0[t] + up1[t], lane_col(q0l[t], r0) + lane_col(q1l[t], r1)) for t in range(2)
    ]

    hb_0 = [left_shift(raw[BH + t], lane_col(right_field(rt, t), e0)) for t in range(2)]
    hb_1 = [left_shift(raw[BH1 + t], lane_col(right_field(rt, t), e1)) for t in range(2)]
    ub_1 = [left_shift(raw[BU01 + t], lane_col(right_field(rt, 2 + t), e1)) for t in range(2)]
    dn1 = section_sums(
        af_row(k, f, 1, end) + raw[BU1] - raw[BU2] - ub_1[0],
        raw[BU1T] - raw[BU2T] - ub_1[1],
        *(krow(1, 0, end) * raw[BH + t] + krow(1, 1, end) * hb_0[t] + krow(1, 2, end) * hb_1[t] for t in range(2)),
    )
    dn0 = section_sums(
        af_row(k, f, 0, end - 1) + raw[BU01] - raw[BU11] + raw[BU2],
        raw[BU01T] - raw[BU11T] + raw[BU2T],
        *(
            krow(0, 0, end - 1) * raw[BH1 + t] + krow(0, 1, end - 1) * raw[BH + t] + krow(0, 2, end - 1) * hb_1[t]
            for t in range(2)
        ),
    )
    down = [
        left_shift(dn1[t] + dn0[t], lane_col(q1r[t], e0) + lane_col(q0r[t], e1)) + dn1[t] for t in range(2)
    ]

    def store(msg_up, msg_down):
        for msg, sums, parts, geo, r in (
            (msg_up, up, (TH, THT, TU1, TU1T, TU2, TU2T, TE2), 1, 0),
            (msg_down, down, (BH, BHT, BU0, BU0T, BU1, BU1T, BE0), 0, end),
        ):
            for n in range(2):
                msg[LV * n : LV * n + LV, :] = sums[n]
            for n, part in enumerate(parts):
                msg[LV * (n + 2) : LV * (n + 3), :] = raw[part]
            for n in range(3):
                msg[72 + n : 73 + n, :] = krow(geo, n, r)
            msg[75:76, :] = af_row(k, f, geo, r)
            msg[76:77, 0:128] = left[r : r + 1, :]
            msg[76:77, 128:256] = right[r : r + 1, :]

    @pl.when(odd_y)
    def _():
        store(msg_a, msg_b)

    @pl.when(jnp.logical_not(odd_y))
    def _():
        store(msg_b, msg_a)


(CY, _, CQ, CZ, CP, _, C0, _, C1, _) = range(10)
(K00, _, K11, _, K0B, _, K1E, _, KM1, _, KMB, _, KMR, _) = range(14)


def turn(turned, *slabs):
    for n, x in enumerate(slabs):
        turned[n] = jnp.transpose(x)
    return [turned.at[n] for n in range(len(slabs))]


def middle_kernel(v, vt, geo, q, kin, slab_l, slab_r, own_l, own_r, vertex, kinetic, cell, edge, keep, ext, turned):
    rows = kin.shape[1]
    end = rows - 1
    for n, x in enumerate((slab_l, slab_r, own_l, own_r)):
        ext[n, BASE : BASE + rows, :] = x[...]
    lt, rt, ot, et = turn(turned, *(ext[n] for n in range(4)))
    q0l, q1l = column_left(lt, *(right_field(ot, n) for n in range(4)))
    q0r, q1r = column_right(rt)
    q0c, q1c = column_left(et, *(right_field(rt, n) for n in range(4)))
    up = lambda x: pltpu.roll(x, 127, 1)
    dn = lambda x: pltpu.roll(x, 1, 1)
    columns = [
        q0l[0] + q1l[0] + up(q1l[0]),
        q0l[1] + q1l[1] + up(q1l[1]),
        up(q1l[0]),
        lt[LEN : LEN + LV, :] + jnp.where(iota((LV, 128), 1) < BASE + end, up(lt[LEN + LV : LEN + 2 * LV, :]), 0.0),
        q0r[0] + q1r[0] + dn(q0r[0]),
        q0r[1] + q1r[1] + dn(q0r[1]),
        *q0c,
        *q1c,
    ]
    packed = jnp.concatenate(columns + [jnp.zeros((128 - LV * len(columns), 128), F32)], axis=0)
    inject = jnp.transpose(packed)[BASE : BASE + rows, :]
    side = iota(kin.shape[1:], 1)
    for lev in range(LV):
        col = lambda n, lev=lev: inject[:, LV * n + lev : LV * n + lev + 1]
        put = lambda n, x, r, lev=lev: keep.__setitem__((n, slice(lev, lev + 1), slice(None)), x[r : r + 1, :])
        grads = []
        for t in range(2):
            q0 = jnp.where(side == kin.shape[2] - 1, col(C0 + t), q[t, 0, lev])
            q1 = jnp.where(side == kin.shape[2] - 1, col(C1 + t), q[t, 1, lev])
            q0d = pltpu.roll(q0, 1, 0)
            q1u = pltpu.roll(q1, end, 0)
            both = q0 + q1
            p, y = both + q0d, both + q1u
            m = p + right_shift(y, col(CY + t))
            m1 = left_shift(p, col(CP + t)) + y
            grads.append((pltpu.roll(m, end, 0) - m, m1 - m, pltpu.roll(m1, 1, 0) - m))
            put(K00 + t, q0, 0)
            put(K11 + t, q1, 1)
            put(K0B + t, q0, end - 1)
            put(K1E + t, q1, end)
            put(KM1 + t, m, 1)
            put(KMB + t, m, end - 1)
            put(KMR + t, m1, end - 1)
            if t == 0:
                cell[lev] = m * (1.0 / 6.0)
                vertex[0, lev] = q0
                vertex[1, lev] = q1
                means = (q0 + right_shift(q1u, col(CQ)), both, q1 + q0d)
        for e in range(3):
            edge[e, lev] = 0.5 * means[e] - geo[2 + e] * (v[e, lev] * grads[0][e] + vt[e, lev] * grads[1][e])
        kinetic[lev] = (kin[lev] + jnp.where(side == 0, col(CZ), 0.0)) * geo[8]


def last_kernel(
    k, f, geo, slab_l, slab_r, own0, raw, keep, vertex_v, kinetic_v, cell_v, edge_v, msg_a, msg_b,
    vertex, kinetic, cell, edge, ext, turned, msgs, rim, tiles, sems,
):
    odd_y = lax.rem(lax.axis_index("py"), 2) == 1
    rows = kinetic_v.shape[1]
    end = rows - 1
    arrays = (
        [(vertex_v.at[n], vertex.at[n]) for n in range(2)]
        + [(kinetic_v, kinetic), (cell_v, cell)]
        + [(edge_v.at[n], edge.at[n]) for n in range(3)]
    )
    copies = []

    def start(src, dst):
        copy = pltpu.make_async_copy(src, dst, sems.at[len(copies)])
        copy.start()
        copies.append(copy)

    top, bottom = slice(0, 8), slice(rows - 8, rows)
    for n, (src, dst) in enumerate(arrays):
        inner = slice(0 if n == 0 else 8, rows if n == 1 else rows - 8)
        start(src.at[:, inner], dst.at[:, inner])

    @pl.when(odd_y)
    def _():
        msgs[0] = msg_b[...]
        msgs[1] = msg_a[...]

    @pl.when(jnp.logical_not(odd_y))
    def _():
        msgs[0] = msg_a[...]
        msgs[1] = msg_b[...]

    above = lambda n: msgs[0, LV * n : LV * n + LV, :]
    below = lambda n: msgs[1, LV * n : LV * n + LV, :]
    ka = [msgs[0, 72 + n : 73 + n, :] for n in range(4)]
    kb = [msgs[1, 72 + n : 73 + n, :] for n in range(4)]
    krow = lambda a, b, r: k[a, b, r : r + 1, :]

    for n, x in enumerate((slab_l, slab_r, own0)):
        ext[n, BASE : BASE + rows, :] = x[...]
    ext[0, DNB : DNB + 1, :] = msgs[0, 76:77, 0:128]
    ext[1, DNB : DNB + 1, :] = msgs[0, 76:77, 128:256]
    ext[1, UPB : UPB + 1, :] = msgs[1, 76:77, 128:256]
    lt, rt, ot = turn(turned, *(ext[n] for n in range(3)))
    lanes = iota((LV, 128), 1)
    low = lambda x, row: jnp.where(lanes == UPB, row[:, 0:1], x)
    high = lambda x, row: jnp.where(lanes == DNB, row[:, 0:1], x)
    h0 = [high(low(right_field(ot, t), below(2 + t)), above(2 + t)) for t in range(2)]
    u00 = [low(right_field(ot, 2 + t), below(4 + t)) for t in range(2)]
    q0l, q1l = column_left(lt, *h0, *u00)
    q0r, q1r = column_right(rt)
    up = lambda x: pltpu.roll(x, 127, 1)
    dn = lambda x: pltpu.roll(x, 1, 1)
    ycol = [q0l[t] + q1l[t] + up(q1l[t]) for t in range(2)]
    pcol = [q0r[t] + q1r[t] + dn(q0r[t]) for t in range(2)]
    r0, re = BASE, BASE + end

    hb1 = [left_shift(below(2 + t), lane_col(right_field(rt, t), UPB)) for t in range(2)]
    ub1 = [left_shift(below(4 + t), lane_col(right_field(rt, 2 + t), UPB)) for t in range(2)]
    h01 = [left_shift(raw[TH + t], lane_col(right_field(rt, t), BASE)) for t in range(2)]
    qb = section_sums(
        kb[3] + below(4) - below(6) + raw[TU2],
        below(5) - below(7) + raw[TU2T],
        *(kb[0] * below(2 + t) + kb[1] * raw[TH + t] + kb[2] * hb1[t] for t in range(2)),
    )
    q1f = section_sums(
        af_row(k, f, 1, 0) + raw[TU1] - raw[TU2] - ub1[0],
        raw[TU1T] - raw[TU2T] - ub1[1],
        *(krow(1, 0, 0) * raw[TH + t] + krow(1, 1, 0) * h01[t] + krow(1, 2, 0) * hb1[t] for t in range(2)),
    )
    ha1 = [left_shift(above(2 + t), lane_col(right_field(rt, t), DNB)) for t in range(2)]
    he1 = [left_shift(raw[BH + t], lane_col(right_field(rt, t), re)) for t in range(2)]
    ue1 = [left_shift(raw[BU0 + t], lane_col(right_field(rt, 2 + t), re)) for t in range(2)]
    qa = section_sums(
        ka[3] + above(4) - above(6) - ue1[0],
        above(5) - above(7) - ue1[1],
        *(ka[0] * above(2 + t) + ka[1] * ha1[t] + ka[2] * he1[t] for t in range(2)),
    )
    q0e = section_sums(
        af_row(k, f, 0, end) + raw[BU0] - raw[BU1] + above(6),
        raw[BU0T] - raw[BU1T] + above(7),
        *(krow(0, 0, end) * raw[BH + t] + krow(0, 1, end) * above(2 + t) + krow(0, 2, end) * he1[t] for t in range(2)),
    )
    grads = []
    for t in range(2):
        p0, y0 = keep[K00 + t] + q1f[t] + qb[t], keep[K00 + t] + q1f[t] + keep[K11 + t]
        pe, ye = q0e[t] + keep[K1E + t] + keep[K0B + t], q0e[t] + keep[K1E + t] + qa[t]
        m0 = p0 + right_shift(y0, lane_col(ycol[t], r0))
        m0r = left_shift(p0, lane_col(pcol[t], r0)) + y0
        me = pe + right_shift(ye, lane_col(ycol[t], re))
        mer = left_shift(pe, lane_col(pcol[t], re)) + ye
        m_above = above(t) + qa[t] + right_shift(qa[t], lane_col(q1l[t], DNB)) + q0e[t]
        m_below = below(t) + qb[t] + left_shift(qb[t], lane_col(q0r[t], UPB)) + q1f[t]
        grads.append(
            (
                keep[KM1 + t] - m0,
                m0r - m0,
                m_below - m0,
                m0r - keep[KM1 + t],
                me - keep[KMB + t],
                m_above - me,
                mer - me,
                keep[KMR + t] - me,
            )
        )
        if t == 0:
            rim[8] = q1f[0]
            rim[9] = m0 * (1.0 / 6.0)
            rim[10] = q0e[0]
            rim[11] = me * (1.0 / 6.0)
            means = (
                keep[K00] + right_shift(keep[K11], lane_col(q1l[0], r0 + 1)),
                keep[K00] + q1f[0],
                q1f[0] + qb[0],
                keep[K11] + keep[K00],
                keep[K0B] + right_shift(keep[K1E], lane_col(q1l[0], re)),
                q0e[0] + right_shift(qa[0], lane_col(q1l[0], DNB)),
                q0e[0] + keep[K1E],
                keep[K1E] + keep[K0B],
            )
    for n, (e, r) in enumerate(RIM):
        r = r % rows
        rim[n] = 0.5 * means[n] - geo[2 + e, r : r + 1, :] * (
            raw[30 + 2 * n] * grads[0][n] + raw[31 + 2 * n] * grads[1][n]
        )
    rim[12] = below(8) * geo[8, 0:1, :]
    rim[13] = right_shift(above(8), lane_col(lt[LEN + LV : LEN + 2 * LV, :], DNB)) * geo[8, end : end + 1, :]

    spot = iota((8, kinetic_v.shape[2]), 0)
    tile = 0
    for part, patches in (
        (top, ((1, ((0, 8),)), (2, ((0, 12),)), (3, ((0, 9),)), (4, ((0, 0),)), (5, ((0, 1),)), (6, ((0, 2), (1, 3))))),
        (bottom, ((0, ((7, 10),)), (2, ((7, 13),)), (3, ((7, 11),)), (4, ((6, 4), (7, 5))), (5, ((7, 6),)), (6, ((7, 7),)))),
    ):
        for n, changes in patches:
            src, dst = arrays[n]
            for lev in range(LV):
                x = src[lev, part, :]
                for r, m in changes:
                    new = rim[m, lev : lev + 1, :]
                    x = jnp.where(spot == r, x + new if n == 2 else new, x)
                tiles[tile, lev] = x
            start(tiles.at[tile], dst.at[:, part])
            tile += 1
    for copy in copies:
        copy.wait()


LAST_COPIES = 7 + 12


def shift(x, axis, by):
    n = lax.axis_size(axis)
    return lax.ppermute(x, axis, [(i, (i + by) % n) for i in range(n)])


def swap(x, axis, start):
    n = lax.axis_size(axis)
    pairs = []
    for i in range(start, n + start, 2):
        a, b = i % n, (i + 1) % n
        pairs += [(a, b), (b, a)]
    return lax.ppermute(x, axis, pairs)


VM = pl.BlockSpec(memory_space=pltpu.VMEM)
ANY = pl.BlockSpec(memory_space=pl.ANY)


def call(kernel, args, outs, scratch=(), sems=0, hbm_in=False, hbm_out=False, flops=0):
    args = [pltpu.with_memory_space_constraint(x, pltpu.HBM if hbm_in else pltpu.VMEM) for x in args]
    shape = (lambda s: jax.ShapeDtypeStruct(s, F32)) if hbm_out else (lambda s: pltpu.VMEM(s, F32))
    return pl.pallas_call(
        kernel,
        out_shape=[shape(s) for s in outs],
        in_specs=[ANY if hbm_in else VM] * len(args),
        out_specs=[ANY if hbm_out else VM] * len(outs),
        scratch_shapes=[pltpu.VMEM(s, F32) for s in scratch]
        + ([pltpu.SemaphoreType.DMA((sems,))] if sems else []),
        compiler_params=pltpu.CompilerParams(vmem_limit_bytes=16 * 2**20),
        cost_estimate=pl.CostEstimate(flops=flops, transcendentals=0, bytes_accessed=0) if flops else None,
    )(*args)


def step(*args):
    levels, rows, cols = args[1].shape
    slab = (rows, 128)
    send_right, send_left, *held = call(
        pack_kernel, args, [slab, slab] + [x.shape for x in args], sems=PACK_COPIES, hbm_in=True
    )
    v, _, vt, _, _, _, _, k, f = held
    slab_l = shift(send_right, "px", 1)
    slab_r = shift(send_left, "px", -1)
    whole = [(2, levels, rows, cols), (levels, rows, cols), (levels, rows, cols), (3, levels, rows, cols)]
    raw, geo, q, kin = call(
        vertex_kernel,
        held,
        [(RAW, levels, cols), (9, rows, cols), (2, 2, levels, rows, cols), (levels, rows, cols)],
        flops=40_000_000,
    )
    turned = [(4, 128, 128), (4, 128, 128)]
    msg_a, msg_b = call(
        merge_kernel, [slab_l, slab_r, send_left, raw, k, f], [(80, cols), (80, cols)], turned
    )
    msg_b = swap(msg_b, "py", 1)
    msg_a = swap(msg_a, "py", 0)
    *parts, keep = call(
        middle_kernel,
        [v, vt, geo, q, kin, slab_l, slab_r, send_left, send_right],
        whole + [(14, levels, cols)],
        turned,
        flops=40_000_000,
    )
    return tuple(
        call(
            last_kernel,
            [k, f, geo, slab_l, slab_r, send_left, raw, keep, *parts, msg_a, msg_b],
            whole,
            turned + [(2, 80, cols), (14, levels, cols), (12, levels, 8, cols)],
            sems=LAST_COPIES,
            hbm_out=True,
        )
    )


def solution(mesh):
    field = P(None, "py", "px")
    pair = P(None, None, "py", "px")
    return jax.shard_map(
        step,
        mesh=mesh,
        in_specs=(pair, field, pair, field, field, field, P("py", "px"), pair, field),
        out_specs=(pair, field, field, pair),
        check_vma=False,
    )
```

```python
import functools

import jax
import jax.numpy as jnp
from jax import lax
from jax.experimental import pallas as pl
from jax.experimental.pallas import tpu as pltpu
from jax.sharding import PartitionSpec as P

F32 = jnp.float32
LV = 8
BASE = 8
UPB, DNB = BASE - 1, BASE + 32


def iota(shape, dim):
    return lax.broadcasted_iota(jnp.int32, shape, dim)


def left_shift(x, col):
    n = x.shape[1]
    return jnp.where(iota(x.shape, 1) == n - 1, col, pltpu.roll(x, n - 1, 1))


def right_shift(x, col):
    return jnp.where(iota(x.shape, 1) == 0, col, pltpu.roll(x, 1, 1))


def row_up(x, row):
    n = x.shape[0]
    return jnp.where(iota(x.shape, 0) == n - 1, row, pltpu.roll(x, n - 1, 0))


def row_down(x, row):
    return jnp.where(iota(x.shape, 0) == 0, row, pltpu.roll(x, 1, 0))


def section_sums(n0, dn, d0, dd):
    n1, d1 = n0 + dn, d0 + dd
    ns, ds = n0 + n1, d0 + d1
    ends = d0 * d1
    inv = 1.0 / (ends * ds)
    half = ns * ends * inv
    side = ds * inv
    last = n1 * d0 * side
    first = n0 * d1 * side
    return (first + last) * (1.0 / 6.0) + half * (2.0 / 3.0), half * (1.0 / 3.0) + last * (1.0 / 6.0)


def energy(w, v, vt):
    return w * (v * v + v * vt + vt * vt * (1.0 / 3.0))


RGEO = 96
LGEO, LEN, LFLD = 40, 48, 64
(TH, THT, TH1, _, TU0, TU0T, TU1, TU1T, TU11, TU11T, TU2, TU2T, TU21, TU21T, TG2) = range(15)
(BH, BHT, BH1, _, BU0, BU0T, BU01, BU01T, BU1, BU1T, BU11, BU11T, BU2, BU2T, BG0) = range(15, 30)
RIM = ((0, 0), (1, 0), (2, 0), (2, 1), (0, -2), (0, -1), (1, -1), (2, -1))
RAW = 30 + 2 * len(RIM)


def pack_kernel(
    v, h, vt, ht, d, el, area, k, f, send_right, send_left, vo, ho, vto, hto, do, eo, ao, ko, fo, sems
):
    rows, cols = h.shape[1], h.shape[2]
    half = cols - 128
    started = []

    def start(src, dst):
        copy = pltpu.make_async_copy(src, dst, sems.at[len(started)])
        copy.start()
        started.append(copy)
        return copy

    fixed = [start(x, y) for x, y in ((d, do), (el, eo), (k, ko), (f, fo))]
    by_level = []
    for lev in range(0, LV, LV // 2):
        cut = slice(lev, lev + LV // 2)
        by_level.append([start(x.at[cut], y.at[cut]) for x, y in ((h, ho), (ht, hto))])
        by_level[-1] += [start(x.at[:, cut], y.at[:, cut]) for x, y in ((v, vo), (vt, vto))]
    area_copy = start(area, ao)
    for copy in fixed:
        copy.wait()

    lanes = iota((rows, 128), 1)

    def push(stack, x, wide=1, first=0):
        if stack is None:
            return x
        back = pltpu.roll(stack, 128 - wide, 1)
        return jnp.where(lanes == 127, x, back) if first else jnp.where(lanes < wide, x, back)

    def place(slab, stack, by, start, stop):
        moved = pltpu.roll(stack, by % 128, 1) if by % 128 else stack
        return jnp.where((lanes >= start) & (lanes < stop), moved, slab)

    def geometry(part):
        out = [ko[a, b, :, part] for a in range(2) for b in range(3)]
        return out + [(out[3 * a] + out[3 * a + 1] + out[3 * a + 2]) * fo[a, :, part] for a in range(2)]

    low, high = slice(0, 128), slice(half, cols)
    geo_left = geo_right = None
    for x, y in zip(geometry(low), geometry(high)):
        geo_left = push(geo_left, x)
        geo_right = push(geo_right, y, 1, 127)
    near = [do[e, :, low] for e in range(3)]
    far = [do[e, :, high] for e in range(3)]
    weight = [0.25 * far[e] * eo[e, :, high] for e in range(3)]
    left, right = [None] * 8, [None] * 10
    for lev in range(LV):
        if lev % (LV // 2) == 0:
            for copy in by_level[lev // (LV // 2)]:
                copy.wait()
        for part, dist, stacks in ((low, near, left), (high, far, right)):
            fields = [ho[lev, :, part], hto[lev, :, part]]
            fields += [dist[e] * x[e, lev, :, part] for e in range(3) for x in (vo, vto)]
            if part is high:
                fields += [energy(weight[e], vo[e, lev, :, part], vto[e, lev, :, part]) for e in (1, 2)]
            for n, x in enumerate(fields):
                stacks[n] = push(stacks[n], x, *((1, 127) if part is high else (2,) if n < 4 else (1,)))
    to_left = jnp.zeros((rows, 128), F32)
    to_right = right[7]
    for n in range(4):
        to_left = place(to_left, left[n], 16 * n + 14, 16 * n, 16 * n + 16)
        to_left = place(to_left, left[n + 4], 64 + LV * n + 7, 64 + LV * n, 72 + LV * n)
    to_left = place(to_left, geo_left, RGEO + 7, RGEO, RGEO + 8)
    for n in range(7):
        to_right = place(to_right, right[n], LFLD + LV * n - 120, LFLD + LV * n, LFLD + LV * n + LV)
    for n in range(2):
        to_right = place(to_right, right[8 + n], LEN + LV * n - 120, LEN + LV * n, LEN + LV * n + LV)
    to_right = place(to_right, geo_right, LGEO - 120, LGEO, LGEO + 8)
    send_right[...] = to_right
    send_left[...] = to_left
    area_copy.wait()


PACK_COPIES = 4 + 4 * 2 + 1


def vertex_kernel(v, h, vt, ht, d, el, area, k, f, raw, geo, q):
    rows = h.shape[1]
    end = rows - 1
    for x, n in ((h, TH), (ht, THT)):
        raw[n] = x[:, 0, :]
        raw[n + 2] = x[:, 1, :]
    for x, n in ((h, BH), (ht, BHT)):
        raw[n] = x[:, end, :]
        raw[n + 2] = x[:, end - 1, :]
    for x, t in ((v, 0), (vt, 1)):
        for e, r, n in (
            (0, 0, TU0),
            (1, 0, TU1),
            (1, 1, TU11),
            (2, 0, TU2),
            (2, 1, TU21),
            (0, end, BU0),
            (0, end - 1, BU01),
            (1, end, BU1),
            (1, end - 1, BU11),
            (2, end, BU2),
        ):
            raw[n + t] = d[e, r : r + 1, :] * x[e, :, r, :]
    for e, r, n in ((2, 0, TG2), (0, end, BG0)):
        raw[n] = jnp.broadcast_to(0.25 * el[e, r : r + 1, :] / d[e, r : r + 1, :], raw.shape[1:])
    for a in range(2):
        geo[a] = (k[a, 0] + k[a, 1] + k[a, 2]) * f[a]
    for e in range(3):
        geo[2 + e] = (1.0 / 12.0) / d[e]
        geo[5 + e] = 0.25 * d[e] * el[e]
    geo[8] = 1.0 / area[...]
    for n, (e, r) in enumerate(RIM):
        for x, t in ((v, 0), (vt, 1)):
            raw[30 + 2 * n + t] = x[e, :, r % rows, :]

    up = lambda x: pltpu.roll(x, rows - 1, 0)
    dn = lambda x: pltpu.roll(x, 1, 0)
    right = lambda x: pltpu.roll(x, x.shape[1] - 1, 1)
    for lev in range(LV):
        hh = [x[lev] for x in (h, ht)]
        u = [[d[e] * x[e, lev] for x in (v, vt)] for e in range(3)]
        h1 = [right(x) for x in hh]
        u01 = [right(x) for x in u[0]]
        n0 = [u[0][t] - u[1][t] + up(u[2][t]) for t in range(2)]
        n1 = [u[1][t] - u[2][t] - dn(u01[t]) for t in range(2)]
        d0 = [k[0, 0] * hh[t] + k[0, 1] * up(hh[t]) + k[0, 2] * h1[t] for t in range(2)]
        d1 = [k[1, 0] * hh[t] + k[1, 1] * h1[t] + k[1, 2] * dn(h1[t]) for t in range(2)]
        q0 = section_sums(geo[0] + n0[0], n0[1], *d0)
        q1 = section_sums(geo[1] + n1[0], n1[1], *d1)
        for t in range(2):
            q[t, 0, lev] = q0[t]
            q[t, 1, lev] = q1[t]


def af_row(k, f, a, r):
    return (k[a, 0, r : r + 1, :] + k[a, 1, r : r + 1, :] + k[a, 2, r : r + 1, :]) * f[a, r : r + 1, :]


def left_field(t, n):
    return t[LFLD + LV * n : LFLD + LV * n + LV, :]


def right_field(t, n, c=0):
    if n >= 4:
        return t[32 + LV * n : 32 + LV * n + LV, :]
    return t[pl.ds(16 * n + c, LV, stride=2), :]


def column_left(lt, h0, h0t, u00, u00t):
    k = [lt[LGEO + n : LGEO + n + 1, :] for n in range(8)]
    up = lambda x: pltpu.roll(x, 127, 1)
    dn = lambda x: pltpu.roll(x, 1, 1)
    h, hp, u0, u0p, u1, u1p, u2, u2p = (left_field(lt, n) for n in range(8))
    q0 = section_sums(
        k[6] + u0 - u1 + up(u2),
        u0p - u1p + up(u2p),
        k[0] * h + k[1] * up(h) + k[2] * h0,
        k[0] * hp + k[1] * up(hp) + k[2] * h0t,
    )
    q1 = section_sums(
        k[7] + u1 - u2 - dn(u00),
        u1p - u2p - dn(u00t),
        k[3] * h + k[4] * h0 + k[5] * dn(h0),
        k[3] * hp + k[4] * h0t + k[5] * dn(h0t),
    )
    return q0, q1


def column_right(rt):
    k = [rt[RGEO + n : RGEO + n + 1, :] for n in range(8)]
    up = lambda x: pltpu.roll(x, 127, 1)
    dn = lambda x: pltpu.roll(x, 1, 1)
    h, hp, u0, u0p, u1, u1p, u2, u2p = (right_field(rt, n) for n in range(8))
    h1, h1p, u01, u01p = (right_field(rt, n, 1) for n in range(4))
    q0 = section_sums(
        k[6] + u0 - u1 + up(u2),
        u0p - u1p + up(u2p),
        k[0] * h + k[1] * up(h) + k[2] * h1,
        k[0] * hp + k[1] * up(hp) + k[2] * h1p,
    )
    q1 = section_sums(
        k[7] + u1 - u2 - dn(u01),
        u1p - u2p - dn(u01p),
        k[3] * h + k[4] * h1 + k[5] * dn(h1),
        k[3] * hp + k[4] * h1p + k[5] * dn(h1p),
    )
    return q0, q1


def lane_col(x, lane):
    return x[:, lane : lane + 1]


def merge_kernel(slab_l, slab_r, own0, raw, k, f, msg_a, msg_b, ext, turned):
    odd_y = lax.rem(lax.axis_index("py"), 2) == 1
    rows = slab_l.shape[0]
    end = rows - 1
    left, right = slab_l[...], slab_r[...]
    ext[0, BASE : BASE + rows, :] = left
    ext[1, BASE : BASE + rows, :] = right
    ext[2, BASE : BASE + rows, :] = own0[...]
    lt, rt, ot = turn(turned, *(ext[n] for n in range(3)))
    q0l, q1l = column_left(lt, *(right_field(ot, n) for n in range(4)))
    q0r, q1r = column_right(rt)
    r0, r1 = BASE, BASE + 1
    e0, e1 = BASE + end, BASE + end - 1
    krow = lambda a, b, r: k[a, b, r : r + 1, :]

    h_0 = [left_shift(raw[TH + t], lane_col(right_field(rt, t), r0)) for t in range(2)]
    h_1 = [left_shift(raw[TH1 + t], lane_col(right_field(rt, t), r1)) for t in range(2)]
    u_0 = [left_shift(raw[TU0 + t], lane_col(right_field(rt, 2 + t), r0)) for t in range(2)]
    up0 = section_sums(
        af_row(k, f, 0, 0) + raw[TU0] - raw[TU1] + raw[TU21],
        raw[TU0T] - raw[TU1T] + raw[TU21T],
        *(krow(0, 0, 0) * raw[TH + t] + krow(0, 1, 0) * raw[TH1 + t] + krow(0, 2, 0) * h_0[t] for t in range(2)),
    )
    up1 = section_sums(
        af_row(k, f, 1, 1) + raw[TU11] - raw[TU21] - u_0[0],
        raw[TU11T] - raw[TU21T] - u_0[1],
        *(krow(1, 0, 1) * raw[TH1 + t] + krow(1, 1, 1) * h_1[t] + krow(1, 2, 1) * h_0[t] for t in range(2)),
    )
    up = [
        up0[t] + right_shift(up0[t] + up1[t], lane_col(q0l[t], r0) + lane_col(q1l[t], r1)) for t in range(2)
    ]

    hb_0 = [left_shift(raw[BH + t], lane_col(right_field(rt, t), e0)) for t in range(2)]
    hb_1 = [left_shift(raw[BH1 + t], lane_col(right_field(rt, t), e1)) for t in range(2)]
    ub_1 = [left_shift(raw[BU01 + t], lane_col(right_field(rt, 2 + t), e1)) for t in range(2)]
    dn1 = section_sums(
        af_row(k, f, 1, end) + raw[BU1] - raw[BU2] - ub_1[0],
        raw[BU1T] - raw[BU2T] - ub_1[1],
        *(krow(1, 0, end) * raw[BH + t] + krow(1, 1, end) * hb_0[t] + krow(1, 2, end) * hb_1[t] for t in range(2)),
    )
    dn0 = section_sums(
        af_row(k, f, 0, end - 1) + raw[BU01] - raw[BU11] + raw[BU2],
        raw[BU01T] - raw[BU11T] + raw[BU2T],
        *(
            krow(0, 0, end - 1) * raw[BH1 + t] + krow(0, 1, end - 1) * raw[BH + t] + krow(0, 2, end - 1) * hb_1[t]
            for t in range(2)
        ),
    )
    down = [
        left_shift(dn1[t] + dn0[t], lane_col(q1r[t], e0) + lane_col(q0r[t], e1)) + dn1[t] for t in range(2)
    ]

    def store(msg_up, msg_down):
        for msg, sums, parts, geo, r in (
            (msg_up, up, (TH, THT, TU1, TU1T, TU2, TU2T, TG2), 1, 0),
            (msg_down, down, (BH, BHT, BU0, BU0T, BU1, BU1T, BG0), 0, end),
        ):
            for n in range(2):
                msg[LV * n : LV * n + LV, :] = sums[n]
            for n, part in enumerate(parts[:6]):
                msg[LV * (n + 2) : LV * (n + 3), :] = raw[part]
            for n in range(3):
                msg[64 + n : 65 + n, :] = krow(geo, n, r)
            msg[67:68, :] = af_row(k, f, geo, r)
            msg[68:69, 0:128] = left[r : r + 1, :]
            msg[68:69, 128:256] = right[r : r + 1, :]
            msg[69:70, :] = raw[parts[6], 0:1, :]
            msg[70:72, :] = jnp.zeros((2, msg.shape[1]), F32)

    @pl.when(odd_y)
    def _():
        store(msg_a, msg_b)

    @pl.when(jnp.logical_not(odd_y))
    def _():
        store(msg_b, msg_a)


(CY, _, CQ, CZ, CP, _, C0, _, C1, _) = range(10)
(K00, _, K11, _, K0B, _, K1E, _, KM1, _, KMB, _, KMR, _) = range(14)


def turn(turned, *slabs):
    for n, x in enumerate(slabs):
        turned[n] = jnp.transpose(x)
    return [turned.at[n] for n in range(len(slabs))]


def middle_kernel(parity, *refs):
    @pl.when(lax.rem(lax.axis_index("py"), 2) == parity)
    def _():
        middle(*refs[:8], *refs[-7:])


def middle(v, vt, geo, q, slab_l, slab_r, own_l, own_r, vertex, kinetic, cell, edge, keep, ext, turned):
    rows = kinetic.shape[1]
    end = rows - 1
    for n, x in enumerate((slab_l, slab_r, own_l, own_r)):
        ext[n, BASE : BASE + rows, :] = x[...]
    lt, rt, ot, et = turn(turned, *(ext[n] for n in range(4)))
    q0l, q1l = column_left(lt, *(right_field(ot, n) for n in range(4)))
    q0r, q1r = column_right(rt)
    q0c, q1c = column_left(et, *(right_field(rt, n) for n in range(4)))
    up = lambda x: pltpu.roll(x, 127, 1)
    dn = lambda x: pltpu.roll(x, 1, 1)
    columns = [
        q0l[0] + q1l[0] + up(q1l[0]),
        q0l[1] + q1l[1] + up(q1l[1]),
        up(q1l[0]),
        lt[LEN : LEN + LV, :] + jnp.where(iota((LV, 128), 1) < BASE + end, up(lt[LEN + LV : LEN + 2 * LV, :]), 0.0),
        q0r[0] + q1r[0] + dn(q0r[0]),
        q0r[1] + q1r[1] + dn(q0r[1]),
        *q0c,
        *q1c,
    ]
    packed = jnp.concatenate(columns + [jnp.zeros((128 - LV * len(columns), 128), F32)], axis=0)
    inject = jnp.transpose(packed)[BASE : BASE + rows, :]
    moving = [pltpu.roll(inject, ((0 if n <= CZ else 127) - LV * n) % 128, 1) for n in range(len(columns))]
    side = iota(kinetic.shape[1:], 1)
    final = kinetic.shape[2] - 1
    for lev in range(LV):
        if lev:
            moving = [pltpu.roll(x, 127, 1) for x in moving]
        col = lambda n: jnp.concatenate([moving[n]] * 2, axis=1)
        put = lambda n, x, r, lev=lev: keep.__setitem__((n, slice(lev, lev + 1), slice(None)), x[r : r + 1, :])
        grads = []
        for t in range(2):
            q0 = jnp.where(side == final, col(C0 + t), q[t, 0, lev])
            q1 = jnp.where(side == final, col(C1 + t), q[t, 1, lev])
            q0d = pltpu.roll(q0, 1, 0)
            q1u = pltpu.roll(q1, end, 0)
            both = q0 + q1
            p, y = both + q0d, both + q1u
            m = p + right_shift(y, col(CY + t))
            m1 = left_shift(p, col(CP + t)) + y
            grads.append((pltpu.roll(m, end, 0) - m, m1 - m, pltpu.roll(m1, 1, 0) - m))
            put(K00 + t, q0, 0)
            put(K11 + t, q1, 1)
            put(K0B + t, q0, end - 1)
            put(K1E + t, q1, end)
            put(KM1 + t, m, 1)
            put(KMB + t, m, end - 1)
            put(KMR + t, m1, end - 1)
            if t == 0:
                cell[lev] = m * (1.0 / 6.0)
                vertex[0, lev] = q0
                vertex[1, lev] = q1
                means = (q0 + right_shift(q1u, col(CQ)), both, q1 + q0d)
        for e in range(3):
            edge[e, lev] = 0.5 * means[e] - geo[2 + e] * (v[e, lev] * grads[0][e] + vt[e, lev] * grads[1][e])
        en = [energy(geo[5 + e], v[e, lev], vt[e, lev]) for e in range(3)]
        zz = right_shift(en[1] + row_up(en[2], 0.0), col(CZ))
        kinetic[lev] = (en[0] + en[1] + en[2] + row_down(en[0], 0.0) + zz) * geo[8]


def last_kernel(
    k, f, geo, slab_l, slab_r, own0, raw, keep, vertex_v, kinetic_v, cell_v, edge_v, msg_a, msg_b,
    vertex, kinetic, cell, edge, ext, turned, msgs, rim, tiles, sems,
):
    odd_y = lax.rem(lax.axis_index("py"), 2) == 1
    rows = kinetic_v.shape[1]
    end = rows - 1
    arrays = (
        [(vertex_v.at[n], vertex.at[n]) for n in range(2)]
        + [(kinetic_v, kinetic), (cell_v, cell)]
        + [(edge_v.at[n], edge.at[n]) for n in range(3)]
    )
    copies = []

    def start(src, dst):
        copy = pltpu.make_async_copy(src, dst, sems.at[len(copies)])
        copy.start()
        copies.append(copy)

    top, bottom = slice(0, 8), slice(rows - 8, rows)
    for n, (src, dst) in enumerate(arrays):
        inner = slice(0 if n == 0 else 8, rows if n == 1 else rows - 8)
        start(src.at[:, inner], dst.at[:, inner])

    @pl.when(odd_y)
    def _():
        msgs[0] = msg_b[...]
        msgs[1] = msg_a[...]

    @pl.when(jnp.logical_not(odd_y))
    def _():
        msgs[0] = msg_a[...]
        msgs[1] = msg_b[...]

    above = lambda n: msgs[0, LV * n : LV * n + LV, :]
    below = lambda n: msgs[1, LV * n : LV * n + LV, :]
    ka = [msgs[0, 64 + n : 65 + n, :] for n in range(4)]
    kb = [msgs[1, 64 + n : 65 + n, :] for n in range(4)]
    krow = lambda a, b, r: k[a, b, r : r + 1, :]

    for n, x in enumerate((slab_l, slab_r, own0)):
        ext[n, BASE : BASE + rows, :] = x[...]
    ext[0, DNB : DNB + 1, :] = msgs[0, 68:69, 0:128]
    ext[1, DNB : DNB + 1, :] = msgs[0, 68:69, 128:256]
    ext[1, UPB : UPB + 1, :] = msgs[1, 68:69, 128:256]
    lt, rt, ot = turn(turned, *(ext[n] for n in range(3)))
    lanes = iota((LV, 128), 1)
    low = lambda x, row: jnp.where(lanes == UPB, row[:, 0:1], x)
    high = lambda x, row: jnp.where(lanes == DNB, row[:, 0:1], x)
    h0 = [high(low(right_field(ot, t), below(2 + t)), above(2 + t)) for t in range(2)]
    u00 = [low(right_field(ot, 2 + t), below(4 + t)) for t in range(2)]
    q0l, q1l = column_left(lt, *h0, *u00)
    q0r, q1r = column_right(rt)
    up = lambda x: pltpu.roll(x, 127, 1)
    dn = lambda x: pltpu.roll(x, 1, 1)
    ycol = [q0l[t] + q1l[t] + up(q1l[t]) for t in range(2)]
    pcol = [q0r[t] + q1r[t] + dn(q0r[t]) for t in range(2)]
    r0, re = BASE, BASE + end

    hb1 = [left_shift(below(2 + t), lane_col(right_field(rt, t), UPB)) for t in range(2)]
    ub1 = [left_shift(below(4 + t), lane_col(right_field(rt, 2 + t), UPB)) for t in range(2)]
    h01 = [left_shift(raw[TH + t], lane_col(right_field(rt, t), BASE)) for t in range(2)]
    qb = section_sums(
        kb[3] + below(4) - below(6) + raw[TU2],
        below(5) - below(7) + raw[TU2T],
        *(kb[0] * below(2 + t) + kb[1] * raw[TH + t] + kb[2] * hb1[t] for t in range(2)),
    )
    q1f = section_sums(
        af_row(k, f, 1, 0) + raw[TU1] - raw[TU2] - ub1[0],
        raw[TU1T] - raw[TU2T] - ub1[1],
        *(krow(1, 0, 0) * raw[TH + t] + krow(1, 1, 0) * h01[t] + krow(1, 2, 0) * hb1[t] for t in range(2)),
    )
    ha1 = [left_shift(above(2 + t), lane_col(right_field(rt, t), DNB)) for t in range(2)]
    he1 = [left_shift(raw[BH + t], lane_col(right_field(rt, t), re)) for t in range(2)]
    ue1 = [left_shift(raw[BU0 + t], lane_col(right_field(rt, 2 + t), re)) for t in range(2)]
    qa = section_sums(
        ka[3] + above(4) - above(6) - ue1[0],
        above(5) - above(7) - ue1[1],
        *(ka[0] * above(2 + t) + ka[1] * ha1[t] + ka[2] * he1[t] for t in range(2)),
    )
    q0e = section_sums(
        af_row(k, f, 0, end) + raw[BU0] - raw[BU1] + above(6),
        raw[BU0T] - raw[BU1T] + above(7),
        *(krow(0, 0, end) * raw[BH + t] + krow(0, 1, end) * above(2 + t) + krow(0, 2, end) * he1[t] for t in range(2)),
    )
    grads = []
    for t in range(2):
        p0, y0 = keep[K00 + t] + q1f[t] + qb[t], keep[K00 + t] + q1f[t] + keep[K11 + t]
        pe, ye = q0e[t] + keep[K1E + t] + keep[K0B + t], q0e[t] + keep[K1E + t] + qa[t]
        m0 = p0 + right_shift(y0, lane_col(ycol[t], r0))
        m0r = left_shift(p0, lane_col(pcol[t], r0)) + y0
        me = pe + right_shift(ye, lane_col(ycol[t], re))
        mer = left_shift(pe, lane_col(pcol[t], re)) + ye
        m_above = above(t) + qa[t] + right_shift(qa[t], lane_col(q1l[t], DNB)) + q0e[t]
        m_below = below(t) + qb[t] + left_shift(qb[t], lane_col(q0r[t], UPB)) + q1f[t]
        grads.append(
            (
                keep[KM1 + t] - m0,
                m0r - m0,
                m_below - m0,
                m0r - keep[KM1 + t],
                me - keep[KMB + t],
                m_above - me,
                mer - me,
                keep[KMR + t] - me,
            )
        )
        if t == 0:
            rim[8] = q1f[0]
            rim[9] = m0 * (1.0 / 6.0)
            rim[10] = q0e[0]
            rim[11] = me * (1.0 / 6.0)
            means = (
                keep[K00] + right_shift(keep[K11], lane_col(q1l[0], r0 + 1)),
                keep[K00] + q1f[0],
                q1f[0] + qb[0],
                keep[K11] + keep[K00],
                keep[K0B] + right_shift(keep[K1E], lane_col(q1l[0], re)),
                q0e[0] + right_shift(qa[0], lane_col(q1l[0], DNB)),
                q0e[0] + keep[K1E],
                keep[K1E] + keep[K0B],
            )
    for n, (e, r) in enumerate(RIM):
        r = r % rows
        rim[n] = 0.5 * means[n] - geo[2 + e, r : r + 1, :] * (
            raw[30 + 2 * n] * grads[0][n] + raw[31 + 2 * n] * grads[1][n]
        )
    rim[12] = energy(msgs[1, 69:70, :], below(4), below(5)) * geo[8, 0:1, :]
    rim[13] = right_shift(energy(msgs[0, 69:70, :], above(6), above(7)), lane_col(lt[LEN + LV : LEN + 2 * LV, :], DNB)) * geo[8, end : end + 1, :]

    spot = iota((8, kinetic_v.shape[2]), 0)
    tile = 0
    for part, patches in (
        (top, ((1, ((0, 8),)), (2, ((0, 12),)), (3, ((0, 9),)), (4, ((0, 0),)), (5, ((0, 1),)), (6, ((0, 2), (1, 3))))),
        (bottom, ((0, ((7, 10),)), (2, ((7, 13),)), (3, ((7, 11),)), (4, ((6, 4), (7, 5))), (5, ((7, 6),)), (6, ((7, 7),)))),
    ):
        for n, changes in patches:
            src, dst = arrays[n]
            for lev in range(LV):
                x = src[lev, part, :]
                for r, m in changes:
                    new = rim[m, lev : lev + 1, :]
                    x = jnp.where(spot == r, x + new if n == 2 else new, x)
                tiles[tile, lev] = x
            start(tiles.at[tile], dst.at[:, part])
            tile += 1
    for copy in copies:
        copy.wait()


LAST_COPIES = 7 + 12


def shift(x, axis, by):
    n = lax.axis_size(axis)
    return lax.ppermute(x, axis, [(i, (i + by) % n) for i in range(n)])


def swap(x, axis, start):
    n = lax.axis_size(axis)
    pairs = []
    for i in range(start, n + start, 2):
        a, b = i % n, (i + 1) % n
        pairs += [(a, b), (b, a)]
    return lax.ppermute(x, axis, pairs)


VM = pl.BlockSpec(memory_space=pltpu.VMEM)
ANY = pl.BlockSpec(memory_space=pl.ANY)


def call(kernel, args, outs, scratch=(), sems=0, hbm_in=False, hbm_out=False, flops=0, alias=None):
    args = [pltpu.with_memory_space_constraint(x, pltpu.HBM if hbm_in else pltpu.VMEM) for x in args]
    shape = (lambda s: jax.ShapeDtypeStruct(s, F32)) if hbm_out else (lambda s: pltpu.VMEM(s, F32))
    return pl.pallas_call(
        kernel,
        out_shape=[shape(s) for s in outs],
        in_specs=[ANY if hbm_in else VM] * len(args),
        out_specs=[ANY if hbm_out else VM] * len(outs),
        scratch_shapes=[pltpu.VMEM(s, F32) for s in scratch]
        + ([pltpu.SemaphoreType.DMA((sems,))] if sems else []),
        input_output_aliases=alias or {},
        compiler_params=pltpu.CompilerParams(vmem_limit_bytes=16 * 2**20),
        cost_estimate=pl.CostEstimate(flops=flops, transcendentals=0, bytes_accessed=0) if flops else None,
    )(*args)


def step(*args):
    levels, rows, cols = args[1].shape
    slab = (rows, 128)
    send_right, send_left, *held = call(
        pack_kernel, args, [slab, slab] + [x.shape for x in args], sems=PACK_COPIES, hbm_in=True
    )
    v, _, vt, _, _, _, _, k, f = held
    slab_l = shift(send_right, "px", 1)
    slab_r = shift(send_left, "px", -1)
    whole = [(2, levels, rows, cols), (levels, rows, cols), (levels, rows, cols), (3, levels, rows, cols)]
    raw, geo, q = call(
        vertex_kernel,
        held,
        [(RAW, levels, cols), (9, rows, cols), (2, 2, levels, rows, cols)],
        flops=40_000_000,
    )
    turned = [(4, 128, 128), (4, 128, 128)]
    msg_a, msg_b = call(
        merge_kernel, [slab_l, slab_r, send_left, raw, k, f], [(72, cols), (72, cols)], turned
    )
    msg_b = swap(msg_b, "py", 1)
    msg_a = swap(msg_a, "py", 0)
    sources = [v, vt, geo, q, slab_l, slab_r, send_left, send_right]
    results = whole + [(14, levels, cols)]
    parts = call(functools.partial(middle_kernel, 1), sources, results, turned, flops=40_000_000)
    *parts, keep = call(
        functools.partial(middle_kernel, 0),
        [*sources, *parts],
        results,
        turned,
        flops=40_000_000,
        alias={len(sources) + n: n for n in range(5)},
    )
    return tuple(
        call(
            last_kernel,
            [k, f, geo, slab_l, slab_r, send_left, raw, keep, *parts, msg_a, msg_b],
            whole,
            turned + [(2, 72, cols), (14, levels, cols), (12, levels, 8, cols)],
            sems=LAST_COPIES,
            hbm_out=True,
        )
    )


def solution(mesh):
    field = P(None, "py", "px")
    pair = P(None, None, "py", "px")
    return jax.shard_map(
        step,
        mesh=mesh,
        in_specs=(pair, field, pair, field, field, field, P("py", "px"), pair, field),
        out_specs=(pair, field, field, pair),
        check_vma=False,
    )
```

```python
import functools

import jax
import jax.numpy as jnp
from jax import lax
from jax.experimental import pallas as pl
from jax.experimental.pallas import tpu as pltpu
from jax.sharding import PartitionSpec as P

F32 = jnp.float32
LV = 8
BASE = 8
UPB, DNB = BASE - 1, BASE + 32
OWN = 64


def iota(shape, dim):
    return lax.broadcasted_iota(jnp.int32, shape, dim)


def left_shift(x, col):
    n = x.shape[1]
    return jnp.where(iota(x.shape, 1) == n - 1, col, pltpu.roll(x, n - 1, 1))


def right_shift(x, col):
    return jnp.where(iota(x.shape, 1) == 0, col, pltpu.roll(x, 1, 1))


def row_up(x, row):
    n = x.shape[0]
    return jnp.where(iota(x.shape, 0) == n - 1, row, pltpu.roll(x, n - 1, 0))


def row_down(x, row):
    return jnp.where(iota(x.shape, 0) == 0, row, pltpu.roll(x, 1, 0))


def section_sums(n0, dn, d0, dd):
    n1, d1 = n0 + dn, d0 + dd
    ns, ds = n0 + n1, d0 + d1
    ends = d0 * d1
    inv = 1.0 / (ends * ds)
    half = ns * ends * inv
    side = ds * inv
    last = n1 * d0 * side
    first = n0 * d1 * side
    return (first + last) * (1.0 / 6.0) + half * (2.0 / 3.0), half * (1.0 / 3.0) + last * (1.0 / 6.0)


def energy(w, v, vt):
    return w * (v * v + v * vt + vt * vt * (1.0 / 3.0))


RGEO = 96
LGEO, LEN, LFLD = 40, 48, 64
(TH, THT, _, _, TU0, _, TU1, TU1T, TU11, _, TU2, TU2T, TU21, _, TG2) = range(15)
(BH, BHT, _, _, BU0, BU0T, BU01, _, BU1, BU1T, BU11, _, BU2, _, BG0) = range(15, 30)
RIM = ((0, 0), (1, 0), (2, 0), (2, 1), (0, -2), (0, -1), (1, -1), (2, -1))
QROW = 30 + 2 * len(RIM)
RAW = QROW + 8


def pack_kernel(
    v, h, vt, ht, d, el, area, k, f, send_right, send_left, vo, ho, vto, hto, do, eo, ao, ko, fo, sems
):
    rows, cols = h.shape[1], h.shape[2]
    half = cols - 128
    started = []

    def start(src, dst):
        copy = pltpu.make_async_copy(src, dst, sems.at[len(started)])
        copy.start()
        started.append(copy)
        return copy

    fixed = [start(x, y) for x, y in ((d, do), (el, eo), (k, ko), (f, fo))]
    by_level = []
    for lev in range(0, LV, LV // 2):
        cut = slice(lev, lev + LV // 2)
        by_level.append([start(x.at[cut], y.at[cut]) for x, y in ((h, ho), (ht, hto))])
        by_level[-1] += [start(x.at[:, cut], y.at[:, cut]) for x, y in ((v, vo), (vt, vto))]
    area_copy = start(area, ao)
    for copy in fixed:
        copy.wait()

    lanes = iota((rows, 128), 1)

    def push(stack, x, wide=1, first=0):
        if stack is None:
            return x
        back = pltpu.roll(stack, 128 - wide, 1)
        return jnp.where(lanes == 127, x, back) if first else jnp.where(lanes < wide, x, back)

    def place(slab, stack, by, start, stop):
        moved = pltpu.roll(stack, by % 128, 1) if by % 128 else stack
        return jnp.where((lanes >= start) & (lanes < stop), moved, slab)

    def geometry(part):
        out = [ko[a, b, :, part] for a in range(2) for b in range(3)]
        return out + [(out[3 * a] + out[3 * a + 1] + out[3 * a + 2]) * fo[a, :, part] for a in range(2)]

    low, high = slice(0, 128), slice(half, cols)
    geo_left = geo_right = None
    for x, y in zip(geometry(low), geometry(high)):
        geo_left = push(geo_left, x)
        geo_right = push(geo_right, y, 1, 127)
    near = [do[e, :, low] for e in range(3)]
    far = [do[e, :, high] for e in range(3)]
    weight = [0.25 * far[e] * eo[e, :, high] for e in range(3)]
    left, right = [None] * 8, [None] * 10
    for lev in range(LV):
        if lev % (LV // 2) == 0:
            for copy in by_level[lev // (LV // 2)]:
                copy.wait()
        for part, dist, stacks in ((low, near, left), (high, far, right)):
            fields = [ho[lev, :, part], hto[lev, :, part]]
            fields += [dist[e] * x[e, lev, :, part] for e in range(3) for x in (vo, vto)]
            if part is high:
                fields += [energy(weight[e], vo[e, lev, :, part], vto[e, lev, :, part]) for e in (1, 2)]
            for n, x in enumerate(fields):
                stacks[n] = push(stacks[n], x, *((1, 127) if part is high else (2,) if n < 4 else (1,)))
    to_left = jnp.zeros((rows, 128), F32)
    to_right = right[7]
    for n in range(4):
        to_left = place(to_left, left[n], 16 * n + 14, 16 * n, 16 * n + 16)
        to_left = place(to_left, left[n + 4], 64 + LV * n + 7, 64 + LV * n, 72 + LV * n)
    to_left = place(to_left, geo_left, RGEO + 7, RGEO, RGEO + 8)
    for n in range(7):
        to_right = place(to_right, right[n], LFLD + LV * n - 120, LFLD + LV * n, LFLD + LV * n + LV)
    for n in range(2):
        to_right = place(to_right, right[8 + n], LEN + LV * n - 120, LEN + LV * n, LEN + LV * n + LV)
    to_right = place(to_right, geo_right, LGEO - 120, LGEO, LGEO + 8)
    send_right[...] = to_right
    send_left[...] = to_left
    area_copy.wait()


PACK_COPIES = 4 + 4 * 2 + 1


def vertex_kernel(v, h, vt, ht, d, el, area, k, f, raw, geo, q, msg_a, msg_b):
    rows = h.shape[1]
    end = rows - 1
    for x, n in ((h, TH), (ht, THT)):
        raw[n] = x[:, 0, :]
        raw[n + 2] = x[:, 1, :]
    for x, n in ((h, BH), (ht, BHT)):
        raw[n] = x[:, end, :]
        raw[n + 2] = x[:, end - 1, :]
    for x, t in ((v, 0), (vt, 1)):
        for e, r, n in (
            (0, 0, TU0),
            (1, 0, TU1),
            (1, 1, TU11),
            (2, 0, TU2),
            (2, 1, TU21),
            (0, end, BU0),
            (0, end - 1, BU01),
            (1, end, BU1),
            (1, end - 1, BU11),
            (2, end, BU2),
        ):
            raw[n + t] = d[e, r : r + 1, :] * x[e, :, r, :]
    for e, r, n in ((2, 0, TG2), (0, end, BG0)):
        raw[n] = jnp.broadcast_to(0.25 * el[e, r : r + 1, :] / d[e, r : r + 1, :], raw.shape[1:])
    for a in range(2):
        geo[a] = (k[a, 0] + k[a, 1] + k[a, 2]) * f[a]
    for e in range(3):
        geo[2 + e] = (1.0 / 12.0) / d[e]
        geo[5 + e] = 0.25 * d[e] * el[e]
    geo[8] = 1.0 / area[...]
    for n, (e, r) in enumerate(RIM):
        for x, t in ((v, 0), (vt, 1)):
            raw[30 + 2 * n + t] = x[e, :, r % rows, :]

    up = lambda x: pltpu.roll(x, rows - 1, 0)
    dn = lambda x: pltpu.roll(x, 1, 0)
    right = lambda x: pltpu.roll(x, x.shape[1] - 1, 1)
    for lev in range(LV):
        hh = [x[lev] for x in (h, ht)]
        u = [[d[e] * x[e, lev] for x in (v, vt)] for e in range(3)]
        h1 = [right(x) for x in hh]
        u01 = [right(x) for x in u[0]]
        n0 = [u[0][t] - u[1][t] + up(u[2][t]) for t in range(2)]
        n1 = [u[1][t] - u[2][t] - dn(u01[t]) for t in range(2)]
        d0 = [k[0, 0] * hh[t] + k[0, 1] * up(hh[t]) + k[0, 2] * h1[t] for t in range(2)]
        d1 = [k[1, 0] * hh[t] + k[1, 1] * h1[t] + k[1, 2] * dn(h1[t]) for t in range(2)]
        q0 = section_sums(geo[0] + n0[0], n0[1], *d0)
        q1 = section_sums(geo[1] + n1[0], n1[1], *d1)
        for t in range(2):
            q[t, 0, lev] = q0[t]
            q[t, 1, lev] = q1[t]
            for n, x, r in ((0, q0, 0), (1, q1, 1), (2, q1, end), (3, q0, end - 1)):
                raw[QROW + 2 * n + t, lev : lev + 1, :] = x[t][r : r + 1, :]

    def fill(msg_up, msg_down):
        for msg, parts, a, r in (
            (msg_up, (TH, THT, TU1, TU1T, TU2, TU2T), 1, 0),
            (msg_down, (BH, BHT, BU0, BU0T, BU1, BU1T), 0, end),
        ):
            for n, part in enumerate(parts):
                msg[LV * (n + 2) : LV * (n + 3), :] = raw[part]
            for n in range(3):
                msg[64 + n : 65 + n, :] = k[a, n, r : r + 1, :]
            msg[67:68, :] = af_row(k, f, a, r)
            msg[69:70, :] = raw[BG0 if r else TG2, 0:1, :]
            msg[70:72, :] = jnp.zeros((2, msg.shape[1]), F32)

    by_parity(fill, msg_a, msg_b)


def by_parity(body, first, second):
    odd = lax.rem(lax.axis_index("py"), 2) == 1

    @pl.when(odd)
    def _():
        body(first, second)

    @pl.when(jnp.logical_not(odd))
    def _():
        body(second, first)


def af_row(k, f, a, r):
    return (k[a, 0, r : r + 1, :] + k[a, 1, r : r + 1, :] + k[a, 2, r : r + 1, :]) * f[a, r : r + 1, :]


def left_field(t, n):
    return t[LFLD + LV * n : LFLD + LV * n + LV, :]


def right_field(t, n, c=0):
    if n >= 4:
        return t[32 + LV * n : 32 + LV * n + LV, :]
    return t[pl.ds(16 * n + c, LV, stride=2), :]


def column_left(lt, h0, h0t, u00, u00t):
    k = [lt[LGEO + n : LGEO + n + 1, :] for n in range(8)]
    up = lambda x: pltpu.roll(x, 127, 1)
    dn = lambda x: pltpu.roll(x, 1, 1)
    h, hp, u0, u0p, u1, u1p, u2, u2p = (left_field(lt, n) for n in range(8))
    q0 = section_sums(
        k[6] + u0 - u1 + up(u2),
        u0p - u1p + up(u2p),
        k[0] * h + k[1] * up(h) + k[2] * h0,
        k[0] * hp + k[1] * up(hp) + k[2] * h0t,
    )
    q1 = section_sums(
        k[7] + u1 - u2 - dn(u00),
        u1p - u2p - dn(u00t),
        k[3] * h + k[4] * h0 + k[5] * dn(h0),
        k[3] * hp + k[4] * h0t + k[5] * dn(h0t),
    )
    return q0, q1


def column_right(rt):
    k = [rt[RGEO + n : RGEO + n + 1, :] for n in range(8)]
    up = lambda x: pltpu.roll(x, 127, 1)
    dn = lambda x: pltpu.roll(x, 1, 1)
    h, hp, u0, u0p, u1, u1p, u2, u2p = (right_field(rt, n) for n in range(8))
    h1, h1p, u01, u01p = (right_field(rt, n, 1) for n in range(4))
    q0 = section_sums(
        k[6] + u0 - u1 + up(u2),
        u0p - u1p + up(u2p),
        k[0] * h + k[1] * up(h) + k[2] * h1,
        k[0] * hp + k[1] * up(hp) + k[2] * h1p,
    )
    q1 = section_sums(
        k[7] + u1 - u2 - dn(u01),
        u1p - u2p - dn(u01p),
        k[3] * h + k[4] * h1 + k[5] * dn(h1),
        k[3] * hp + k[4] * h1p + k[5] * dn(h1p),
    )
    return q0, q1


def moved(x, lane, to):
    y = pltpu.roll(x, (to - lane) % 128, 1) if to != lane else x
    return jnp.concatenate([y, y], axis=1)


def last_lane(x, lane):
    return moved(x, lane, 127)


def first_lane(x, lane):
    return moved(x, lane, 0)


def merge_kernel(slab_l, slab_r, own_l, own_r, raw, old_a, old_b, msg_a, msg_b, ext, turned):
    rows = slab_l.shape[0]
    for n, pair in enumerate(((slab_l, own_r), (own_l, slab_r))):
        for m, x in enumerate(pair):
            ext[n, 16 * m : 16 * m + 8, :] = x[0:8, :]
            ext[n, 16 * m + 8 : 16 * m + 16, :] = x[rows - 8 : rows, :]
    lt, rt = turn(turned, ext[0], ext[1])
    q0, q1 = column_left(lt, *(right_field(rt, n) for n in range(4)))
    q0r, q1r = column_right(rt)
    row = lambda n, t: raw[QROW + 2 * n + t]
    last = iota((LV, raw.shape[2]), 1) == raw.shape[2] - 1
    up, down = [], []
    for t in range(2):
        sums = row(0, t) + row(1, t)
        first = jnp.where(last, last_lane(q0[t], 16), row(0, t))
        up.append(first + right_shift(sums, first_lane(q0[t], 0) + first_lane(q1[t], 1)))
        one = jnp.where(last, last_lane(q1[t], 31), row(2, t))
        two = jnp.where(last, last_lane(q0[t], 30), row(3, t))
        down.append(left_shift(one + two, last_lane(q1r[t], 31) + last_lane(q0r[t], 30)) + one)

    def store(msg_up, msg_down):
        for msg, sums, r in ((msg_up, up, 0), (msg_down, down, rows - 1)):
            for n in range(2):
                msg[LV * n : LV * n + LV, :] = sums[n]
            msg[68:69, 0:128] = slab_l[r : r + 1, :]
            msg[68:69, 128:256] = slab_r[r : r + 1, :]

    by_parity(store, msg_a, msg_b)


(CY, _, CQ, CZ, CP, _, C0, _, C1, _) = range(10)
(K00, _, K11, _, K0B, _, K1E, _, KM1, _, KMB, _, KMR, _) = range(14)


def turn(turned, *slabs):
    for n, x in enumerate(slabs):
        turned[n] = jnp.transpose(x)
    return [turned.at[n] for n in range(len(slabs))]


def middle_kernel(parity, *refs):
    @pl.when(lax.rem(lax.axis_index("py"), 2) == parity)
    def _():
        middle(*refs[:8], *refs[-7:])


def middle(v, vt, geo, q, slab_l, slab_r, own_l, own_r, vertex, kinetic, cell, edge, keep, ext, turned):
    rows = kinetic.shape[1]
    end = rows - 1
    for n, x in enumerate((slab_l, slab_r, own_l, own_r)):
        ext[n, BASE : BASE + rows, :] = x[...]
    lt, rt, ot, et = turn(turned, *(ext[n] for n in range(4)))
    q0l, q1l = column_left(lt, *(right_field(ot, n) for n in range(4)))
    q0r, q1r = column_right(rt)
    q0c, q1c = column_left(et, *(right_field(rt, n) for n in range(4)))
    up = lambda x: pltpu.roll(x, 127, 1)
    dn = lambda x: pltpu.roll(x, 1, 1)
    columns = [
        q0l[0] + q1l[0] + up(q1l[0]),
        q0l[1] + q1l[1] + up(q1l[1]),
        up(q1l[0]),
        lt[LEN : LEN + LV, :] + jnp.where(iota((LV, 128), 1) < BASE + end, up(lt[LEN + LV : LEN + 2 * LV, :]), 0.0),
        q0r[0] + q1r[0] + dn(q0r[0]),
        q0r[1] + q1r[1] + dn(q0r[1]),
        *q0c,
        *q1c,
    ]
    packed = jnp.concatenate(columns + [jnp.zeros((128 - LV * len(columns), 128), F32)], axis=0)
    inject = jnp.transpose(packed)[BASE : BASE + rows, :]
    moving = [pltpu.roll(inject, ((0 if n <= CZ else 127) - LV * n) % 128, 1) for n in range(len(columns))]
    side = iota(kinetic.shape[1:], 1)
    final = kinetic.shape[2] - 1
    for lev in range(LV):
        if lev:
            moving = [pltpu.roll(x, 127, 1) for x in moving]
        col = lambda n: jnp.concatenate([moving[n]] * 2, axis=1)
        put = lambda n, x, r, lev=lev: keep.__setitem__((n, slice(lev, lev + 1), slice(None)), x[r : r + 1, :])
        grads = []
        for t in range(2):
            q0 = jnp.where(side == final, col(C0 + t), q[t, 0, lev])
            q1 = jnp.where(side == final, col(C1 + t), q[t, 1, lev])
            q0d = pltpu.roll(q0, 1, 0)
            q1u = pltpu.roll(q1, end, 0)
            both = q0 + q1
            p, y = both + q0d, both + q1u
            m = p + right_shift(y, col(CY + t))
            m1 = left_shift(p, col(CP + t)) + y
            grads.append((pltpu.roll(m, end, 0) - m, m1 - m, pltpu.roll(m1, 1, 0) - m))
            put(K00 + t, q0, 0)
            put(K11 + t, q1, 1)
            put(K0B + t, q0, end - 1)
            put(K1E + t, q1, end)
            put(KM1 + t, m, 1)
            put(KMB + t, m, end - 1)
            put(KMR + t, m1, end - 1)
            if t == 0:
                cell[lev] = m * (1.0 / 6.0)
                vertex[0, lev] = q0
                vertex[1, lev] = q1
                means = (q0 + right_shift(q1u, col(CQ)), both, q1 + q0d)
        for e in range(3):
            edge[e, lev] = 0.5 * means[e] - geo[2 + e] * (v[e, lev] * grads[0][e] + vt[e, lev] * grads[1][e])
        en = [energy(geo[5 + e], v[e, lev], vt[e, lev]) for e in range(3)]
        zz = right_shift(en[1] + row_up(en[2], 0.0), col(CZ))
        kinetic[lev] = (en[0] + en[1] + en[2] + row_down(en[0], 0.0) + zz) * geo[8]


def rims(vertex, kinetic, cell, edge, ext, turned, k, f, geo, slab_l, slab_r, own0, raw, keep, up_msg, down_msg):
    rows = slab_l.shape[0]
    end = rows - 1
    above = lambda n: up_msg[LV * n : LV * n + LV, :]
    below = lambda n: down_msg[LV * n : LV * n + LV, :]
    ka = [up_msg[64 + n : 65 + n, :] for n in range(4)]
    kb = [down_msg[64 + n : 65 + n, :] for n in range(4)]
    krow = lambda a, b, r: k[a, b, r : r + 1, :]

    ext[0, BASE : BASE + rows, :] = slab_l[...]
    ext[1, BASE : BASE + rows, :] = slab_r[...]
    ext[1, OWN + BASE : OWN + BASE + rows, :] = own0[...]
    ext[0, DNB : DNB + 1, :] = up_msg[68:69, 0:128]
    ext[1, DNB : DNB + 1, :] = up_msg[68:69, 128:256]
    ext[1, UPB : UPB + 1, :] = down_msg[68:69, 128:256]
    lt, rt = turn(turned, ext[0], ext[1])
    own = [pltpu.roll(right_field(rt, n), OWN, 1) for n in range(4)]
    lanes = iota((LV, 128), 1)
    low = lambda x, row: jnp.where(lanes == UPB, pltpu.roll(row[:, 0:128], UPB, 1), x)
    high = lambda x, row: jnp.where(lanes == DNB, pltpu.roll(row[:, 0:128], DNB, 1), x)
    h0 = [high(low(own[t], below(2 + t)), above(2 + t)) for t in range(2)]
    u00 = [low(own[2 + t], below(4 + t)) for t in range(2)]
    q0l, q1l = column_left(lt, *h0, *u00)
    q0r, q1r = column_right(rt)
    up = lambda x: pltpu.roll(x, 127, 1)
    dn = lambda x: pltpu.roll(x, 1, 1)
    ycol = [q0l[t] + q1l[t] + up(q1l[t]) for t in range(2)]
    pcol = [q0r[t] + q1r[t] + dn(q0r[t]) for t in range(2)]
    r0, re = BASE, BASE + end

    hb1 = [left_shift(below(2 + t), last_lane(right_field(rt, t), UPB)) for t in range(2)]
    ub1 = [left_shift(below(4 + t), last_lane(right_field(rt, 2 + t), UPB)) for t in range(2)]
    h01 = [left_shift(raw[TH + t], last_lane(right_field(rt, t), BASE)) for t in range(2)]
    qb = section_sums(
        kb[3] + below(4) - below(6) + raw[TU2],
        below(5) - below(7) + raw[TU2T],
        *(kb[0] * below(2 + t) + kb[1] * raw[TH + t] + kb[2] * hb1[t] for t in range(2)),
    )
    q1f = section_sums(
        af_row(k, f, 1, 0) + raw[TU1] - raw[TU2] - ub1[0],
        raw[TU1T] - raw[TU2T] - ub1[1],
        *(krow(1, 0, 0) * raw[TH + t] + krow(1, 1, 0) * h01[t] + krow(1, 2, 0) * hb1[t] for t in range(2)),
    )
    ha1 = [left_shift(above(2 + t), last_lane(right_field(rt, t), DNB)) for t in range(2)]
    he1 = [left_shift(raw[BH + t], last_lane(right_field(rt, t), re)) for t in range(2)]
    ue1 = [left_shift(raw[BU0 + t], last_lane(right_field(rt, 2 + t), re)) for t in range(2)]
    qa = section_sums(
        ka[3] + above(4) - above(6) - ue1[0],
        above(5) - above(7) - ue1[1],
        *(ka[0] * above(2 + t) + ka[1] * ha1[t] + ka[2] * he1[t] for t in range(2)),
    )
    q0e = section_sums(
        af_row(k, f, 0, end) + raw[BU0] - raw[BU1] + above(6),
        raw[BU0T] - raw[BU1T] + above(7),
        *(krow(0, 0, end) * raw[BH + t] + krow(0, 1, end) * above(2 + t) + krow(0, 2, end) * he1[t] for t in range(2)),
    )
    vertex[1, :, 0, :] = q1f[0]
    vertex[0, :, end, :] = q0e[0]
    low_energy = energy(down_msg[69:70, :], below(4), below(5))
    high_energy = energy(up_msg[69:70, :], above(6), above(7))
    high_energy = right_shift(high_energy, first_lane(lt[LEN + LV : LEN + 2 * LV, :], DNB))
    kinetic[:, 0, :] = kinetic[:, 0, :] + low_energy * geo[8, 0:1, :]
    kinetic[:, end, :] = kinetic[:, end, :] + high_energy * geo[8, end : end + 1, :]
    grads = []
    for t in range(2):
        p0, y0 = keep[K00 + t] + q1f[t] + qb[t], keep[K00 + t] + q1f[t] + keep[K11 + t]
        pe, ye = q0e[t] + keep[K1E + t] + keep[K0B + t], q0e[t] + keep[K1E + t] + qa[t]
        m0 = p0 + right_shift(y0, first_lane(ycol[t], r0))
        m0r = left_shift(p0, last_lane(pcol[t], r0)) + y0
        me = pe + right_shift(ye, first_lane(ycol[t], re))
        mer = left_shift(pe, last_lane(pcol[t], re)) + ye
        m_above = above(t) + qa[t] + right_shift(qa[t], first_lane(q1l[t], DNB)) + q0e[t]
        m_below = below(t) + qb[t] + left_shift(qb[t], last_lane(q0r[t], UPB)) + q1f[t]
        grads.append(
            (
                keep[KM1 + t] - m0,
                m0r - m0,
                m_below - m0,
                m0r - keep[KM1 + t],
                me - keep[KMB + t],
                m_above - me,
                mer - me,
                keep[KMR + t] - me,
            )
        )
        if t == 0:
            cell[:, 0, :] = m0 * (1.0 / 6.0)
            cell[:, end, :] = me * (1.0 / 6.0)
            means = (
                keep[K00] + right_shift(keep[K11], first_lane(q1l[0], r0 + 1)),
                keep[K00] + q1f[0],
                q1f[0] + qb[0],
                keep[K11] + keep[K00],
                keep[K0B] + right_shift(keep[K1E], first_lane(q1l[0], re)),
                q0e[0] + right_shift(qa[0], first_lane(q1l[0], DNB)),
                q0e[0] + keep[K1E],
                keep[K1E] + keep[K0B],
            )
    for n, (e, r) in enumerate(RIM):
        r = r % rows
        edge[e, :, r, :] = 0.5 * means[n] - geo[2 + e, r : r + 1, :] * (
            raw[30 + 2 * n] * grads[0][n] + raw[31 + 2 * n] * grads[1][n]
        )


def last_kernel(
    k, f, geo, slab_l, slab_r, own0, raw, keep, vertex_i, kinetic_i, cell_i, edge_i, msg_a, msg_b,
    vertex, kinetic, cell, edge, vertex_v, kinetic_v, cell_v, edge_v, ext, turned, sems,
):
    rows = kinetic_v.shape[1]
    copies = []

    def start(src, dst):
        copy = pltpu.make_async_copy(src, dst, sems.at[len(copies)])
        copy.start()
        copies.append(copy)

    def start_rows(low, high, vertices):
        part = slice(low, high)
        for n, part_n in vertices:
            start(vertex_v.at[n, :, part_n], vertex.at[n, :, part_n])
        start(kinetic_v.at[:, part], kinetic.at[:, part])
        start(cell_v.at[:, part], cell.at[:, part])
        start(edge_v.at[:, :, part], edge.at[:, :, part])

    start_rows(8, rows - 8, ((0, slice(0, rows - 8)), (1, slice(8, rows))))
    by_parity(
        functools.partial(
            rims, vertex_v, kinetic_v, cell_v, edge_v, ext, turned, k, f, geo, slab_l, slab_r, own0, raw, keep
        ),
        msg_b,
        msg_a,
    )
    start_rows(0, 8, ((1, slice(0, 8)),))
    start_rows(rows - 8, rows, ((0, slice(rows - 8, rows)),))
    for copy in copies:
        copy.wait()


LAST_COPIES = 5 + 4 + 4


def shift(x, axis, by):
    n = lax.axis_size(axis)
    return lax.ppermute(x, axis, [(i, (i + by) % n) for i in range(n)])


def swap(x, axis, start):
    n = lax.axis_size(axis)
    pairs = []
    for i in range(start, n + start, 2):
        a, b = i % n, (i + 1) % n
        pairs += [(a, b), (b, a)]
    return lax.ppermute(x, axis, pairs)


VM = pl.BlockSpec(memory_space=pltpu.VMEM)
ANY = pl.BlockSpec(memory_space=pl.ANY)


def call(kernel, args, outs, scratch=(), sems=0, hbm_in=False, hbm_out=0, flops=0, alias=None):
    args = [pltpu.with_memory_space_constraint(x, pltpu.HBM if hbm_in else pltpu.VMEM) for x in args]
    return pl.pallas_call(
        kernel,
        out_shape=[jax.ShapeDtypeStruct(s, F32) if n < hbm_out else pltpu.VMEM(s, F32) for n, s in enumerate(outs)],
        in_specs=[ANY if hbm_in else VM] * len(args),
        out_specs=[ANY if n < hbm_out else VM for n in range(len(outs))],
        scratch_shapes=[pltpu.VMEM(s, F32) for s in scratch]
        + ([pltpu.SemaphoreType.DMA((sems,))] if sems else []),
        input_output_aliases=alias or {},
        compiler_params=pltpu.CompilerParams(vmem_limit_bytes=16 * 2**20),
        cost_estimate=pl.CostEstimate(flops=flops, transcendentals=0, bytes_accessed=0) if flops else None,
    )(*args)


def step(*args):
    levels, rows, cols = args[1].shape
    slab = (rows, 128)
    send_right, send_left, *held = call(
        pack_kernel, args, [slab, slab] + [x.shape for x in args], sems=PACK_COPIES, hbm_in=True
    )
    v, _, vt, _, _, _, _, k, f = held
    slab_l = shift(send_right, "px", 1)
    slab_r = shift(send_left, "px", -1)
    whole = [(2, levels, rows, cols), (levels, rows, cols), (levels, rows, cols), (3, levels, rows, cols)]
    raw, geo, q, msg_a, msg_b = call(
        vertex_kernel,
        held,
        [(RAW, levels, cols), (9, rows, cols), (2, 2, levels, rows, cols), (72, cols), (72, cols)],
        flops=40_000_000,
    )
    turned = [(4, 128, 128), (4, 128, 128)]
    msg_a, msg_b = call(
        merge_kernel,
        [slab_l, slab_r, send_left, send_right, raw, msg_a, msg_b],
        [(72, cols), (72, cols)],
        [(2, 128, 128), (2, 128, 128)],
        alias={5: 0, 6: 1},
    )
    msg_b = swap(msg_b, "py", 1)
    msg_a = swap(msg_a, "py", 0)
    sources = [v, vt, geo, q, slab_l, slab_r, send_left, send_right]
    results = whole + [(14, levels, cols)]
    parts = call(functools.partial(middle_kernel, 1), sources, results, turned, flops=40_000_000)
    *parts, keep = call(
        functools.partial(middle_kernel, 0),
        [*sources, *parts],
        results,
        turned,
        flops=40_000_000,
        alias={len(sources) + n: n for n in range(5)},
    )
    outs = call(
        last_kernel,
        [k, f, geo, slab_l, slab_r, send_left, raw, keep, *parts, msg_a, msg_b],
        whole + whole,
        [(2, 128, 128), (2, 128, 128)],
        sems=LAST_COPIES,
        hbm_out=4,
        alias={8 + n: 4 + n for n in range(4)},
    )
    return tuple(outs[:4])


def solution(mesh):
    field = P(None, "py", "px")
    pair = P(None, None, "py", "px")
    return jax.shard_map(
        step,
        mesh=mesh,
        in_specs=(pair, field, pair, field, field, field, P("py", "px"), pair, field),
        out_specs=(pair, field, field, pair),
        check_vma=False,
    )
```

```python
import functools

import jax
import jax.numpy as jnp
from jax import lax
from jax.experimental import pallas as pl
from jax.experimental.pallas import tpu as pltpu
from jax.sharding import PartitionSpec as P

F32 = jnp.float32
LV = 8
BASE = 8
HALO, OWN = 32, 64


def iota(shape, dim):
    return lax.broadcasted_iota(jnp.int32, shape, dim)


def left_shift(x, col):
    n = x.shape[1]
    return jnp.where(iota(x.shape, 1) == n - 1, col, pltpu.roll(x, n - 1, 1))


def right_shift(x, col):
    return jnp.where(iota(x.shape, 1) == 0, col, pltpu.roll(x, 1, 1))


def row_up(x, row):
    n = x.shape[0]
    return jnp.where(iota(x.shape, 0) == n - 1, row, pltpu.roll(x, n - 1, 0))


def row_down(x, row):
    return jnp.where(iota(x.shape, 0) == 0, row, pltpu.roll(x, 1, 0))


def section_sums(n0, dn, d0, dd):
    n1, d1 = n0 + dn, d0 + dd
    ns, ds = n0 + n1, d0 + d1
    ends = d0 * d1
    inv = 1.0 / (ends * ds)
    half = ns * ends * inv
    side = ds * inv
    last = n1 * d0 * side
    first = n0 * d1 * side
    return (first + last) * (1.0 / 6.0) + half * (2.0 / 3.0), half * (1.0 / 3.0) + last * (1.0 / 6.0)


def energy(w, v, vt):
    return w * (v * v + v * vt + vt * vt * (1.0 / 3.0))


RGEO = 96
LGEO, LEN, LFLD = 40, 48, 64
(TH, THT, _, _, TU0, _, TU1, TU1T, TU11, _, TU2, TU2T, TU21, _, TG2) = range(15)
(BH, BHT, _, _, BU0, BU0T, BU01, _, BU1, BU1T, BU11, _, BU2, _, BG0) = range(15, 30)
RIM = ((0, 0), (1, 0), (2, 0), (2, 1), (0, -2), (0, -1), (1, -1), (2, -1))
QROW = 30 + 2 * len(RIM)
RAW = QROW + 8


def pack_kernel(
    v, h, vt, ht, d, el, area, k, f, send_right, send_left, vo, ho, vto, hto, do, eo, ao, ko, fo, sems
):
    rows, cols = h.shape[1], h.shape[2]
    half = cols - 128
    for x, y in ((d, do), (el, eo), (k, ko), (f, fo)):
        pltpu.make_async_copy(x, y, sems.at[0]).start()
    pltpu.make_async_copy(area, ao, sems.at[0]).start()
    for n in range(2):
        cut = slice(n * LV // 2, (n + 1) * LV // 2)
        for x, y in ((h, ho), (ht, hto)):
            pltpu.make_async_copy(x.at[cut], y.at[cut], sems.at[1 + 2 * n]).start()
        for x, y in ((v, vo), (vt, vto)):
            pltpu.make_async_copy(x.at[:, cut], y.at[:, cut], sems.at[2 + 2 * n]).start()
    pltpu.make_async_copy(v.at[:, 0:5], vo.at[:, 0:5], sems.at[0]).wait()

    lanes = iota((rows, 128), 1)

    def push(stack, x, wide=1, first=0):
        if stack is None:
            return x
        back = pltpu.roll(stack, 128 - wide, 1)
        return jnp.where(lanes == 127, x, back) if first else jnp.where(lanes < wide, x, back)

    def place(slab, stack, by, start, stop):
        moved = pltpu.roll(stack, by % 128, 1) if by % 128 else stack
        return jnp.where((lanes >= start) & (lanes < stop), moved, slab)

    def geometry(part):
        out = [ko[a, b, :, part] for a in range(2) for b in range(3)]
        return out + [(out[3 * a] + out[3 * a + 1] + out[3 * a + 2]) * fo[a, :, part] for a in range(2)]

    low, high = slice(0, 128), slice(half, cols)
    geo_left = geo_right = None
    for x, y in zip(geometry(low), geometry(high)):
        geo_left = push(geo_left, x)
        geo_right = push(geo_right, y, 1, 127)
    near = [do[e, :, low] for e in range(3)]
    far = [do[e, :, high] for e in range(3)]
    weight = [0.25 * far[e] * eo[e, :, high] for e in range(3)]
    left, right = [None] * 8, [None] * 10
    for lev in range(LV):
        if lev % (LV // 2) == 0:
            n = 2 * (lev // (LV // 2))
            pltpu.make_async_copy(h, ho, sems.at[1 + n]).wait()
            pltpu.make_async_copy(v, vo, sems.at[2 + n]).wait()
        for part, dist, stacks in ((low, near, left), (high, far, right)):
            fields = [ho[lev, :, part], hto[lev, :, part]]
            fields += [dist[e] * x[e, lev, :, part] for e in range(3) for x in (vo, vto)]
            if part is high:
                fields += [energy(weight[e], vo[e, lev, :, part], vto[e, lev, :, part]) for e in (1, 2)]
            for n, x in enumerate(fields):
                stacks[n] = push(stacks[n], x, *((1, 127) if part is high else (2,) if n < 4 else (1,)))
    to_left = jnp.zeros((rows, 128), F32)
    to_right = right[7]
    for n in range(4):
        to_left = place(to_left, left[n], 16 * n + 14, 16 * n, 16 * n + 16)
        to_left = place(to_left, left[n + 4], 64 + LV * n + 7, 64 + LV * n, 72 + LV * n)
    to_left = place(to_left, geo_left, RGEO + 7, RGEO, RGEO + 8)
    for n in range(7):
        to_right = place(to_right, right[n], LFLD + LV * n - 120, LFLD + LV * n, LFLD + LV * n + LV)
    for n in range(2):
        to_right = place(to_right, right[8 + n], LEN + LV * n - 120, LEN + LV * n, LEN + LV * n + LV)
    to_right = place(to_right, geo_right, LGEO - 120, LGEO, LGEO + 8)
    send_right[...] = to_right
    send_left[...] = to_left


PACK_WAITS = 5


def vertex_kernel(v, h, vt, ht, d, el, area, k, f, raw, geo, q, msg_a, msg_b):
    rows = h.shape[1]
    end = rows - 1
    for x, n in ((h, TH), (ht, THT)):
        raw[n] = x[:, 0, :]
        raw[n + 2] = x[:, 1, :]
    for x, n in ((h, BH), (ht, BHT)):
        raw[n] = x[:, end, :]
        raw[n + 2] = x[:, end - 1, :]
    for x, t in ((v, 0), (vt, 1)):
        for e, r, n in (
            (0, 0, TU0),
            (1, 0, TU1),
            (1, 1, TU11),
            (2, 0, TU2),
            (2, 1, TU21),
            (0, end, BU0),
            (0, end - 1, BU01),
            (1, end, BU1),
            (1, end - 1, BU11),
            (2, end, BU2),
        ):
            raw[n + t] = d[e, r : r + 1, :] * x[e, :, r, :]
    for e, r, n in ((2, 0, TG2), (0, end, BG0)):
        raw[n] = jnp.broadcast_to(0.25 * el[e, r : r + 1, :] / d[e, r : r + 1, :], raw.shape[1:])
    for a in range(2):
        geo[a] = (k[a, 0] + k[a, 1] + k[a, 2]) * f[a]
    for e in range(3):
        geo[2 + e] = (1.0 / 12.0) / d[e]
        geo[5 + e] = 0.25 * d[e] * el[e]
    geo[8] = 1.0 / area[...]
    for n, (e, r) in enumerate(RIM):
        for x, t in ((v, 0), (vt, 1)):
            raw[30 + 2 * n + t] = x[e, :, r % rows, :]

    up = lambda x: pltpu.roll(x, rows - 1, 0)
    dn = lambda x: pltpu.roll(x, 1, 0)
    right = lambda x: pltpu.roll(x, x.shape[1] - 1, 1)
    for lev in range(LV):
        hh = [x[lev] for x in (h, ht)]
        u = [[d[e] * x[e, lev] for x in (v, vt)] for e in range(3)]
        h1 = [right(x) for x in hh]
        u01 = [right(x) for x in u[0]]
        n0 = [u[0][t] - u[1][t] + up(u[2][t]) for t in range(2)]
        n1 = [u[1][t] - u[2][t] - dn(u01[t]) for t in range(2)]
        d0 = [k[0, 0] * hh[t] + k[0, 1] * up(hh[t]) + k[0, 2] * h1[t] for t in range(2)]
        d1 = [k[1, 0] * hh[t] + k[1, 1] * h1[t] + k[1, 2] * dn(h1[t]) for t in range(2)]
        q0 = section_sums(geo[0] + n0[0], n0[1], *d0)
        q1 = section_sums(geo[1] + n1[0], n1[1], *d1)
        for t in range(2):
            q[t, 0, lev] = q0[t]
            q[t, 1, lev] = q1[t]
            for n, x, r in ((0, q0, 0), (1, q1, 1), (2, q1, end), (3, q0, end - 1)):
                raw[QROW + 2 * n + t, lev : lev + 1, :] = x[t][r : r + 1, :]

    def fill(msg_up, msg_down):
        for msg, parts, a, r in (
            (msg_up, (TH, THT, TU1, TU1T, TU2, TU2T), 1, 0),
            (msg_down, (BH, BHT, BU0, BU0T, BU1, BU1T), 0, end),
        ):
            for n, part in enumerate(parts):
                msg[LV * (n + 2) : LV * (n + 3), :] = raw[part]
            for n in range(3):
                msg[64 + n : 65 + n, :] = k[a, n, r : r + 1, :]
            msg[67:68, :] = af_row(k, f, a, r)
            msg[69:70, :] = raw[BG0 if r else TG2, 0:1, :]
            msg[70:72, :] = jnp.zeros((2, msg.shape[1]), F32)

    by_parity(fill, msg_a, msg_b)


def by_parity(body, first, second):
    odd = lax.rem(lax.axis_index("py"), 2) == 1

    @pl.when(odd)
    def _():
        body(first, second)

    @pl.when(jnp.logical_not(odd))
    def _():
        body(second, first)


def af_row(k, f, a, r):
    return (k[a, 0, r : r + 1, :] + k[a, 1, r : r + 1, :] + k[a, 2, r : r + 1, :]) * f[a, r : r + 1, :]


def left_field(t, n):
    return t[LFLD + LV * n : LFLD + LV * n + LV, :]


def right_field(t, n, c=0):
    if n >= 4:
        return t[32 + LV * n : 32 + LV * n + LV, :]
    return t[pl.ds(16 * n + c, LV, stride=2), :]


def column_left(lt, h0, h0t, u00, u00t):
    k = [lt[LGEO + n : LGEO + n + 1, :] for n in range(8)]
    up = lambda x: pltpu.roll(x, 127, 1)
    dn = lambda x: pltpu.roll(x, 1, 1)
    h, hp, u0, u0p, u1, u1p, u2, u2p = (left_field(lt, n) for n in range(8))
    q0 = section_sums(
        k[6] + u0 - u1 + up(u2),
        u0p - u1p + up(u2p),
        k[0] * h + k[1] * up(h) + k[2] * h0,
        k[0] * hp + k[1] * up(hp) + k[2] * h0t,
    )
    q1 = section_sums(
        k[7] + u1 - u2 - dn(u00),
        u1p - u2p - dn(u00t),
        k[3] * h + k[4] * h0 + k[5] * dn(h0),
        k[3] * hp + k[4] * h0t + k[5] * dn(h0t),
    )
    return q0, q1


def column_right(rt):
    k = [rt[RGEO + n : RGEO + n + 1, :] for n in range(8)]
    up = lambda x: pltpu.roll(x, 127, 1)
    dn = lambda x: pltpu.roll(x, 1, 1)
    h, hp, u0, u0p, u1, u1p, u2, u2p = (right_field(rt, n) for n in range(8))
    h1, h1p, u01, u01p = (right_field(rt, n, 1) for n in range(4))
    q0 = section_sums(
        k[6] + u0 - u1 + up(u2),
        u0p - u1p + up(u2p),
        k[0] * h + k[1] * up(h) + k[2] * h1,
        k[0] * hp + k[1] * up(hp) + k[2] * h1p,
    )
    q1 = section_sums(
        k[7] + u1 - u2 - dn(u01),
        u1p - u2p - dn(u01p),
        k[3] * h + k[4] * h1 + k[5] * dn(h1),
        k[3] * hp + k[4] * h1p + k[5] * dn(h1p),
    )
    return q0, q1


def moved(x, lane, to):
    y = pltpu.roll(x, (to - lane) % 128, 1) if to != lane else x
    return jnp.concatenate([y, y], axis=1)


def last_lane(x, lane):
    return moved(x, lane, 127)


def first_lane(x, lane):
    return moved(x, lane, 0)


def merge_kernel(slab_l, slab_r, own_l, own_r, raw, old_a, old_b, msg_a, msg_b, ext, turned):
    rows = slab_l.shape[0]
    for n, pair in enumerate(((slab_l, own_r), (own_l, slab_r))):
        for m, x in enumerate(pair):
            ext[n, 16 * m : 16 * m + 8, :] = x[0:8, :]
            ext[n, 16 * m + 8 : 16 * m + 16, :] = x[rows - 8 : rows, :]
    for n in range(2):
        turned[n, :, 0:32] = jnp.transpose(ext[n, 0:32, :])
    lt, rt = turned.at[0], turned.at[1]
    q0, q1 = column_left(lt, *(right_field(rt, n) for n in range(4)))
    q0r, q1r = column_right(rt)
    row = lambda n, t: raw[QROW + 2 * n + t]
    last = iota((LV, raw.shape[2]), 1) == raw.shape[2] - 1
    up, down = [], []
    for t in range(2):
        sums = row(0, t) + row(1, t)
        first = jnp.where(last, last_lane(q0[t], 16), row(0, t))
        up.append(first + right_shift(sums, first_lane(q0[t], 0) + first_lane(q1[t], 1)))
        one = jnp.where(last, last_lane(q1[t], 31), row(2, t))
        two = jnp.where(last, last_lane(q0[t], 30), row(3, t))
        down.append(left_shift(one + two, last_lane(q1r[t], 31) + last_lane(q0r[t], 30)) + one)

    def store(msg_up, msg_down):
        for msg, sums, r in ((msg_up, up, 0), (msg_down, down, rows - 1)):
            for n in range(2):
                msg[LV * n : LV * n + LV, :] = sums[n]
            msg[68:69, 0:128] = slab_l[r : r + 1, :]
            msg[68:69, 128:256] = slab_r[r : r + 1, :]

    by_parity(store, msg_a, msg_b)


(CY, _, CQ, CZ, CP, _, C0, _, C1, _) = range(10)
(K00, _, K11, _, K0B, _, K1E, _, KM1, _, KMB, _, KMR, _) = range(14)


def turn(turned, *slabs):
    for n, x in enumerate(slabs):
        turned[n] = jnp.transpose(x)
    return [turned.at[n] for n in range(len(slabs))]


def middle_kernel(parity, *refs):
    @pl.when(lax.rem(lax.axis_index("py"), 2) == parity)
    def _():
        middle(*refs[:8], *refs[-7:])


def middle(v, vt, geo, q, slab_l, slab_r, own_l, own_r, vertex, kinetic, cell, edge, keep, ext, turned):
    rows = kinetic.shape[1]
    end = rows - 1
    for n, x in enumerate((slab_l, slab_r, own_l, own_r)):
        ext[n, BASE : BASE + rows, :] = x[...]
    lt, rt, ot, et = turn(turned, *(ext[n] for n in range(4)))
    q0l, q1l = column_left(lt, *(right_field(ot, n) for n in range(4)))
    q0r, q1r = column_right(rt)
    q0c, q1c = column_left(et, *(right_field(rt, n) for n in range(4)))
    up = lambda x: pltpu.roll(x, 127, 1)
    dn = lambda x: pltpu.roll(x, 1, 1)
    columns = [
        q0l[0] + q1l[0] + up(q1l[0]),
        q0l[1] + q1l[1] + up(q1l[1]),
        up(q1l[0]),
        lt[LEN : LEN + LV, :] + jnp.where(iota((LV, 128), 1) < BASE + end, up(lt[LEN + LV : LEN + 2 * LV, :]), 0.0),
        q0r[0] + q1r[0] + dn(q0r[0]),
        q0r[1] + q1r[1] + dn(q0r[1]),
        *q0c,
        *q1c,
    ]
    packed = jnp.concatenate(columns + [jnp.zeros((128 - LV * len(columns), 128), F32)], axis=0)
    inject = jnp.transpose(packed)[BASE : BASE + rows, :]
    moving = [pltpu.roll(inject, ((0 if n <= CZ else 127) - LV * n) % 128, 1) for n in range(len(columns))]
    side = iota(kinetic.shape[1:], 1)
    final = kinetic.shape[2] - 1
    for lev in range(LV):
        if lev:
            moving = [pltpu.roll(x, 127, 1) for x in moving]
        col = lambda n: jnp.concatenate([moving[n]] * 2, axis=1)
        put = lambda n, x, r, lev=lev: keep.__setitem__((n, slice(lev, lev + 1), slice(None)), x[r : r + 1, :])
        grads = []
        for t in range(2):
            q0 = jnp.where(side == final, col(C0 + t), q[t, 0, lev])
            q1 = jnp.where(side == final, col(C1 + t), q[t, 1, lev])
            q0d = pltpu.roll(q0, 1, 0)
            q1u = pltpu.roll(q1, end, 0)
            both = q0 + q1
            p, y = both + q0d, both + q1u
            m = p + right_shift(y, col(CY + t))
            m1 = left_shift(p, col(CP + t)) + y
            grads.append((pltpu.roll(m, end, 0) - m, m1 - m, pltpu.roll(m1, 1, 0) - m))
            put(K00 + t, q0, 0)
            put(K11 + t, q1, 1)
            put(K0B + t, q0, end - 1)
            put(K1E + t, q1, end)
            put(KM1 + t, m, 1)
            put(KMB + t, m, end - 1)
            put(KMR + t, m1, end - 1)
            if t == 0:
                cell[lev] = m * (1.0 / 6.0)
                vertex[0, lev] = q0
                vertex[1, lev] = q1
                means = (q0 + right_shift(q1u, col(CQ)), both, q1 + q0d)
        for e in range(3):
            edge[e, lev] = 0.5 * means[e] - geo[2 + e] * (v[e, lev] * grads[0][e] + vt[e, lev] * grads[1][e])
        en = [energy(geo[5 + e], v[e, lev], vt[e, lev]) for e in range(3)]
        zz = right_shift(en[1] + row_up(en[2], 0.0), col(CZ))
        kinetic[lev] = (en[0] + en[1] + en[2] + row_down(en[0], 0.0) + zz) * geo[8]


def rims(vertex, kinetic, cell, edge, ext, turned, k, f, geo, slab_l, slab_r, own0, raw, keep, up_msg, down_msg):
    rows = slab_l.shape[0]
    end = rows - 1
    above = lambda n: up_msg[LV * n : LV * n + LV, :]
    below = lambda n: down_msg[LV * n : LV * n + LV, :]
    ka = [up_msg[64 + n : 65 + n, :] for n in range(4)]
    kb = [down_msg[64 + n : 65 + n, :] for n in range(4)]
    krow = lambda a, b, r: k[a, b, r : r + 1, :]

    before, r0, re, after = 7, 8, 23, 24
    for n, x in enumerate((slab_l, slab_r, own0)):
        ext[0, HALO * n + r0 : HALO * n + r0 + 8, :] = x[0:8, :]
        ext[0, HALO * n + re - 7 : HALO * n + re + 1, :] = x[rows - 8 : rows, :]
    ext[0, after : after + 1, :] = up_msg[68:69, 0:128]
    ext[0, HALO + after : HALO + after + 1, :] = up_msg[68:69, 128:256]
    ext[0, HALO + before : HALO + before + 1, :] = down_msg[68:69, 128:256]
    (both,) = turn(turned, ext[0])
    own = [pltpu.roll(right_field(both, n), 128 - OWN, 1) for n in range(4)]
    lanes = iota((LV, 128), 1)
    low = lambda x, row: jnp.where(lanes == before, pltpu.roll(row[:, 0:128], before, 1), x)
    high = lambda x, row: jnp.where(lanes == after, pltpu.roll(row[:, 0:128], after, 1), x)
    h0 = [high(low(own[t], below(2 + t)), above(2 + t)) for t in range(2)]
    u00 = [low(own[2 + t], below(4 + t)) for t in range(2)]
    q0l, q1l = column_left(both, *h0, *u00)
    q0r, q1r = column_right(both)
    up = lambda x: pltpu.roll(x, 127, 1)
    dn = lambda x: pltpu.roll(x, 1, 1)
    ycol = [q0l[t] + q1l[t] + up(q1l[t]) for t in range(2)]
    pcol = [q0r[t] + q1r[t] + dn(q0r[t]) for t in range(2)]

    hb1 = [left_shift(below(2 + t), last_lane(right_field(both, t), HALO + before)) for t in range(2)]
    ub1 = [left_shift(below(4 + t), last_lane(right_field(both, 2 + t), HALO + before)) for t in range(2)]
    h01 = [left_shift(raw[TH + t], last_lane(right_field(both, t), HALO + r0)) for t in range(2)]
    qb = section_sums(
        kb[3] + below(4) - below(6) + raw[TU2],
        below(5) - below(7) + raw[TU2T],
        *(kb[0] * below(2 + t) + kb[1] * raw[TH + t] + kb[2] * hb1[t] for t in range(2)),
    )
    q1f = section_sums(
        af_row(k, f, 1, 0) + raw[TU1] - raw[TU2] - ub1[0],
        raw[TU1T] - raw[TU2T] - ub1[1],
        *(krow(1, 0, 0) * raw[TH + t] + krow(1, 1, 0) * h01[t] + krow(1, 2, 0) * hb1[t] for t in range(2)),
    )
    ha1 = [left_shift(above(2 + t), last_lane(right_field(both, t), HALO + after)) for t in range(2)]
    he1 = [left_shift(raw[BH + t], last_lane(right_field(both, t), HALO + re)) for t in range(2)]
    ue1 = [left_shift(raw[BU0 + t], last_lane(right_field(both, 2 + t), HALO + re)) for t in range(2)]
    qa = section_sums(
        ka[3] + above(4) - above(6) - ue1[0],
        above(5) - above(7) - ue1[1],
        *(ka[0] * above(2 + t) + ka[1] * ha1[t] + ka[2] * he1[t] for t in range(2)),
    )
    q0e = section_sums(
        af_row(k, f, 0, end) + raw[BU0] - raw[BU1] + above(6),
        raw[BU0T] - raw[BU1T] + above(7),
        *(krow(0, 0, end) * raw[BH + t] + krow(0, 1, end) * above(2 + t) + krow(0, 2, end) * he1[t] for t in range(2)),
    )
    vertex[1, :, 0, :] = q1f[0]
    vertex[0, :, end, :] = q0e[0]
    low_energy = energy(down_msg[69:70, :], below(4), below(5))
    high_energy = energy(up_msg[69:70, :], above(6), above(7))
    high_energy = right_shift(high_energy, first_lane(both[LEN + LV : LEN + 2 * LV, :], after))
    kinetic[:, 0, :] = kinetic[:, 0, :] + low_energy * geo[8, 0:1, :]
    kinetic[:, end, :] = kinetic[:, end, :] + high_energy * geo[8, end : end + 1, :]
    grads = []
    for t in range(2):
        p0, y0 = keep[K00 + t] + q1f[t] + qb[t], keep[K00 + t] + q1f[t] + keep[K11 + t]
        pe, ye = q0e[t] + keep[K1E + t] + keep[K0B + t], q0e[t] + keep[K1E + t] + qa[t]
        m0 = p0 + right_shift(y0, first_lane(ycol[t], r0))
        m0r = left_shift(p0, last_lane(pcol[t], HALO + r0)) + y0
        me = pe + right_shift(ye, first_lane(ycol[t], re))
        mer = left_shift(pe, last_lane(pcol[t], HALO + re)) + ye
        m_above = above(t) + qa[t] + right_shift(qa[t], first_lane(q1l[t], after)) + q0e[t]
        m_below = below(t) + qb[t] + left_shift(qb[t], last_lane(q0r[t], HALO + before)) + q1f[t]
        grads.append(
            (
                keep[KM1 + t] - m0,
                m0r - m0,
                m_below - m0,
                m0r - keep[KM1 + t],
                me - keep[KMB + t],
                m_above - me,
                mer - me,
                keep[KMR + t] - me,
            )
        )
        if t == 0:
            cell[:, 0, :] = m0 * (1.0 / 6.0)
            cell[:, end, :] = me * (1.0 / 6.0)
            means = (
                keep[K00] + right_shift(keep[K11], first_lane(q1l[0], r0 + 1)),
                keep[K00] + q1f[0],
                q1f[0] + qb[0],
                keep[K11] + keep[K00],
                keep[K0B] + right_shift(keep[K1E], first_lane(q1l[0], re)),
                q0e[0] + right_shift(qa[0], first_lane(q1l[0], after)),
                q0e[0] + keep[K1E],
                keep[K1E] + keep[K0B],
            )
    for n, (e, r) in enumerate(RIM):
        r = r % rows
        edge[e, :, r, :] = 0.5 * means[n] - geo[2 + e, r : r + 1, :] * (
            raw[30 + 2 * n] * grads[0][n] + raw[31 + 2 * n] * grads[1][n]
        )


def last_kernel(
    k, f, geo, slab_l, slab_r, own0, raw, keep, vertex_i, kinetic_i, cell_i, edge_i, msg_a, msg_b,
    vertex, kinetic, cell, edge, vertex_v, kinetic_v, cell_v, edge_v, ext, turned, sems,
):
    rows = kinetic_v.shape[1]
    outputs = ((vertex_v, vertex), (kinetic_v, kinetic), (cell_v, cell), (edge_v, edge))

    def start_rows(low, high, vertices):
        part = slice(low, high)
        for n, part_n in vertices:
            pltpu.make_async_copy(vertex_v.at[n, :, part_n], vertex.at[n, :, part_n], sems.at[0]).start()
        for n in (1, 2):
            src, dst = outputs[n]
            pltpu.make_async_copy(src.at[:, part], dst.at[:, part], sems.at[n]).start()
        pltpu.make_async_copy(edge_v.at[:, :, part], edge.at[:, :, part], sems.at[3]).start()

    start_rows(8, rows - 8, ((0, slice(0, rows - 8)), (1, slice(8, rows))))
    by_parity(
        functools.partial(
            rims, vertex_v, kinetic_v, cell_v, edge_v, ext, turned, k, f, geo, slab_l, slab_r, own0, raw, keep
        ),
        msg_b,
        msg_a,
    )
    start_rows(0, 8, ((1, slice(0, 8)),))
    start_rows(rows - 8, rows, ((0, slice(rows - 8, rows)),))
    for n, (src, dst) in enumerate(outputs):
        pltpu.make_async_copy(src, dst, sems.at[n]).wait()


def shift(x, axis, by):
    n = lax.axis_size(axis)
    return lax.ppermute(x, axis, [(i, (i + by) % n) for i in range(n)])


def swap(x, axis, start):
    n = lax.axis_size(axis)
    pairs = []
    for i in range(start, n + start, 2):
        a, b = i % n, (i + 1) % n
        pairs += [(a, b), (b, a)]
    return lax.ppermute(x, axis, pairs)


VM = pl.BlockSpec(memory_space=pltpu.VMEM)
ANY = pl.BlockSpec(memory_space=pl.ANY)


def call(kernel, args, outs, scratch=(), sems=0, hbm_in=False, hbm_out=0, flops=0, alias=None):
    args = [pltpu.with_memory_space_constraint(x, pltpu.HBM if hbm_in else pltpu.VMEM) for x in args]
    return pl.pallas_call(
        kernel,
        out_shape=[jax.ShapeDtypeStruct(s, F32) if n < hbm_out else pltpu.VMEM(s, F32) for n, s in enumerate(outs)],
        in_specs=[ANY if hbm_in else VM] * len(args),
        out_specs=[ANY if n < hbm_out else VM for n in range(len(outs))],
        scratch_shapes=[pltpu.VMEM(s, F32) for s in scratch]
        + ([pltpu.SemaphoreType.DMA((sems,))] if sems else []),
        input_output_aliases=alias or {},
        compiler_params=pltpu.CompilerParams(vmem_limit_bytes=16 * 2**20),
        cost_estimate=pl.CostEstimate(flops=flops, transcendentals=0, bytes_accessed=0) if flops else None,
    )(*args)


def step(*args):
    levels, rows, cols = args[1].shape
    slab = (rows, 128)
    send_right, send_left, *held = call(
        pack_kernel, args, [slab, slab] + [x.shape for x in args], sems=PACK_WAITS, hbm_in=True
    )
    v, _, vt, _, _, _, _, k, f = held
    slab_l = shift(send_right, "px", 1)
    slab_r = shift(send_left, "px", -1)
    whole = [(2, levels, rows, cols), (levels, rows, cols), (levels, rows, cols), (3, levels, rows, cols)]
    raw, geo, q, msg_a, msg_b = call(
        vertex_kernel,
        held,
        [(RAW, levels, cols), (9, rows, cols), (2, 2, levels, rows, cols), (72, cols), (72, cols)],
        flops=40_000_000,
    )
    turned = [(4, 128, 128), (4, 128, 128)]
    msg_a, msg_b = call(
        merge_kernel,
        [slab_l, slab_r, send_left, send_right, raw, msg_a, msg_b],
        [(72, cols), (72, cols)],
        [(2, 128, 128), (2, 128, 128)],
        alias={5: 0, 6: 1},
    )
    msg_b = swap(msg_b, "py", 1)
    msg_a = swap(msg_a, "py", 0)
    sources = [v, vt, geo, q, slab_l, slab_r, send_left, send_right]
    results = whole + [(14, levels, cols)]
    parts = call(functools.partial(middle_kernel, 1), sources, results, turned, flops=40_000_000)
    *parts, keep = call(
        functools.partial(middle_kernel, 0),
        [*sources, *parts],
        results,
        turned,
        flops=40_000_000,
        alias={len(sources) + n: n for n in range(5)},
    )
    outs = call(
        last_kernel,
        [k, f, geo, slab_l, slab_r, send_left, raw, keep, *parts, msg_a, msg_b],
        whole + whole,
        [(1, 128, 128), (1, 128, 128)],
        sems=4,
        hbm_out=4,
        alias={8 + n: 4 + n for n in range(4)},
    )
    return tuple(outs[:4])


def solution(mesh):
    field = P(None, "py", "px")
    pair = P(None, None, "py", "px")
    return jax.shard_map(
        step,
        mesh=mesh,
        in_specs=(pair, field, pair, field, field, field, P("py", "px"), pair, field),
        out_specs=(pair, field, field, pair),
        check_vma=False,
    )
```
